128 devices in a mesh: dp: 4 (over x), cp: 32 (over z, y, core).
Axes of the slice: x: 4, y: 4, z: 4, core: 2. Of those that a mesh axis runs over, the one named last changes fastest.
Arguments:
- tokens: bfloat16 [4, 4096, 4096], P('dp', 'cp'), may hold values from -60 to 60
- qkv_weight: bfloat16 [4096, 3072], replicated, may hold values from -0.09375 to 0.09375
- owner_slot: int32 [4, 32], P('dp', 'cp'), may hold values from 0 to 3, as said below
- slab_sequence: int32 [4, 32], replicated, may hold values from 0 to 16, as said below
- slab_order: int32 [4, 32], replicated, may hold values from 0 to 15, as said below
Outputs:
- context: bfloat16 [4, 4096, 2048], P('dp', 'cp')
The draws below stay inside these ranges and needn't reach their ends.
Inputs may be any that keep to these rules, and one draw needn't show every extreme that they name: For every column c, the entries owner_slot[a, c] over all rows a are 0 to 3, each once. `slab_sequence`: in each row, the slabs with one sequence number carry the orders 0 to L-1, each once, L being their count; no sequence has more than 16 slabs. `slab_order`: see slab_sequence.
All inputs are finite; a program needn't handle non-finite values.
Results may differ from the reference program's by a relative error of at most 0.006.
The reference program's roundings to bfloat16 on the way count: a program that leaves them out, or rounds other values in their place, can miss the bound.
Values may be sent and summed in bfloat16 or wider, within the bound.
No kernel may reach another device: no remote copies, remote signals or barrier semaphores. Data moves between devices by JAX's collectives and lax.ppermute only.
A program may use at most 128 MiB of HBM per device.

```python
import jax
import jax.numpy as jnp
from jax import lax

D = 4096
QH = 16
KVH = 4
HD = 128
SLAB = 128
SLABS_DEV = 1
GROUPS = 4
ROW_SLABS = 32
ROW_TOK = 4096


def sequence_plan(key):
    half_count = ROW_SLABS // 2
    chosen_row = jax.random.randint(jax.random.fold_in(key, 9), (), 0, GROUPS)
    singles_flags = jnp.arange(GROUPS, dtype=jnp.int32) == chosen_row

    def one_row(row_key, singles):
        first_key, second_key = jax.random.split(row_key)
        index = jnp.arange(ROW_SLABS, dtype=jnp.int32)
        random_starts = jax.random.randint(first_key, (ROW_SLABS,), 0, 8) == 0
        later_starts = random_starts | (index == half_count) | singles
        starts = jnp.where(index < half_count, index == 0, later_starts)
        numbers = jnp.cumsum(starts.astype(jnp.int32)) - 1
        begins = lax.cummax(jnp.where(starts, index, 0))
        shuffle = jax.random.permutation(second_key, ROW_SLABS)
        return (numbers[shuffle].astype(jnp.int32), (index - begins)[shuffle].astype(jnp.int32))
    return jax.vmap(one_row)(jax.random.split(jax.random.fold_in(key, 7), GROUPS), singles_flags)


def draw_slab_sequence(key, part):
    return sequence_plan(key)[0]


def draw_slab_order(key, part):
    return sequence_plan(key)[1]


def draw_owner_slot(key, part):
    columns_count = ROW_SLABS // SLABS_DEV
    column_keys = jax.random.split(jax.random.fold_in(key, 3), columns_count)

    def one_column(column_key):
        return jax.random.permutation(column_key, GROUPS * SLABS_DEV).astype(jnp.int32).reshape(GROUPS, SLABS_DEV)
    stacked = jax.vmap(one_column)(column_keys)
    return stacked.transpose(1, 0, 2).reshape(GROUPS, ROW_SLABS)


def draw_tokens(key, part):
    first_key, second_key = jax.random.split(jax.random.fold_in(key, 11))
    values = jax.random.normal(first_key, (GROUPS, ROW_TOK, D), jnp.float32)
    values = jnp.clip(values, -6.0, 6.0)
    return values.astype(jnp.bfloat16)


def scatter_about(stream_key, extent, spread, most, kind=jnp.bfloat16):
    drawn = jax.random.normal(stream_key, extent, jnp.float32) * spread
    return jnp.minimum(jnp.maximum(drawn, -most), most).astype(kind)


def setup_inputs(seed: int = 0) -> dict:
    key_of = jax.random.split(jax.random.key(seed), 6)
    tokens = draw_tokens(jax.random.fold_in(key_of[5], 71), 0)
    qkv_weight = scatter_about(key_of[1], (D, (QH + 2 * KVH) * HD), D ** -0.5, 0.09375)
    owner_slot = draw_owner_slot(jax.random.fold_in(key_of[5], 71), 0)
    slab_sequence = draw_slab_sequence(jax.random.fold_in(key_of[5], 71), 0)
    slab_order = draw_slab_order(jax.random.fold_in(key_of[5], 71), 0)
    return dict(tokens=tokens, qkv_weight=qkv_weight, owner_slot=owner_slot, slab_sequence=slab_sequence, slab_order=slab_order)


ROPE_BASE = 500000.0
NEG_FILL = -1e30


def rotate(heads, positions):
    half_dim = heads.shape[-1] // 2
    frequency = ROPE_BASE ** (-jnp.arange(half_dim, dtype=jnp.float32) * 2.0 / heads.shape[-1])
    angles = positions.astype(jnp.float32)[:, None] * frequency[None, :]
    cosine = jnp.cos(angles)[:, None, :]
    sine_part = jnp.sin(angles)[:, None, :]
    first_half = heads[..., :half_dim]
    second_half = heads[..., half_dim:]
    return jnp.concatenate([first_half * cosine - second_half * sine_part, second_half * cosine + first_half * sine_part], axis=-1)


def project(input_rows, weight, positions):
    projected = jnp.dot(input_rows, weight, preferred_element_type=jnp.float32)
    count_rows = input_rows.shape[0]
    query = rotate(projected[:, :QH * HD].reshape(count_rows, QH, HD), positions).astype(jnp.bfloat16)
    key_heads = rotate(projected[:, QH * HD:(QH + KVH) * HD].reshape(count_rows, KVH, HD), positions).astype(jnp.bfloat16)
    value_heads = projected[:, (QH + KVH) * HD:].astype(jnp.bfloat16)
    key_value = jnp.concatenate([key_heads.reshape(count_rows, KVH * HD), value_heads], axis=1)
    return query.reshape(count_rows, QH * HD), key_value


def attend(query, key_value, query_pos, query_code, key_code):
    count_rows = query.shape[0]
    block_rows = min(512, count_rows)
    group_size = QH // KVH
    keys_f = key_value[:, :KVH * HD].reshape(-1, KVH, HD).astype(jnp.float32)
    values_f = key_value[:, KVH * HD:].reshape(-1, KVH, HD).astype(jnp.float32)

    def per_block(args):
        query_block, pos_block, code_block = args
        query_f = query_block.reshape(block_rows, KVH, group_size, HD).astype(jnp.float32)
        scores = jnp.einsum('tgjh,ngh->gjtn', query_f, keys_f) * (HD ** -0.5)
        allowed = (key_code[None, :] <= code_block[:, None]) & (key_code[None, :] >= (code_block - pos_block)[:, None])
        scores = jnp.where(allowed, scores, NEG_FILL)
        row_max = jnp.max(scores, axis=-1, keepdims=True)
        weights = jnp.where(allowed, jnp.exp(scores - row_max), 0.0)
        denom_sum = jnp.sum(weights, axis=-1)
        rounded = lax.optimization_barrier(weights.astype(jnp.bfloat16))
        weighted = jnp.einsum('gjtn,ngh->gjth', rounded.astype(jnp.float32), values_f)
        context = weighted / denom_sum[..., None]
        return context.transpose(2, 0, 1, 3).reshape(block_rows, QH * HD).astype(jnp.bfloat16)

    blocks = count_rows // block_rows
    result = lax.map(per_block, (query.reshape(blocks, block_rows, QH * HD), query_pos.reshape(blocks, block_rows), query_code.reshape(blocks, block_rows)))
    return result.reshape(count_rows, QH * HD)


def reference(tokens, qkv_weight, owner_slot, slab_sequence, slab_order):
    columns_count = ROW_SLABS // SLABS_DEV
    slabs = tokens.reshape(GROUPS, columns_count, SLABS_DEV, SLAB, D)
    targets = owner_slot.reshape(GROUPS, columns_count, SLABS_DEV)
    columns = jnp.broadcast_to(jnp.arange(columns_count, dtype=jnp.int32)[None, :, None], targets.shape)
    owner_rows = jnp.zeros_like(slabs).at[targets // SLABS_DEV, columns, targets % SLABS_DEV].set(slabs)
    owner_rows = owner_rows.reshape(GROUPS, ROW_TOK, D)
    offsets = jnp.arange(SLAB, dtype=jnp.int32)
    positions = (slab_order[:, :, None] * SLAB + offsets[None, None, :]).reshape(GROUPS, ROW_TOK)
    codes = (slab_sequence[:, :, None] * ROW_TOK).reshape(GROUPS, ROW_SLABS, 1) + positions.reshape(GROUPS, ROW_SLABS, SLAB)
    codes = codes.reshape(GROUPS, ROW_TOK).astype(jnp.int32)

    def per_row(args):
        input_rows, row_pos, row_code = args
        query, key_value = project(input_rows, qkv_weight, row_pos)
        return attend(query, key_value, row_pos, row_code, row_code)

    return lax.map(per_row, (owner_rows, positions, codes))
```

```python
import jax
import jax.numpy as jnp
from jax import lax
from jax.experimental import pallas as pl
from jax.experimental.pallas import tpu as pltpu
from jax.sharding import PartitionSpec as P

QH = 16
KVH = 4
HD = 128
SLAB = 128
GROUP = QH // KVH
ROPE_BASE = 500000.0
NEG_FILL = -1e30
AXES = ("dp", "cp")
SIDE = 4
KV_COLS = 2 * KVH * HD
Q_COLS = QH * HD


def pairs(move):
    out = []
    for x in range(SIDE):
        for z in range(SIDE):
            for y in range(SIDE):
                for c in range(2):
                    nx, nz, ny, nc = move(x, z, y, c)
                    here = x * 32 + (z * SIDE + y) * 2 + c
                    there = (nx % SIDE) * 32 + ((nz % SIDE) * SIDE + ny % SIDE) * 2 + nc % 2
                    out.append((here, there))
    return out


def shift_x(k):
    return pairs(lambda x, z, y, c: (x + k, z, y, c))


def shift_first(k):
    return pairs(lambda x, z, y, c: (x, z + k, y, c) if c == 0 else (x, z, y + k, c))


def shift_second(k):
    return pairs(lambda x, z, y, c: (x, z, y + k, c) if c == 0 else (x, z + k, y, c))


OTHER_CORE = pairs(lambda x, z, y, c: (x, z, y, c + 1))


def permute(value, table):
    return lax.ppermute(value, AXES, table)


def rope_tables(order, cos_ref, sin_ref):
    lane = lax.broadcasted_iota(jnp.int32, (SLAB, HD), 1)
    half = jnp.where(lane < HD // 2, lane, lane - HD // 2).astype(jnp.float32)
    frequency = jnp.exp(half * (-2.0 / HD * 13.122363377404328))
    row = lax.broadcasted_iota(jnp.int32, (SLAB, HD), 0)
    angle = (order * SLAB + row).astype(jnp.float32) * frequency
    cos_ref[...] = jnp.cos(angle)
    sine = jnp.sin(angle)
    sin_ref[...] = jnp.where(lane < HD // 2, -sine, sine)


def rope(block, cos_ref, sin_ref):
    return block * cos_ref[...] + pltpu.roll(block, HD // 2, 1) * sin_ref[...]


def store_masked(outs, owner, my_row, columns, value):
    for k, out in enumerate(outs):
        mine = owner == lax.rem(my_row + k, SIDE)

        @pl.when(mine)
        def _():
            out[:, columns] = value

        @pl.when(jnp.logical_not(mine))
        def _():
            out[:, columns] = jnp.zeros_like(value)


def kv_kernel(owner_ref, order_ref, x_ref, w_ref, o0, o1, o2, o3, cos_ref, sin_ref):
    step = pl.program_id(0)
    owner = owner_ref[0, 0]
    my_row = lax.axis_index("dp")

    @pl.when(step == 0)
    def _():
        rope_tables(order_ref[owner, lax.axis_index("cp")], cos_ref, sin_ref)

    projected = jnp.dot(x_ref[...], w_ref[...], preferred_element_type=jnp.float32)
    for h in range(2):
        columns = slice(h * HD, (h + 1) * HD)
        block = projected[:, columns]

        @pl.when(step < 2)
        def _():
            value = rope(block, cos_ref, sin_ref).astype(jnp.bfloat16)
            store_masked((o0, o1, o2, o3), owner, my_row, columns, value)

        @pl.when(step >= 2)
        def _():
            value = block.T.astype(jnp.bfloat16)
            store_masked((o0, o1, o2, o3), owner, my_row, columns, value)


def q_kernel(owner_ref, order_ref, x_ref, w_ref, o0, o1, o2, o3, cos_ref, sin_ref):
    owner = owner_ref[0, 0]
    my_row = lax.axis_index("dp")

    @pl.when(pl.program_id(0) == 0)
    def _():
        rope_tables(order_ref[owner, lax.axis_index("cp")], cos_ref, sin_ref)

    projected = jnp.dot(x_ref[...], w_ref[...], preferred_element_type=jnp.float32)
    for h in range(2):
        columns = slice(h * HD, (h + 1) * HD)
        value = rope(projected[:, columns], cos_ref, sin_ref).T.astype(jnp.bfloat16)
        store_masked((o0, o1, o2, o3), owner, my_row, columns, value)


def project(kernel, name, rows, weight, owner_slot, slab_order, first_block, blocks):
    depth = rows.shape[1]
    width = 2 * HD
    out = jax.ShapeDtypeStruct((SLAB, blocks * width), jnp.bfloat16)
    return pl.pallas_call(
        kernel,
        grid=(blocks,),
        in_specs=[
            pl.BlockSpec(memory_space=pltpu.SMEM),
            pl.BlockSpec(memory_space=pltpu.SMEM),
            pl.BlockSpec((SLAB, depth), lambda j: (0, 0)),
            pl.BlockSpec((depth, width), lambda j: (0, first_block + j)),
        ],
        out_specs=[pl.BlockSpec((SLAB, width), lambda j: (0, j))] * 4,
        out_shape=[out] * 4,
        scratch_shapes=[pltpu.VMEM((SLAB, HD), jnp.float32)] * 2,
        compiler_params=pltpu.CompilerParams(dimension_semantics=("arbitrary",)),
        cost_estimate=pl.CostEstimate(
            flops=2 * SLAB * depth * blocks * width,
            bytes_accessed=2 * depth * (SLAB + blocks * width),
            transcendentals=0,
        ),
        name=name,
    )(owner_slot, slab_order, rows, weight)


def attend_kernel(place_ref, order_ref, q_ref, *refs):
    pieces = refs[:16]
    out_ref, kv, sems, acc, peak, total = refs[16:]
    order = order_ref[0]
    factor = HD**-0.5 * 1.4426950408889634

    for s in range(32):
        place = place_ref[s]

        @pl.when(place >= 0)
        def _():
            pltpu.make_async_copy(
                pieces[s // 2].at[pl.ds((s % 2) * SLAB, SLAB)], kv.at[place], sems.at[place]
            ).start()

    def wait(i):
        pltpu.make_async_copy(pieces[0].at[pl.ds(0, SLAB)], kv.at[i], sems.at[i]).wait()

    wait(order)
    key_row = lax.broadcasted_iota(jnp.int32, (SLAB, GROUP * HD), 0)
    token = lax.rem(lax.broadcasted_iota(jnp.int32, (SLAB, GROUP * HD), 1), SLAB)
    for g in range(KVH):
        queries = q_ref[:, g * GROUP * HD : (g + 1) * GROUP * HD]
        scores = jnp.dot(
            kv[order, :, g * HD : (g + 1) * HD], queries, preferred_element_type=jnp.float32
        )
        scores = jnp.where(key_row <= token, scores, NEG_FILL)
        top = jnp.max(scores, axis=0, keepdims=True)
        weights = jnp.exp2((scores - top) * factor)
        peak[g] = top
        total[g] = jnp.sum(weights, axis=0, keepdims=True)
        acc[g] = jnp.dot(
            kv[order, :, (KVH + g) * HD : (KVH + g + 1) * HD],
            weights.astype(jnp.bfloat16),
            preferred_element_type=jnp.float32,
        )

    def body(i, carry):
        wait(i)
        for g in range(KVH):
            queries = q_ref[:, g * GROUP * HD : (g + 1) * GROUP * HD]
            scores = jnp.dot(
                kv[i, :, g * HD : (g + 1) * HD], queries, preferred_element_type=jnp.float32
            )
            old = peak[g]
            top = jnp.maximum(old, jnp.max(scores, axis=0, keepdims=True))
            weights = jnp.exp2((scores - top) * factor)
            rescale = jnp.exp2((old - top) * factor)
            peak[g] = top
            total[g] = total[g] * rescale + jnp.sum(weights, axis=0, keepdims=True)
            acc[g] = acc[g] * rescale + jnp.dot(
                kv[i, :, (KVH + g) * HD : (KVH + g + 1) * HD],
                weights.astype(jnp.bfloat16),
                preferred_element_type=jnp.float32,
            )
        return carry

    lax.fori_loop(0, order, body, 0)
    for g in range(KVH):
        context = acc[g] / total[g]
        for h in range(GROUP):
            head = g * GROUP + h
            out_ref[:, head * HD : (head + 1) * HD] = context[
                :, h * SLAB : (h + 1) * SLAB
            ].T.astype(jnp.bfloat16)


def attend(query, pieces, place, order):
    return pl.pallas_call(
        attend_kernel,
        in_specs=[
            pl.BlockSpec(memory_space=pltpu.SMEM),
            pl.BlockSpec(memory_space=pltpu.SMEM),
            pl.BlockSpec(memory_space=pltpu.VMEM),
        ]
        + [pl.BlockSpec(memory_space=pl.ANY)] * 16,
        out_specs=pl.BlockSpec(memory_space=pltpu.VMEM),
        out_shape=jax.ShapeDtypeStruct((SLAB, Q_COLS), jnp.bfloat16),
        scratch_shapes=[
            pltpu.VMEM((16, SLAB, KV_COLS), jnp.bfloat16),
            pltpu.SemaphoreType.DMA((16,)),
            pltpu.VMEM((KVH, HD, GROUP * SLAB), jnp.float32),
            pltpu.VMEM((KVH, 1, GROUP * SLAB), jnp.float32),
            pltpu.VMEM((KVH, 1, GROUP * SLAB), jnp.float32),
        ],
        cost_estimate=pl.CostEstimate(
            flops=4 * SLAB * 8 * SLAB * Q_COLS, bytes_accessed=4 << 20, transcendentals=0
        ),
        name="attend",
    )(place, order, query, *pieces)


def places(slab_sequence, slab_order):
    my_row = lax.axis_index("dp")
    column = lax.axis_index("cp")
    sequence = lax.dynamic_index_in_dim(slab_sequence, my_row, 0, keepdims=False)
    order = lax.dynamic_index_in_dim(slab_order, my_row, 0, keepdims=False)
    index = jnp.arange(32, dtype=jnp.int32)
    my_sequence = jnp.sum(jnp.where(index == column, sequence, 0))
    my_order = jnp.sum(jnp.where(index == column, order, 0))
    core = column % 2
    y, z = (column // 2) % SIDE, column // 8
    slots = []
    for partner in range(2):
        held = core if partner == 0 else 1 - core
        for first, second in (
            ((0, 1), 0), ((3, 2), 0), ((0, 1), 1), ((3, 2), 1),
            ((3, 2), 3), ((0, 1), 3), ((0, 1), 2), ((3, 2), 2),
        ):
            for k in first:
                slots.append((held, k, second, partner))
    found = []
    for held, k, second, partner in slots:
        sz = jnp.where(held == 0, z - k, z - second) % SIDE
        sy = jnp.where(held == 0, y - second, y - k) % SIDE
        found.append((sz * SIDE + sy) * 2 + held)
    source = jnp.stack(found)
    hit = source[:, None] == index[None, :]
    slot_sequence = jnp.sum(jnp.where(hit, sequence[None, :], 0), axis=1)
    slot_order = jnp.sum(jnp.where(hit, order[None, :], 0), axis=1)
    wanted = (slot_sequence == my_sequence) & (slot_order <= my_order)
    return jnp.where(wanted, slot_order, -1), my_order.reshape(1)


def local(tokens, qkv_weight, owner_slot, slab_sequence, slab_order):
    rows = tokens[0]
    place, order = places(slab_sequence, slab_order)
    kv = project(
        kv_kernel, "kv_proj", rows, qkv_weight, owner_slot, slab_order, QH // 2, KVH
    )
    queries = project(q_kernel, "q_proj", rows, qkv_weight, owner_slot, slab_order, 0, QH // 2)
    moved = [permute(kv[k], shift_x(k)) for k in (1, 3, 2)]
    own = kv[0] + moved[0] + moved[1] + moved[2]
    own, *queries = lax.optimization_barrier((own, *queries))
    first = [permute(own, shift_first(k)) for k in (1, 3, 2)]
    moved = [permute(queries[k], shift_x(k)) for k in (1, 3, 2)]
    query = queries[0] + moved[0] + moved[1] + moved[2]
    low = jnp.concatenate([own, first[0]], axis=0)
    high = jnp.concatenate([first[1], first[2]], axis=0)
    left = [permute(v, shift_second(1)) for v in (low, high)]
    right = [permute(v, shift_second(3)) for v in (high, low)]
    far = [permute(left[0], shift_second(1)), permute(right[0], shift_second(3))]
    pieces = [low, high, *left, *right, *far]
    pieces = pieces + [permute(v, OTHER_CORE) for v in pieces]
    return attend(query, pieces, place, order)[None]


def solution(mesh):
    in_specs = (P("dp", "cp", None), P(), P("dp", "cp"), P(), P())
    out_specs = P("dp", "cp", None)
    return jax.shard_map(local, mesh=mesh, in_specs=in_specs, out_specs=out_specs, check_vma=False)
```

```python
import functools

import jax
import jax.numpy as jnp
from jax import lax
from jax.experimental import pallas as pl
from jax.experimental.pallas import tpu as pltpu
from jax.sharding import PartitionSpec as P

QH = 16
KVH = 4
HD = 128
SLAB = 128
GROUP = QH // KVH
ROPE_BASE = 500000.0
NEG_FILL = -1e30
AXES = ("dp", "cp")
SIDE = 4
KV_COLS = 2 * KVH * HD
Q_COLS = QH * HD


def pairs(move):
    out = []
    for x in range(SIDE):
        for z in range(SIDE):
            for y in range(SIDE):
                for c in range(2):
                    nx, nz, ny, nc = move(x, z, y, c)
                    here = x * 32 + (z * SIDE + y) * 2 + c
                    there = (nx % SIDE) * 32 + ((nz % SIDE) * SIDE + ny % SIDE) * 2 + nc % 2
                    out.append((here, there))
    return out


def shift_x(k):
    return pairs(lambda x, z, y, c: (x + k, z, y, c))


def shift_first(k):
    return pairs(lambda x, z, y, c: (x, z + k, y, c) if c == 0 else (x, z, y + k, c))


def shift_second(k):
    return pairs(lambda x, z, y, c: (x, z, y + k, c) if c == 0 else (x, z + k, y, c))


OTHER_CORE = pairs(lambda x, z, y, c: (x, z, y, c + 1))


def permute(value, table):
    return lax.ppermute(value, AXES, table)


def rope_tables(order, slot, cos_ref, sin_ref):
    lane = lax.broadcasted_iota(jnp.int32, (SLAB, HD), 1)
    half = jnp.where(lane < HD // 2, lane, lane - HD // 2).astype(jnp.float32)
    frequency = jnp.exp(half * (-2.0 / HD * 13.122363377404328))
    row = lax.broadcasted_iota(jnp.int32, (SLAB, HD), 0)
    angle = (order * SLAB + row).astype(jnp.float32) * frequency
    cos_ref[slot] = jnp.cos(angle)
    sine = jnp.sin(angle)
    sin_ref[slot] = jnp.where(lane < HD // 2, -sine, sine)


def rope(block, slot, cos_ref, sin_ref):
    return block * cos_ref[slot] + pltpu.roll(block, HD // 2, 1) * sin_ref[slot]


def begin(core_ref, owner_ref, other_ref, order_ref, cos_ref, sin_ref):
    column = lax.axis_index("cp")
    core = core_ref[0]
    owners = (owner_ref[0, 0], other_ref[0, 0])
    columns = (column, column + 1 - 2 * core)

    @pl.when(pl.program_id(0) == 0)
    def _():
        for slot in range(2):
            rope_tables(order_ref[owners[slot], columns[slot]], slot, cos_ref, sin_ref)

    bases = (pl.multiple_of(core * SLAB, SLAB), pl.multiple_of((1 - core) * SLAB, SLAB))
    return owners, bases


def store_masked(outs, owner, base, columns, value):
    my_row = lax.axis_index("dp")
    for k, out in enumerate(outs):
        mine = owner == lax.rem(my_row + k, SIDE)
        out[pl.ds(base, SLAB), columns] = jnp.where(mine, value, jnp.zeros_like(value))


def kv_kernel(core_ref, owner_ref, other_ref, order_ref, x_ref, y_ref, w_ref, *refs):
    outs, (cos_ref, sin_ref) = refs[:4], refs[4:]
    owners, bases = begin(core_ref, owner_ref, other_ref, order_ref, cos_ref, sin_ref)
    both = jnp.concatenate([x_ref[...], y_ref[...]], axis=0)
    projected = jnp.dot(both, w_ref[...], preferred_element_type=jnp.float32)
    step = pl.program_id(0)

    @pl.when(step == 0)
    def _():
        for slot in range(2):
            for h in range(2):
                columns = slice(h * HD, (h + 1) * HD)
                block = projected[slot * SLAB : (slot + 1) * SLAB, columns]
                value = rope(block, slot, cos_ref, sin_ref).astype(jnp.bfloat16)
                store_masked(outs, owners[slot], bases[slot], columns, value)

    @pl.when(step == 1)
    def _():
        for slot in range(2):
            for h in range(2):
                columns = slice(h * HD, (h + 1) * HD)
                block = projected[slot * SLAB : (slot + 1) * SLAB, columns]
                value = block.T.astype(jnp.bfloat16)
                store_masked(outs, owners[slot], bases[slot], columns, value)


def q_kernel(core_ref, owner_ref, other_ref, order_ref, x_ref, y_ref, w_ref, *refs):
    outs, (cos_ref, sin_ref) = refs[:4], refs[4:]
    owners, bases = begin(core_ref, owner_ref, other_ref, order_ref, cos_ref, sin_ref)
    both = jnp.concatenate([x_ref[...], y_ref[...]], axis=0)
    projected = jnp.dot(both, w_ref[...], preferred_element_type=jnp.float32)
    for slot in range(2):
        for h in range(w_ref.shape[1] // HD):
            columns = slice(h * HD, (h + 1) * HD)
            block = projected[slot * SLAB : (slot + 1) * SLAB, columns]
            value = rope(block, slot, cos_ref, sin_ref).T.astype(jnp.bfloat16)
            store_masked(outs, owners[slot], bases[slot], columns, value)


def project(kernel, name, core, owners, slab_order, rows, others, weight, block, blocks, width):
    depth = rows.shape[1]
    out = jax.ShapeDtypeStruct((2 * SLAB, blocks * width), jnp.bfloat16)
    return pl.pallas_call(
        kernel,
        grid_spec=pltpu.PrefetchScalarGridSpec(
            num_scalar_prefetch=1,
            grid=(blocks,),
            in_specs=[
                pl.BlockSpec(memory_space=pltpu.SMEM),
                pl.BlockSpec(memory_space=pltpu.SMEM),
                pl.BlockSpec(memory_space=pltpu.SMEM),
                pl.BlockSpec((SLAB, depth), lambda j, c: (0, 0)),
                pl.BlockSpec((SLAB, depth), lambda j, c: (0, 0)),
                pl.BlockSpec((depth, width), lambda j, c: (0, block(j, c[0]))),
            ],
            out_specs=[pl.BlockSpec((2 * SLAB, width), lambda j, c: (0, j))] * 4,
            scratch_shapes=[pltpu.VMEM((2, SLAB, HD), jnp.float32)] * 2,
        ),
        out_shape=[out] * 4,
        compiler_params=pltpu.CompilerParams(dimension_semantics=("arbitrary",)),
        cost_estimate=pl.CostEstimate(
            flops=4 * SLAB * depth * blocks * width,
            bytes_accessed=2 * depth * (2 * SLAB + blocks * width),
            transcendentals=0,
        ),
        name=name,
    )(core, *owners, slab_order, rows, others, weight)


FACTOR = HD**-0.5 * 1.4426950408889634
WIDE = GROUP * SLAB
LOW, HIGH = (0, 1), (3, 2)
LOCAL = ((LOW, 0), (HIGH, 0))
NEAR = ((LOW, 1), (HIGH, 1), (HIGH, 3), (LOW, 3))
FAR = ((LOW, 2), (HIGH, 2))


def attend_kernel(spots, first, last, sequence_ref, order_ref, q_ref, *refs):
    pieces, refs = refs[: len(spots)], refs[len(spots) :]
    if not first:
        old, refs = refs[:3], refs[3:]
    outs, refs = (refs[:2], refs[2:]) if last else (refs[:3], refs[3:])
    if last:
        acc, peak, total = refs[:3]
        refs = refs[3:]
    else:
        acc, peak, total = outs
    kv, scores_ref, lists = refs
    row = lax.axis_index("dp")
    column = lax.axis_index("cp")
    core, y, z = lax.rem(column, 2), lax.rem(column // 2, SIDE), column // (2 * SIDE)
    mine = [column + 1 - 2 * core, column]
    sequences = [sequence_ref[row, m] for m in mine]
    orders = [order_ref[row, m] for m in mine]
    counts = [0, 0]
    for a, (chips, second) in enumerate(spots):
        for b, k in enumerate(chips):
            sz = lax.rem(z + 2 * SIDE - jnp.where(core == 0, k, second), SIDE)
            sy = lax.rem(y + 2 * SIDE - jnp.where(core == 0, second, k), SIDE)
            for c in range(2):
                slot = a * 4 + b * 2 + c
                source = (sz * SIDE + sy) * 2 + c
                sequence, order = sequence_ref[row, source], order_ref[row, source]
                needed = False
                for t in range(2):
                    wanted = (sequence == sequences[t]) & (order < orders[t])
                    lists[t, counts[t]] = slot
                    counts[t] = counts[t] + wanted.astype(jnp.int32)
                    needed = needed | wanted | (source == mine[t])

                @pl.when(needed)
                def _():
                    kv[slot] = pieces[a][(b * 2 + c) * SLAB : (b * 2 + c + 1) * SLAB, :]

    for t in range(2):
        slab = core if t == 1 else 1 - core
        base = pl.multiple_of(slab * SLAB, SLAB)
        count = counts[t]
        pairs_here = (count + 1) // 2
        queries = [q_ref[pl.ds(base, SLAB), g * WIDE : (g + 1) * WIDE] for g in range(2)]
        starts = []
        for g in range(2):
            u = t * 2 + g
            if first:
                key_row = lax.broadcasted_iota(jnp.int32, (SLAB, WIDE), 0)
                token = lax.rem(lax.broadcasted_iota(jnp.int32, (SLAB, WIDE), 1), SLAB)
                scores = jnp.dot(
                    kv[slab, :, g * HD : (g + 1) * HD], queries[g], preferred_element_type=jnp.float32
                )
                scores = jnp.where(key_row <= token, scores, NEG_FILL)
                scores_ref[8, g, :SLAB] = scores
                peak[u] = jnp.max(scores.reshape(SLAB // 8, 8, WIDE), axis=0)
            else:
                peak[u] = old[1][u]
                starts.append(jnp.max(old[1][u], axis=0, keepdims=True))

        def picked(p):
            one = lists[t, 2 * p]
            two = lists[t, jnp.minimum(2 * p + 1, count - 1)]
            return one, two

        def score(p, carry):
            one, two = picked(p)
            full = 2 * p + 1 < count
            for g in range(2):
                u = t * 2 + g
                keys = slice(g * HD, (g + 1) * HD)
                both = jnp.concatenate([kv[one, :, keys], kv[two, :, keys]], axis=0)
                q = q_ref[pl.ds(base, SLAB), g * WIDE : (g + 1) * WIDE]
                scores = jnp.dot(both, q, preferred_element_type=jnp.float32)
                low = scores[:SLAB]
                high = jnp.where(full, scores[SLAB:], NEG_FILL)
                scores_ref[p, g, :SLAB] = low
                scores_ref[p, g, SLAB:] = high
                top = jnp.maximum(low, high).reshape(SLAB // 8, 8, WIDE)
                peak[u] = jnp.maximum(peak[u], jnp.max(top, axis=0))
            return carry

        lax.fori_loop(0, pairs_here, score, 0)
        tops = []
        for g in range(2):
            u = t * 2 + g
            top = jnp.max(peak[u], axis=0, keepdims=True)
            tops.append(top * FACTOR)
            if first:
                weights = jnp.exp2(scores_ref[8, g, :SLAB] * FACTOR - tops[g])
                total[u] = jnp.sum(weights.reshape(SLAB // 8, 8, WIDE), axis=0)
                acc[u] = jnp.dot(
                    kv[slab, :, (2 + g) * HD : (3 + g) * HD],
                    weights.astype(jnp.bfloat16),
                    preferred_element_type=jnp.float32,
                )
            else:
                rescale = jnp.exp2((starts[g] - top) * FACTOR)
                total[u] = old[2][u] * rescale
                acc[u] = old[0][u] * rescale

        def weigh(p, carry):
            one, two = picked(p)
            for g in range(2):
                u = t * 2 + g
                values = slice((2 + g) * HD, (3 + g) * HD)
                weights = jnp.exp2(scores_ref[p, g] * FACTOR - tops[g])
                total[u] = total[u] + jnp.sum(weights.reshape(SLAB // 4, 8, WIDE), axis=0)
                both = jnp.concatenate([kv[one, :, values], kv[two, :, values]], axis=1)
                acc[u] = acc[u] + jnp.dot(
                    both, weights.astype(jnp.bfloat16), preferred_element_type=jnp.float32
                )
            return carry

        lax.fori_loop(0, pairs_here, weigh, 0)
        if last:
            for g in range(2):
                u = t * 2 + g
                context = acc[u] / jnp.sum(total[u], axis=0, keepdims=True)
                for h in range(GROUP):
                    head = g * GROUP + h
                    outs[t][:, head * HD : (head + 1) * HD] = context[
                        :, h * SLAB : (h + 1) * SLAB
                    ].T.astype(jnp.bfloat16)


STATE = ((4, HD, WIDE), (4, 8, WIDE), (4, 8, WIDE))


def attend(spots, slab_sequence, slab_order, query, pieces, state, last, name):
    first = state is None
    vmem = pl.BlockSpec(memory_space=pltpu.VMEM)
    smem = pl.BlockSpec(memory_space=pltpu.SMEM)
    scratch = [
        pltpu.VMEM((4 * len(spots), SLAB, 4 * HD), jnp.bfloat16),
        pltpu.VMEM((9, 2, 2 * SLAB, WIDE), jnp.float32),
        pltpu.SMEM((2, 4 * len(spots) + 1), jnp.int32),
    ]
    if last:
        out_shape = [jax.ShapeDtypeStruct((SLAB, Q_COLS // 2), jnp.bfloat16)] * 2
        scratch = [pltpu.VMEM(s, jnp.float32) for s in STATE] + scratch
    else:
        out_shape = [jax.ShapeDtypeStruct(s, jnp.float32) for s in STATE]
    operands = [slab_sequence, slab_order, query, *pieces, *(state or ())]
    return pl.pallas_call(
        functools.partial(attend_kernel, spots, first, last),
        in_specs=[smem, smem] + [vmem] * (len(operands) - 2),
        out_specs=[vmem] * len(out_shape),
        out_shape=out_shape,
        scratch_shapes=scratch,
        cost_estimate=pl.CostEstimate(
            flops=4 * SLAB * len(spots) * 4 * SLAB * Q_COLS // 2,
            bytes_accessed=2 << 20,
            transcendentals=0,
        ),
        name=name,
    )(*operands)


def local(tokens, qkv_weight, owner_slot, slab_sequence, slab_order):
    rows = tokens[0]
    core = lax.rem(lax.axis_index("cp"), 2)
    others = permute(rows, OTHER_CORE)
    owners = (owner_slot, permute(owner_slot, OTHER_CORE))
    common = (core.reshape(1), owners, slab_order, rows, others, qkv_weight)
    kv = project(kv_kernel, "kv_proj", *common, lambda j, c: QH // 2 + 2 * j + c, 2, 2 * HD)
    queries = project(q_kernel, "q_proj", *common, lambda j, c: 2 * c + j, 2, 4 * HD)
    moved = [permute(kv[k], shift_x(k)) for k in (1, 3, 2)]
    own = kv[0] + moved[0] + moved[1] + moved[2]
    own, *queries = lax.optimization_barrier((own, *queries))
    first = [permute(own, shift_first(k)) for k in (1, 3, 2)]
    moved = [permute(queries[k], shift_x(k)) for k in (1, 3, 2)]
    query = queries[0] + moved[0] + moved[1] + moved[2]
    low = jnp.concatenate([own, first[0]], axis=0)
    high = jnp.concatenate([first[1], first[2]], axis=0)
    left = [permute(v, shift_second(1)) for v in (low, high)]
    right = [permute(v, shift_second(3)) for v in (high, low)]
    far = [permute(left[0], shift_second(1)), permute(right[0], shift_second(3))]
    tables = (slab_sequence, slab_order, query)
    pieces = [low, high, *left, *right, *far]
    sent, kept = attend(LOCAL + NEAR + FAR, *tables, pieces, None, True, "attend")
    received = permute(sent, OTHER_CORE)
    swap = core == 0
    context = jnp.concatenate(
        [jnp.where(swap, kept, received), jnp.where(swap, received, kept)], axis=1
    )
    return context[None]


def solution(mesh):
    in_specs = (P("dp", "cp", None), P(), P("dp", "cp"), P(), P())
    out_specs = P("dp", "cp", None)
    return jax.shard_map(local, mesh=mesh, in_specs=in_specs, out_specs=out_specs, check_vma=False)
```

```python
import functools

import jax
import jax.numpy as jnp
from jax import lax
from jax.experimental import pallas as pl
from jax.experimental.pallas import tpu as pltpu
from jax.sharding import PartitionSpec as P


QH = 16
KVH = 4
HD = 128
SLAB = 128
GROUP = QH // KVH
NEG_FILL = -1e30
AXES = ("dp", "cp")
SIDE = 4
Q_COLS = QH * HD


def pairs(move):
    out = []
    for x in range(SIDE):
        for z in range(SIDE):
            for y in range(SIDE):
                for c in range(2):
                    nx, nz, ny, nc = move(x, z, y, c)
                    here = x * 32 + (z * SIDE + y) * 2 + c
                    there = (nx % SIDE) * 32 + ((nz % SIDE) * SIDE + ny % SIDE) * 2 + nc % 2
                    out.append((here, there))
    return out


def shift_x(k):
    return pairs(lambda x, z, y, c: (x + k, z, y, c))


def shift_first(k):
    return pairs(lambda x, z, y, c: (x, z + k, y, c) if c == 0 else (x, z, y + k, c))


def shift_second(k):
    return pairs(lambda x, z, y, c: (x, z, y + k, c) if c == 0 else (x, z + k, y, c))


OTHER_CORE = pairs(lambda x, z, y, c: (x, z, y, c + 1))


def permute(value, table):
    return lax.ppermute(value, AXES, table)


def rope_tables(order, slot, cos_ref, sin_ref):
    lane = lax.broadcasted_iota(jnp.int32, (SLAB, HD), 1)
    half = jnp.where(lane < HD // 2, lane, lane - HD // 2).astype(jnp.float32)
    frequency = jnp.exp(half * (-2.0 / HD * 13.122363377404328))
    row = lax.broadcasted_iota(jnp.int32, (SLAB, HD), 0)
    angle = (order * SLAB + row).astype(jnp.float32) * frequency
    cos_ref[slot] = jnp.cos(angle)
    sine = jnp.sin(angle)
    sin_ref[slot] = jnp.where(lane < HD // 2, -sine, sine)


def rope(block, slot, cos_ref, sin_ref):
    return block * cos_ref[slot] + pltpu.roll(block, HD // 2, 1) * sin_ref[slot]


def begin(core_ref, owner_ref, other_ref, order_ref, cos_ref, sin_ref):
    column = lax.axis_index("cp")
    core = core_ref[0]
    owners = (owner_ref[0, 0], other_ref[0, 0])
    columns = (column, column + 1 - 2 * core)

    @pl.when(pl.program_id(0) == 0)
    def _():
        for slot in range(2):
            rope_tables(order_ref[owners[slot], columns[slot]], slot, cos_ref, sin_ref)

    bases = (pl.multiple_of(core * SLAB, SLAB), pl.multiple_of((1 - core) * SLAB, SLAB))
    return owners, bases


def store_masked(outs, owner, base, columns, value):
    my_row = lax.axis_index("dp")
    for k, out in enumerate(outs):
        mine = owner == lax.rem(my_row + k, SIDE)
        out[pl.ds(base, SLAB), columns] = jnp.where(mine, value, jnp.zeros_like(value))


def kv_kernel(core_ref, owner_ref, other_ref, order_ref, x_ref, y_ref, w_ref, *refs):
    outs, (cos_ref, sin_ref) = refs[:4], refs[4:]
    owners, bases = begin(core_ref, owner_ref, other_ref, order_ref, cos_ref, sin_ref)
    both = jnp.concatenate([x_ref[...], y_ref[...]], axis=0)
    projected = jnp.dot(both, w_ref[...], preferred_element_type=jnp.float32)
    step = pl.program_id(0)

    @pl.when(step == 0)
    def _():
        for slot in range(2):
            for h in range(2):
                columns = slice(h * HD, (h + 1) * HD)
                block = projected[slot * SLAB : (slot + 1) * SLAB, columns]
                value = rope(block, slot, cos_ref, sin_ref).astype(jnp.bfloat16)
                store_masked(outs, owners[slot], bases[slot], columns, value)

    @pl.when(step == 1)
    def _():
        for slot in range(2):
            for h in range(2):
                columns = slice(h * HD, (h + 1) * HD)
                block = projected[slot * SLAB : (slot + 1) * SLAB, columns]
                value = block.T.astype(jnp.bfloat16)
                store_masked(outs, owners[slot], bases[slot], columns, value)


def q_kernel(core_ref, owner_ref, other_ref, order_ref, x_ref, y_ref, w_ref, *refs):
    outs, (cos_ref, sin_ref) = refs[:4], refs[4:]
    owners, bases = begin(core_ref, owner_ref, other_ref, order_ref, cos_ref, sin_ref)
    both = jnp.concatenate([x_ref[...], y_ref[...]], axis=0)
    projected = jnp.dot(both, w_ref[...], preferred_element_type=jnp.float32)
    for slot in range(2):
        for h in range(w_ref.shape[1] // HD):
            columns = slice(h * HD, (h + 1) * HD)
            block = projected[slot * SLAB : (slot + 1) * SLAB, columns]
            value = rope(block, slot, cos_ref, sin_ref).T.astype(jnp.bfloat16)
            store_masked(outs, owners[slot], bases[slot], columns, value)


def project(kernel, core, owners, slab_order, rows, others, weight, block, blocks, width):
    depth = rows.shape[1]
    out = jax.ShapeDtypeStruct((2 * SLAB, blocks * width), jnp.bfloat16)
    return pl.pallas_call(
        kernel,
        grid_spec=pltpu.PrefetchScalarGridSpec(
            num_scalar_prefetch=1,
            grid=(blocks,),
            in_specs=[
                pl.BlockSpec(memory_space=pltpu.SMEM),
                pl.BlockSpec(memory_space=pltpu.SMEM),
                pl.BlockSpec(memory_space=pltpu.SMEM),
                pl.BlockSpec((SLAB, depth), lambda j, c: (0, 0)),
                pl.BlockSpec((SLAB, depth), lambda j, c: (0, 0)),
                pl.BlockSpec((depth, width), lambda j, c: (0, block(j, c[0]))),
            ],
            out_specs=[pl.BlockSpec((2 * SLAB, width), lambda j, c: (0, j))] * 4,
            scratch_shapes=[pltpu.VMEM((2, SLAB, HD), jnp.float32)] * 2,
        ),
        out_shape=[out] * 4,
        compiler_params=pltpu.CompilerParams(dimension_semantics=("arbitrary",)),
        cost_estimate=pl.CostEstimate(
            flops=4 * SLAB * depth * blocks * width,
            bytes_accessed=2 * depth * (2 * SLAB + blocks * width),
            transcendentals=0,
        ),
    )(core, *owners, slab_order, rows, others, weight)


FACTOR = HD**-0.5 * 1.4426950408889634
WIDE = GROUP * SLAB
LOW, HIGH = (0, 1), (3, 2)
LOCAL = ((LOW, 0), (HIGH, 0))
NEAR = ((LOW, 1), (HIGH, 1), (HIGH, 3), (LOW, 3))
FAR = ((LOW, 2), (HIGH, 2))


def attend_kernel(spots, slabs, first, last, sequence_ref, order_ref, q_ref, *refs):
    pieces, refs = refs[: len(spots)], refs[len(spots) :]
    if not first:
        old, refs = refs[:3], refs[3:]
    outs, refs = (refs[: len(slabs)], refs[len(slabs) :]) if last else (refs[:3], refs[3:])
    if last:
        acc, peak, total = refs[:3]
        refs = refs[3:]
    else:
        acc, peak, total = outs
    kv, scores_ref, lists = refs
    row = lax.axis_index("dp")
    column = lax.axis_index("cp")
    core, y, z = lax.rem(column, 2), lax.rem(column // 2, SIDE), column // (2 * SIDE)
    mine = [column + 1 - 2 * core, column]
    sequences = [sequence_ref[row, m] for m in mine]
    orders = [order_ref[row, m] for m in mine]
    counts = [0, 0]
    for a, (chips, second) in enumerate(spots):
        for b, k in enumerate(chips):
            sz = lax.rem(z + 2 * SIDE - jnp.where(core == 0, k, second), SIDE)
            sy = lax.rem(y + 2 * SIDE - jnp.where(core == 0, second, k), SIDE)
            for c in range(2):
                slot = a * 4 + b * 2 + c
                source = (sz * SIDE + sy) * 2 + c
                sequence, order = sequence_ref[row, source], order_ref[row, source]
                needed = False
                for t in slabs:
                    wanted = (sequence == sequences[t]) & (order < orders[t])
                    lists[t, counts[t]] = slot
                    counts[t] = counts[t] + wanted.astype(jnp.int32)
                    needed = needed | wanted | (source == mine[t])

                @pl.when(needed)
                def _():
                    kv[slot] = pieces[a][(b * 2 + c) * SLAB : (b * 2 + c + 1) * SLAB, :]

    for t in slabs:
        slab = core if t == 1 else 1 - core
        base = pl.multiple_of(slab * SLAB, SLAB)
        count = counts[t]
        pairs_here = (count + 1) // 2
        queries = [q_ref[pl.ds(base, SLAB), g * WIDE : (g + 1) * WIDE] for g in range(2)]
        starts = []
        for g in range(2):
            u = t * 2 + g
            if first:
                key_row = lax.broadcasted_iota(jnp.int32, (SLAB, WIDE), 0)
                token = lax.rem(lax.broadcasted_iota(jnp.int32, (SLAB, WIDE), 1), SLAB)
                scores = jnp.dot(
                    kv[slab, :, g * HD : (g + 1) * HD], queries[g], preferred_element_type=jnp.float32
                )
                scores = jnp.where(key_row <= token, scores, NEG_FILL)
                scores_ref[8, g, :SLAB] = scores
                peak[u] = jnp.max(scores.reshape(SLAB // 8, 8, WIDE), axis=0)
            else:
                peak[u] = old[1][u]
                starts.append(jnp.max(old[1][u], axis=0, keepdims=True))

        def picked(p):
            one = lists[t, 2 * p]
            two = lists[t, jnp.minimum(2 * p + 1, count - 1)]
            return one, two

        def score(p, carry):
            one, two = picked(p)
            full = 2 * p + 1 < count
            for g in range(2):
                u = t * 2 + g
                keys = slice(g * HD, (g + 1) * HD)
                both = jnp.concatenate([kv[one, :, keys], kv[two, :, keys]], axis=0)
                q = q_ref[pl.ds(base, SLAB), g * WIDE : (g + 1) * WIDE]
                scores = jnp.dot(both, q, preferred_element_type=jnp.float32)
                low = scores[:SLAB]
                high = jnp.where(full, scores[SLAB:], NEG_FILL)
                scores_ref[p, g, :SLAB] = low
                scores_ref[p, g, SLAB:] = high
                top = jnp.maximum(low, high).reshape(SLAB // 8, 8, WIDE)
                peak[u] = jnp.maximum(peak[u], jnp.max(top, axis=0))
            return carry

        lax.fori_loop(0, pairs_here, score, 0)
        tops = []
        for g in range(2):
            u = t * 2 + g
            top = jnp.max(peak[u], axis=0, keepdims=True)
            tops.append(top * FACTOR)
            if first:
                weights = jnp.exp2(scores_ref[8, g, :SLAB] * FACTOR - tops[g])
                total[u] = jnp.sum(weights.reshape(SLAB // 8, 8, WIDE), axis=0)
                acc[u] = jnp.dot(
                    kv[slab, :, (2 + g) * HD : (3 + g) * HD],
                    weights.astype(jnp.bfloat16),
                    preferred_element_type=jnp.float32,
                )
            else:
                rescale = jnp.exp2((starts[g] - top) * FACTOR)
                total[u] = old[2][u] * rescale
                acc[u] = old[0][u] * rescale

        def weigh(p, carry):
            one, two = picked(p)
            for g in range(2):
                u = t * 2 + g
                values = slice((2 + g) * HD, (3 + g) * HD)
                weights = jnp.exp2(scores_ref[p, g] * FACTOR - tops[g])
                total[u] = total[u] + jnp.sum(weights.reshape(SLAB // 4, 8, WIDE), axis=0)
                both = jnp.concatenate([kv[one, :, values], kv[two, :, values]], axis=1)
                acc[u] = acc[u] + jnp.dot(
                    both, weights.astype(jnp.bfloat16), preferred_element_type=jnp.float32
                )
            return carry

        lax.fori_loop(0, pairs_here, weigh, 0)
        if last:
            for g in range(2):
                u = t * 2 + g
                context = acc[u] / jnp.sum(total[u], axis=0, keepdims=True)
                for h in range(GROUP):
                    head = g * GROUP + h
                    outs[slabs.index(t)][:, head * HD : (head + 1) * HD] = context[
                        :, h * SLAB : (h + 1) * SLAB
                    ].T.astype(jnp.bfloat16)


STATE = ((4, HD, WIDE), (4, 8, WIDE), (4, 8, WIDE))


def attend(spots, slabs, slab_sequence, slab_order, query, pieces, state, last):
    first = state is None
    vmem = pl.BlockSpec(memory_space=pltpu.VMEM)
    smem = pl.BlockSpec(memory_space=pltpu.SMEM)
    scratch = [
        pltpu.VMEM((4 * len(spots), SLAB, 4 * HD), jnp.bfloat16),
        pltpu.VMEM((9, 2, 2 * SLAB, WIDE), jnp.float32),
        pltpu.SMEM((2, 4 * len(spots) + 1), jnp.int32),
    ]
    if last:
        out_shape = [jax.ShapeDtypeStruct((SLAB, Q_COLS // 2), jnp.bfloat16)] * len(slabs)
        scratch = [pltpu.VMEM(s, jnp.float32) for s in STATE] + scratch
    else:
        out_shape = [jax.ShapeDtypeStruct(s, jnp.float32) for s in STATE]
    operands = [slab_sequence, slab_order, query, *pieces, *(state or ())]
    return pl.pallas_call(
        functools.partial(attend_kernel, spots, slabs, first, last),
        in_specs=[smem, smem] + [vmem] * (len(operands) - 2),
        out_specs=[vmem] * len(out_shape),
        out_shape=out_shape,
        scratch_shapes=scratch,
        cost_estimate=pl.CostEstimate(
            flops=4 * SLAB * len(spots) * 4 * SLAB * Q_COLS // 2,
            bytes_accessed=2 << 20,
            transcendentals=0,
        ),
    )(*operands)


def local(tokens, qkv_weight, owner_slot, slab_sequence, slab_order):
    rows = tokens[0]
    core = lax.rem(lax.axis_index("cp"), 2)
    others = permute(rows, OTHER_CORE)
    owners = (owner_slot, permute(owner_slot, OTHER_CORE))
    common = (core.reshape(1), owners, slab_order, rows, others, qkv_weight)
    kv = project(kv_kernel, *common, lambda j, c: QH // 2 + 2 * j + c, 2, 2 * HD)
    queries = project(q_kernel, *common, lambda j, c: 2 * c + j, 2, 4 * HD)
    moved = [permute(kv[k], shift_x(k)) for k in (1, 3, 2)]
    own = kv[0] + moved[0] + moved[1] + moved[2]
    own, *queries = lax.optimization_barrier((own, *queries))
    first = [permute(own, shift_first(k)) for k in (1, 3, 2)]
    moved = [permute(queries[k], shift_x(k)) for k in (1, 3, 2)]
    query = queries[0] + moved[0] + moved[1] + moved[2]
    low = jnp.concatenate([own, first[0]], axis=0)
    high = jnp.concatenate([first[1], first[2]], axis=0)
    left = [permute(v, shift_second(1)) for v in (low, high)]
    right = [permute(v, shift_second(3)) for v in (high, low)]
    far = [permute(left[0], shift_second(1)), permute(right[0], shift_second(3))]
    tables = (slab_sequence, slab_order, query)
    near = [low, high, *left, *right]
    state = attend(LOCAL + NEAR, (0, 1), *tables, near, None, False)
    (sent,) = attend(FAR, (0,), *tables, far, state, True)
    received = permute(sent, OTHER_CORE)
    (kept,) = attend(FAR, (1,), *tables, far, state, True)
    return join(core.reshape(1), kept, received)[None]


def join_kernel(core_ref, kept_ref, received_ref, out_ref):
    half = Q_COLS // 2
    core = core_ref[0]
    out_ref[:, pl.ds(pl.multiple_of(core * half, half), half)] = kept_ref[...]
    out_ref[:, pl.ds(pl.multiple_of((1 - core) * half, half), half)] = received_ref[...]


def join(core, kept, received):
    vmem = pl.BlockSpec(memory_space=pltpu.VMEM)
    return pl.pallas_call(
        join_kernel,
        in_specs=[pl.BlockSpec(memory_space=pltpu.SMEM), vmem, vmem],
        out_specs=vmem,
        out_shape=jax.ShapeDtypeStruct((SLAB, Q_COLS), jnp.bfloat16),
        cost_estimate=pl.CostEstimate(flops=SLAB * Q_COLS, bytes_accessed=1 << 20, transcendentals=0),
        name="join",
    )(core, kept, received)


def solution(mesh):
    in_specs = (P("dp", "cp", None), P(), P("dp", "cp"), P(), P())
    out_specs = P("dp", "cp", None)
    return jax.shard_map(local, mesh=mesh, in_specs=in_specs, out_specs=out_specs, check_vma=False)
```

```python
import functools

import jax
import jax.numpy as jnp
from jax import lax
from jax.experimental import pallas as pl
from jax.experimental.pallas import tpu as pltpu
from jax.sharding import PartitionSpec as P


QH = 16
KVH = 4
HD = 128
SLAB = 128
GROUP = QH // KVH
NEG_FILL = -1e30
AXES = ("dp", "cp")
SIDE = 4
Q_COLS = QH * HD


def pairs(move):
    out = []
    for x in range(SIDE):
        for z in range(SIDE):
            for y in range(SIDE):
                for c in range(2):
                    nx, nz, ny, nc = move(x, z, y, c)
                    here = x * 32 + (z * SIDE + y) * 2 + c
                    there = (nx % SIDE) * 32 + ((nz % SIDE) * SIDE + ny % SIDE) * 2 + nc % 2
                    out.append((here, there))
    return out


def shift_x(k):
    return pairs(lambda x, z, y, c: (x + k, z, y, c))


def shift_first(k):
    return pairs(lambda x, z, y, c: (x, z + k, y, c) if c == 0 else (x, z, y + k, c))


def shift_second(k):
    return pairs(lambda x, z, y, c: (x, z, y + k, c) if c == 0 else (x, z + k, y, c))


OTHER_CORE = pairs(lambda x, z, y, c: (x, z, y, c + 1))


def permute(value, table):
    return lax.ppermute(value, AXES, table)


def rope_tables(order, slot, cos_ref, sin_ref):
    lane = lax.broadcasted_iota(jnp.int32, (SLAB, HD), 1)
    half = jnp.where(lane < HD // 2, lane, lane - HD // 2).astype(jnp.float32)
    frequency = jnp.exp(half * (-2.0 / HD * 13.122363377404328))
    row = lax.broadcasted_iota(jnp.int32, (SLAB, HD), 0)
    angle = (order * SLAB + row).astype(jnp.float32) * frequency
    cos_ref[slot] = jnp.cos(angle)
    sine = jnp.sin(angle)
    sin_ref[slot] = jnp.where(lane < HD // 2, -sine, sine)


def rope(block, slot, cos_ref, sin_ref):
    return block * cos_ref[slot] + pltpu.roll(block, HD // 2, 1) * sin_ref[slot]


def begin(core_ref, other_ref, owner_ref, order_ref, cos_ref, sin_ref):
    column = lax.axis_index("cp")
    owners = (other_ref[0, 0], owner_ref[0, 0])
    columns = (column + 1 - 2 * core_ref[0], column)

    @pl.when(pl.program_id(0) == 0)
    def _():
        for slot in range(2):
            rope_tables(order_ref[owners[slot], columns[slot]], slot, cos_ref, sin_ref)

    return owners


def store_masked(outs, owner, rows, columns, value):
    my_row = lax.axis_index("dp")
    for k, out in enumerate(outs):
        mine = owner == lax.rem(my_row + k, SIDE)
        out[rows, columns] = jnp.where(mine, value, jnp.zeros_like(value))


def kv_kernel(core_ref, other_ref, owner_ref, order_ref, y_ref, x_ref, w_ref, *refs):
    outs, (cos_ref, sin_ref) = refs[:4], refs[4:]
    owners = begin(core_ref, other_ref, owner_ref, order_ref, cos_ref, sin_ref)
    both = jnp.concatenate([y_ref[...], x_ref[...]], axis=0)
    projected = jnp.dot(both, w_ref[...], preferred_element_type=jnp.float32)
    heads = w_ref.shape[1] // HD
    step = pl.program_id(0)

    @pl.when(step < 2 // heads)
    def _():
        for slot in range(2):
            rows = slice(slot * SLAB, (slot + 1) * SLAB)
            for h in range(heads):
                columns = slice(h * HD, (h + 1) * HD)
                value = rope(projected[rows, columns], slot, cos_ref, sin_ref).astype(jnp.bfloat16)
                store_masked(outs, owners[slot], rows, columns, value)

    @pl.when(step >= 2 // heads)
    def _():
        for slot in range(2):
            rows = slice(slot * SLAB, (slot + 1) * SLAB)
            for h in range(heads):
                columns = slice(h * HD, (h + 1) * HD)
                value = projected[rows, columns].T.astype(jnp.bfloat16)
                store_masked(outs, owners[slot], rows, columns, value)


def q_kernel(core_ref, other_ref, owner_ref, order_ref, y_ref, x_ref, w_ref, *refs):
    outs, (cos_ref, sin_ref) = refs[:8], refs[8:]
    owners = begin(core_ref, other_ref, owner_ref, order_ref, cos_ref, sin_ref)
    both = jnp.concatenate([y_ref[...], x_ref[...]], axis=0)
    projected = jnp.dot(both, w_ref[...], preferred_element_type=jnp.float32)
    for slot in range(2):
        for h in range(w_ref.shape[1] // HD):
            columns = slice(h * HD, (h + 1) * HD)
            block = projected[slot * SLAB : (slot + 1) * SLAB, columns]
            value = rope(block, slot, cos_ref, sin_ref).T.astype(jnp.bfloat16)
            store_masked(outs[4 * slot : 4 * slot + 4], owners[slot], slice(None), columns, value)


def in_vmem(value):
    return pltpu.with_memory_space_constraint(value, pltpu.VMEM)


def project(kernel, core, owners, slab_order, others, rows, weight, block, blocks, width, out):
    depth = rows.shape[1]
    smem = pl.BlockSpec(memory_space=pltpu.SMEM)
    return pl.pallas_call(
        kernel,
        grid_spec=pltpu.PrefetchScalarGridSpec(
            num_scalar_prefetch=1,
            grid=(blocks,),
            in_specs=[
                smem,
                smem,
                smem,
                pl.BlockSpec(memory_space=pltpu.VMEM),
                pl.BlockSpec(memory_space=pltpu.VMEM),
                pl.BlockSpec((depth, width), lambda j, c: (0, block(j, c[0]))),
            ],
            out_specs=[pl.BlockSpec((o.shape[0], width), lambda j, c: (0, j)) for o in out],
            scratch_shapes=[pltpu.VMEM((2, SLAB, HD), jnp.float32)] * 2,
        ),
        out_shape=out,
        compiler_params=pltpu.CompilerParams(
            dimension_semantics=("arbitrary",), vmem_limit_bytes=24 << 20
        ),
        cost_estimate=pl.CostEstimate(
            flops=4 * SLAB * depth * blocks * width,
            bytes_accessed=2 * depth * (2 * SLAB + blocks * width),
            transcendentals=0,
        ),
    )(core, *owners, slab_order, in_vmem(others), in_vmem(rows), weight)


FACTOR = HD**-0.5 * 1.4426950408889634
WIDE = GROUP * SLAB
LOW, HIGH = (0, 1), (3, 2)
LOCAL = ((LOW, 0), (HIGH, 0))
NEAR = ((LOW, 1), (HIGH, 1), (HIGH, 3), (LOW, 3))
FAR = ((LOW, 2), (HIGH, 2))


def attend_kernel(spots, t, first, last, sequence_ref, order_ref, *refs):
    parts, refs = refs[:4], refs[4:]
    pieces, refs = refs[: len(spots)], refs[len(spots) :]
    if not first:
        old, refs = refs[:3], refs[3:]
    if last:
        out, acc, peak, total, q_ref, kv, scores_ref, chosen = refs
    else:
        acc, peak, total, q_ref, kv, scores_ref, chosen = refs
    row = lax.axis_index("dp")
    column = lax.axis_index("cp")
    core, y, z = lax.rem(column, 2), lax.rem(column // 2, SIDE), column // (2 * SIDE)
    mine = column if t == 1 else column + 1 - 2 * core
    my_sequence, my_order = sequence_ref[row, mine], order_ref[row, mine]
    count = jnp.int32(0)
    for a, (chips, second) in enumerate(spots):
        for b, k in enumerate(chips):
            sz = lax.rem(z + 2 * SIDE - jnp.where(core == 0, k, second), SIDE)
            sy = lax.rem(y + 2 * SIDE - jnp.where(core == 0, second, k), SIDE)
            for c in range(2):
                source = (sz * SIDE + sy) * 2 + (core if c == 1 else 1 - core)
                wanted = (sequence_ref[row, source] == my_sequence) & (
                    order_ref[row, source] < my_order
                )

                @pl.when(wanted)
                def _():
                    kv[count] = pieces[a][(b * 2 + c) * SLAB : (b * 2 + c + 1) * SLAB, :]

                count = count + wanted.astype(jnp.int32)

    @pl.when(lax.rem(count, 2) == 1)
    def _():
        kv[count] = jnp.zeros((SLAB, 4 * HD), jnp.bfloat16)

    pairs_here = (count + 1) // 2
    q_ref[...] = parts[0][...] + parts[1][...] + parts[2][...] + parts[3][...]
    starts = []
    for g in range(2):
        if first:
            key_row = lax.broadcasted_iota(jnp.int32, (SLAB, WIDE), 0)
            token = lax.rem(lax.broadcasted_iota(jnp.int32, (SLAB, WIDE), 1), SLAB)
            scores = jnp.dot(
                pieces[0][t * SLAB : (t + 1) * SLAB, g * HD : (g + 1) * HD],
                q_ref[:, g * WIDE : (g + 1) * WIDE],
                preferred_element_type=jnp.float32,
            )
            scores = jnp.where(key_row <= token, scores, NEG_FILL)
            scores_ref[8, g, :SLAB] = scores
            peak[g] = jnp.max(scores.reshape(SLAB // 8, 8, WIDE), axis=0)
        else:
            peak[g] = old[1][g]
            starts.append(jnp.max(old[1][g], axis=0, keepdims=True))

    def score(p, carry):
        full = 2 * p + 1 < count
        for g in range(2):
            keys = slice(g * HD, (g + 1) * HD)
            both = jnp.concatenate([kv[2 * p, :, keys], kv[2 * p + 1, :, keys]], axis=0)
            scores = jnp.dot(
                both, q_ref[:, g * WIDE : (g + 1) * WIDE], preferred_element_type=jnp.float32
            )
            low = scores[:SLAB]
            high = jnp.where(full, scores[SLAB:], NEG_FILL)
            scores_ref[p, g, :SLAB] = low
            scores_ref[p, g, SLAB:] = high
            top = jnp.maximum(low, high).reshape(SLAB // 8, 8, WIDE)
            peak[g] = jnp.maximum(peak[g], jnp.max(top, axis=0))
        return carry

    lax.fori_loop(0, pairs_here, score, 0)
    tops = []
    for g in range(2):
        top = jnp.max(peak[g], axis=0, keepdims=True)
        tops.append(top * FACTOR)
        if first:
            weights = jnp.exp2(scores_ref[8, g, :SLAB] * FACTOR - tops[g])
            total[g] = jnp.sum(weights.reshape(SLAB // 8, 8, WIDE), axis=0)
            acc[g] = jnp.dot(
                pieces[0][t * SLAB : (t + 1) * SLAB, (2 + g) * HD : (3 + g) * HD],
                weights.astype(jnp.bfloat16),
                preferred_element_type=jnp.float32,
            )
        else:
            rescale = jnp.exp2((starts[g] - top) * FACTOR)
            total[g] = old[2][g] * rescale
            acc[g] = old[0][g] * rescale

    def weigh(p, carry):
        for g in range(2):
            values = slice((2 + g) * HD, (3 + g) * HD)
            weights = jnp.exp2(scores_ref[p, g] * FACTOR - tops[g])
            total[g] = total[g] + jnp.sum(weights.reshape(SLAB // 4, 8, WIDE), axis=0)
            both = jnp.concatenate([kv[2 * p, :, values], kv[2 * p + 1, :, values]], axis=1)
            acc[g] = acc[g] + jnp.dot(
                both, weights.astype(jnp.bfloat16), preferred_element_type=jnp.float32
            )
        return carry

    lax.fori_loop(0, pairs_here, weigh, 0)
    if last:
        for g in range(2):
            context = acc[g] / jnp.sum(total[g], axis=0, keepdims=True)
            for h in range(GROUP):
                head = g * GROUP + h
                out[:, head * HD : (head + 1) * HD] = context[:, h * SLAB : (h + 1) * SLAB].T.astype(
                    jnp.bfloat16
                )


STATE = ((2, HD, WIDE), (2, 8, WIDE), (2, 8, WIDE))
HALF = Q_COLS // 2


def attend(spots, t, slab_sequence, slab_order, parts, pieces, state, last):
    first = state is None
    vmem = pl.BlockSpec(memory_space=pltpu.VMEM)
    smem = pl.BlockSpec(memory_space=pltpu.SMEM)
    scratch = [
        pltpu.VMEM((SLAB, HALF), jnp.bfloat16),
        pltpu.VMEM((16, SLAB, 4 * HD), jnp.bfloat16),
        pltpu.VMEM((9, 2, 2 * SLAB, WIDE), jnp.float32),
    ]
    if last:
        out_shape = [pltpu.VMEM((SLAB, HALF), jnp.bfloat16)]
        scratch = [pltpu.VMEM(s, jnp.float32) for s in STATE] + scratch
    else:
        out_shape = [pltpu.VMEM(s, jnp.float32) for s in STATE]
    operands = [in_vmem(v) for v in (*parts, *pieces, *(state or ()))]
    return pl.pallas_call(
        functools.partial(attend_kernel, spots, t, first, last),
        in_specs=[smem, smem] + [vmem] * len(operands),
        out_specs=[vmem] * len(out_shape),
        out_shape=out_shape,
        scratch_shapes=scratch + [pltpu.SMEM((16,), jnp.int32)],
        compiler_params=pltpu.CompilerParams(vmem_limit_bytes=28 << 20),
        cost_estimate=pl.CostEstimate(
            flops=2 * SLAB * len(spots) * 4 * SLAB * HALF,
            bytes_accessed=2 << 20,
            transcendentals=0,
        ),
    )(slab_sequence, slab_order, *operands)


def join_kernel(core_ref, kept_ref, received_ref, out_ref):
    core = core_ref[0]
    out_ref[:, pl.ds(pl.multiple_of(core * HALF, HALF), HALF)] = kept_ref[...]
    out_ref[:, pl.ds(pl.multiple_of((1 - core) * HALF, HALF), HALF)] = received_ref[...]


def join(core, kept, received):
    vmem = pl.BlockSpec(memory_space=pltpu.VMEM)
    return pl.pallas_call(
        join_kernel,
        in_specs=[pl.BlockSpec(memory_space=pltpu.SMEM), vmem, vmem],
        out_specs=vmem,
        out_shape=jax.ShapeDtypeStruct((SLAB, Q_COLS), jnp.bfloat16),
        compiler_params=pltpu.CompilerParams(vmem_limit_bytes=8 << 20),
        cost_estimate=pl.CostEstimate(flops=SLAB * Q_COLS, bytes_accessed=1 << 20, transcendentals=0),
        name="join",
    )(core, in_vmem(kept), in_vmem(received))


def local(tokens, qkv_weight, owner_slot, slab_sequence, slab_order):
    rows = tokens[0]
    core = lax.rem(lax.axis_index("cp"), 2)
    others = permute(rows, OTHER_CORE)
    owners = (permute(owner_slot, OTHER_CORE), owner_slot)
    common = (core.reshape(1), owners, slab_order, others, rows, qkv_weight)
    kv = project(
        kv_kernel, *common, lambda j, c: QH // 2 + 2 * j + c, 2, 2 * HD,
        [jax.ShapeDtypeStruct((2 * SLAB, 4 * HD), jnp.bfloat16)] * 4,
    )
    queries = project(
        q_kernel, *common, lambda j, c: 4 * c + j, 4, 2 * HD,
        [jax.ShapeDtypeStruct((SLAB, HALF), jnp.bfloat16)] * 8,
    )
    moved = [permute(kv[k], shift_x(k)) for k in (1, 3, 2)]
    parts = [[queries[0]] + [permute(queries[k], shift_x(k)) for k in (1, 3, 2)]]
    own = kv[0] + moved[0] + moved[1] + moved[2]
    first = [permute(own, shift_first(k)) for k in (1, 3, 2)]
    parts.append([queries[4]] + [permute(queries[4 + k], shift_x(k)) for k in (1, 3, 2)])
    low = jnp.concatenate([own, first[0]], axis=0)
    high = jnp.concatenate([first[1], first[2]], axis=0)
    left = [permute(v, shift_second(1)) for v in (low, high)]
    right = [permute(v, shift_second(3)) for v in (high, low)]
    far = [permute(left[0], shift_second(1)), permute(right[0], shift_second(3))]
    near = [low, high, *left, *right]
    tables = (slab_sequence, slab_order)
    state = [attend(LOCAL + NEAR, t, *tables, parts[t], near, None, False) for t in range(2)]
    (sent,) = attend(FAR, 0, *tables, parts[0], far, state[0], True)
    received = permute(sent, OTHER_CORE)
    (kept,) = attend(FAR, 1, *tables, parts[1], far, state[1], True)
    return join(core.reshape(1), kept, received)[None]


def solution(mesh):
    in_specs = (P("dp", "cp", None), P(), P("dp", "cp"), P(), P())
    out_specs = P("dp", "cp", None)
    return jax.shard_map(local, mesh=mesh, in_specs=in_specs, out_specs=out_specs, check_vma=False)
```

```python
import functools

import jax
import jax.numpy as jnp
from jax import lax
from jax.experimental import pallas as pl
from jax.experimental.pallas import tpu as pltpu
from jax.sharding import PartitionSpec as P


QH = 16
KVH = 4
HD = 128
SLAB = 128
GROUP = QH // KVH
NEG_FILL = -1e30
AXES = ("dp", "cp")
SIDE = 4
Q_COLS = QH * HD


def pairs(move):
    out = []
    for x in range(SIDE):
        for z in range(SIDE):
            for y in range(SIDE):
                for c in range(2):
                    nx, nz, ny, nc = move(x, z, y, c)
                    here = x * 32 + (z * SIDE + y) * 2 + c
                    there = (nx % SIDE) * 32 + ((nz % SIDE) * SIDE + ny % SIDE) * 2 + nc % 2
                    out.append((here, there))
    return out


def shift_x(k):
    return pairs(lambda x, z, y, c: (x + k, z, y, c))


def shift_first(k):
    return pairs(lambda x, z, y, c: (x, z + k, y, c) if c == 0 else (x, z, y + k, c))


def shift_second(k):
    return pairs(lambda x, z, y, c: (x, z, y + k, c) if c == 0 else (x, z + k, y, c))


OTHER_CORE = pairs(lambda x, z, y, c: (x, z, y, c + 1))


def permute(value, table):
    return lax.ppermute(value, AXES, table)


def rope_tables(order, slot, cos_ref, sin_ref):
    lane = lax.broadcasted_iota(jnp.int32, (SLAB, HD), 1)
    half = jnp.where(lane < HD // 2, lane, lane - HD // 2).astype(jnp.float32)
    frequency = jnp.exp(half * (-2.0 / HD * 13.122363377404328))
    row = lax.broadcasted_iota(jnp.int32, (SLAB, HD), 0)
    angle = (order * SLAB + row).astype(jnp.float32) * frequency
    cos_ref[slot] = jnp.cos(angle)
    sine = jnp.sin(angle)
    sin_ref[slot] = jnp.where(lane < HD // 2, -sine, sine)


def rope(block, slot, cos_ref, sin_ref):
    return block * cos_ref[slot] + pltpu.roll(block, HD // 2, 1) * sin_ref[slot]


def begin(core_ref, other_ref, owner_ref, order_ref, cos_ref, sin_ref):
    column = lax.axis_index("cp")
    owners = (other_ref[0, 0], owner_ref[0, 0])
    columns = (column + 1 - 2 * core_ref[0], column)

    @pl.when(pl.program_id(0) == 0)
    def _():
        for slot in range(2):
            rope_tables(order_ref[owners[slot], columns[slot]], slot, cos_ref, sin_ref)

    return owners


def store_masked(outs, owner, rows, columns, value):
    my_row = lax.axis_index("dp")
    for k, out in enumerate(outs):
        mine = owner == lax.rem(my_row + k, SIDE)
        out[rows, columns] = jnp.where(mine, value, jnp.zeros_like(value))


def kv_kernel(core_ref, other_ref, owner_ref, order_ref, y_ref, x_ref, w_ref, *refs):
    outs, (cos_ref, sin_ref) = refs[:4], refs[4:]
    owners = begin(core_ref, other_ref, owner_ref, order_ref, cos_ref, sin_ref)
    both = jnp.concatenate([y_ref[...], x_ref[...]], axis=0)
    projected = jnp.dot(both, w_ref[...], preferred_element_type=jnp.float32)
    heads = w_ref.shape[1] // HD
    step = pl.program_id(0)

    @pl.when(step < 2 // heads)
    def _():
        for slot in range(2):
            rows = slice(slot * SLAB, (slot + 1) * SLAB)
            for h in range(heads):
                columns = slice(h * HD, (h + 1) * HD)
                value = rope(projected[rows, columns], slot, cos_ref, sin_ref).astype(jnp.bfloat16)
                store_masked(outs, owners[slot], rows, columns, value)

    @pl.when(step >= 2 // heads)
    def _():
        for slot in range(2):
            rows = slice(slot * SLAB, (slot + 1) * SLAB)
            for h in range(heads):
                columns = slice(h * HD, (h + 1) * HD)
                value = projected[rows, columns].T.astype(jnp.bfloat16)
                store_masked(outs, owners[slot], rows, columns, value)


def q_kernel(core_ref, other_ref, owner_ref, order_ref, y_ref, x_ref, w_ref, *refs):
    outs, (cos_ref, sin_ref) = refs[:8], refs[8:]
    owners = begin(core_ref, other_ref, owner_ref, order_ref, cos_ref, sin_ref)
    both = jnp.concatenate([y_ref[...], x_ref[...]], axis=0)
    projected = jnp.dot(both, w_ref[...], preferred_element_type=jnp.float32)
    for slot in range(2):
        for h in range(w_ref.shape[1] // HD):
            columns = slice(h * HD, (h + 1) * HD)
            block = projected[slot * SLAB : (slot + 1) * SLAB, columns]
            value = rope(block, slot, cos_ref, sin_ref).T.astype(jnp.bfloat16)
            store_masked(outs[4 * slot : 4 * slot + 4], owners[slot], slice(None), columns, value)


def in_vmem(value):
    return pltpu.with_memory_space_constraint(value, pltpu.VMEM)


def in_hbm(value):
    return pltpu.with_memory_space_constraint(value, pltpu.HBM)


def project(kernel, core, owners, slab_order, others, rows, weight, block, blocks, width, out):
    depth = rows.shape[1]
    smem = pl.BlockSpec(memory_space=pltpu.SMEM)
    return pl.pallas_call(
        kernel,
        grid_spec=pltpu.PrefetchScalarGridSpec(
            num_scalar_prefetch=1,
            grid=(blocks,),
            in_specs=[
                smem,
                smem,
                smem,
                pl.BlockSpec(memory_space=pltpu.VMEM),
                pl.BlockSpec((SLAB, depth), lambda j, c: (0, 0)),
                pl.BlockSpec((depth, width), lambda j, c: (0, block(j, c[0]))),
            ],
            out_specs=[pl.BlockSpec((o.shape[0], width), lambda j, c: (0, j)) for o in out],
            scratch_shapes=[pltpu.VMEM((2, SLAB, HD), jnp.float32)] * 2,
        ),
        out_shape=out,
        compiler_params=pltpu.CompilerParams(
            dimension_semantics=("arbitrary",), vmem_limit_bytes=24 << 20
        ),
        cost_estimate=pl.CostEstimate(
            flops=4 * SLAB * depth * blocks * width,
            bytes_accessed=2 * depth * (2 * SLAB + blocks * width),
            transcendentals=0,
        ),
    )(core, *owners, in_hbm(slab_order), in_vmem(others), in_hbm(rows), in_hbm(weight))


FACTOR = HD**-0.5 * 1.4426950408889634
WIDE = GROUP * SLAB
LOW, HIGH = (0, 1), (3, 2)
LOCAL = ((LOW, 0), (HIGH, 0))
NEAR = ((LOW, 1), (HIGH, 1), (HIGH, 3), (LOW, 3))
FAR = ((LOW, 2), (HIGH, 2))


def attend_kernel(spots, t, first, last, sequence_ref, order_ref, *refs):
    parts, refs = refs[:4], refs[4:]
    pieces, refs = refs[: len(spots)], refs[len(spots) :]
    if not first:
        old, refs = refs[:3], refs[3:]
    if last:
        out, acc, peak, total, q_ref, kv, scores_ref, chosen = refs
    else:
        acc, peak, total, q_ref, kv, scores_ref, chosen = refs
    row = lax.axis_index("dp")
    column = lax.axis_index("cp")
    core, y, z = lax.rem(column, 2), lax.rem(column // 2, SIDE), column // (2 * SIDE)
    mine = column if t == 1 else column + 1 - 2 * core
    my_sequence, my_order = sequence_ref[row, mine], order_ref[row, mine]
    count = jnp.int32(0)
    for a, (chips, second) in enumerate(spots):
        for b, k in enumerate(chips):
            sz = lax.rem(z + 2 * SIDE - jnp.where(core == 0, k, second), SIDE)
            sy = lax.rem(y + 2 * SIDE - jnp.where(core == 0, second, k), SIDE)
            for c in range(2):
                source = (sz * SIDE + sy) * 2 + (core if c == 1 else 1 - core)
                wanted = (sequence_ref[row, source] == my_sequence) & (
                    order_ref[row, source] < my_order
                )

                @pl.when(wanted)
                def _():
                    kv[count] = pieces[a][(b * 2 + c) * SLAB : (b * 2 + c + 1) * SLAB, :]

                count = count + wanted.astype(jnp.int32)

    @pl.when(lax.rem(count, 2) == 1)
    def _():
        kv[count] = jnp.zeros((SLAB, 4 * HD), jnp.bfloat16)

    pairs_here = (count + 1) // 2
    q_ref[...] = parts[0][...] + parts[1][...] + parts[2][...] + parts[3][...]
    starts = []
    for g in range(2):
        if first:
            key_row = lax.broadcasted_iota(jnp.int32, (SLAB, WIDE), 0)
            token = lax.rem(lax.broadcasted_iota(jnp.int32, (SLAB, WIDE), 1), SLAB)
            scores = jnp.dot(
                pieces[0][t * SLAB : (t + 1) * SLAB, g * HD : (g + 1) * HD],
                q_ref[:, g * WIDE : (g + 1) * WIDE],
                preferred_element_type=jnp.float32,
            )
            scores = jnp.where(key_row <= token, scores, NEG_FILL)
            scores_ref[8, g, :SLAB] = scores
            peak[g] = jnp.max(scores.reshape(SLAB // 8, 8, WIDE), axis=0)
        else:
            peak[g] = old[1][g]
            starts.append(jnp.max(old[1][g], axis=0, keepdims=True))

    def score(p, carry):
        full = 2 * p + 1 < count
        for g in range(2):
            keys = slice(g * HD, (g + 1) * HD)
            both = jnp.concatenate([kv[2 * p, :, keys], kv[2 * p + 1, :, keys]], axis=0)
            scores = jnp.dot(
                both, q_ref[:, g * WIDE : (g + 1) * WIDE], preferred_element_type=jnp.float32
            )
            low = scores[:SLAB]
            high = jnp.where(full, scores[SLAB:], NEG_FILL)
            scores_ref[p, g, :SLAB] = low
            scores_ref[p, g, SLAB:] = high
            top = jnp.maximum(low, high).reshape(SLAB // 8, 8, WIDE)
            peak[g] = jnp.maximum(peak[g], jnp.max(top, axis=0))
        return carry

    lax.fori_loop(0, pairs_here, score, 0)
    tops = []
    for g in range(2):
        top = jnp.max(peak[g], axis=0, keepdims=True)
        tops.append(top * FACTOR)
        if first:
            weights = jnp.exp2(scores_ref[8, g, :SLAB] * FACTOR - tops[g])
            total[g] = jnp.sum(weights.reshape(SLAB // 8, 8, WIDE), axis=0)
            acc[g] = jnp.dot(
                pieces[0][t * SLAB : (t + 1) * SLAB, (2 + g) * HD : (3 + g) * HD],
                weights.astype(jnp.bfloat16),
                preferred_element_type=jnp.float32,
            )
        else:
            rescale = jnp.exp2((starts[g] - top) * FACTOR)
            total[g] = old[2][g] * rescale
            acc[g] = old[0][g] * rescale

    def weigh(p, carry):
        for g in range(2):
            values = slice((2 + g) * HD, (3 + g) * HD)
            weights = jnp.exp2(scores_ref[p, g] * FACTOR - tops[g])
            total[g] = total[g] + jnp.sum(weights.reshape(SLAB // 4, 8, WIDE), axis=0)
            both = jnp.concatenate([kv[2 * p, :, values], kv[2 * p + 1, :, values]], axis=1)
            acc[g] = acc[g] + jnp.dot(
                both, weights.astype(jnp.bfloat16), preferred_element_type=jnp.float32
            )
        return carry

    lax.fori_loop(0, pairs_here, weigh, 0)
    if last:
        for g in range(2):
            context = acc[g] / jnp.sum(total[g], axis=0, keepdims=True)
            for h in range(GROUP):
                head = g * GROUP + h
                out[:, head * HD : (head + 1) * HD] = context[:, h * SLAB : (h + 1) * SLAB].T.astype(
                    jnp.bfloat16
                )


STATE = ((2, HD, WIDE), (2, 8, WIDE), (2, 8, WIDE))
HALF = Q_COLS // 2


def attend(spots, t, slab_sequence, slab_order, parts, pieces, state, last):
    first = state is None
    vmem = pl.BlockSpec(memory_space=pltpu.VMEM)
    smem = pl.BlockSpec(memory_space=pltpu.SMEM)
    scratch = [
        pltpu.VMEM((SLAB, HALF), jnp.bfloat16),
        pltpu.VMEM((16, SLAB, 4 * HD), jnp.bfloat16),
        pltpu.VMEM((9, 2, 2 * SLAB, WIDE), jnp.float32),
    ]
    if last:
        out_shape = [pltpu.VMEM((SLAB, HALF), jnp.bfloat16)]
        scratch = [pltpu.VMEM(s, jnp.float32) for s in STATE] + scratch
    else:
        out_shape = [pltpu.VMEM(s, jnp.float32) for s in STATE]
    operands = [in_vmem(v) for v in (*parts, *pieces, *(state or ()))]
    return pl.pallas_call(
        functools.partial(attend_kernel, spots, t, first, last),
        in_specs=[smem, smem] + [vmem] * len(operands),
        out_specs=[vmem] * len(out_shape),
        out_shape=out_shape,
        scratch_shapes=scratch + [pltpu.SMEM((16,), jnp.int32)],
        compiler_params=pltpu.CompilerParams(vmem_limit_bytes=28 << 20),
        cost_estimate=pl.CostEstimate(
            flops=2 * SLAB * len(spots) * 4 * SLAB * HALF,
            bytes_accessed=2 << 20,
            transcendentals=0,
        ),
    )(in_hbm(slab_sequence), in_hbm(slab_order), *operands)


def join_kernel(core_ref, kept_ref, received_ref, out_ref):
    core = core_ref[0]
    out_ref[:, pl.ds(pl.multiple_of(core * HALF, HALF), HALF)] = kept_ref[...]
    out_ref[:, pl.ds(pl.multiple_of((1 - core) * HALF, HALF), HALF)] = received_ref[...]


def join(core, kept, received):
    vmem = pl.BlockSpec(memory_space=pltpu.VMEM)
    return pl.pallas_call(
        join_kernel,
        in_specs=[pl.BlockSpec(memory_space=pltpu.SMEM), vmem, vmem],
        out_specs=vmem,
        out_shape=jax.ShapeDtypeStruct((SLAB, Q_COLS), jnp.bfloat16),
        compiler_params=pltpu.CompilerParams(vmem_limit_bytes=8 << 20),
        cost_estimate=pl.CostEstimate(flops=SLAB * Q_COLS, bytes_accessed=1 << 20, transcendentals=0),
        name="join",
    )(core, in_vmem(kept), in_vmem(received))


def local(tokens, qkv_weight, owner_slot, slab_sequence, slab_order):
    rows = tokens[0]
    core = lax.rem(lax.axis_index("cp"), 2)
    others = permute(rows, OTHER_CORE)
    owners = (permute(owner_slot, OTHER_CORE), owner_slot)
    common = (core.reshape(1), owners, slab_order, others, rows, qkv_weight)
    kv = project(
        kv_kernel, *common, lambda j, c: QH // 2 + 2 * j + c, 2, 2 * HD,
        [jax.ShapeDtypeStruct((2 * SLAB, 4 * HD), jnp.bfloat16)] * 4,
    )
    queries = project(
        q_kernel, *common, lambda j, c: 2 * c + j, 2, 4 * HD,
        [jax.ShapeDtypeStruct((SLAB, HALF), jnp.bfloat16)] * 8,
    )
    moved = [permute(kv[k], shift_x(k)) for k in (1, 3, 2)]
    parts = [[queries[0]] + [permute(queries[k], shift_x(k)) for k in (1, 3, 2)]]
    own = kv[0] + moved[0] + moved[1] + moved[2]
    first = [permute(own, shift_first(k)) for k in (1, 3, 2)]
    parts.append([queries[4]] + [permute(queries[4 + k], shift_x(k)) for k in (1, 3, 2)])
    low = jnp.concatenate([own, first[0]], axis=0)
    high = jnp.concatenate([first[1], first[2]], axis=0)
    left = [permute(v, shift_second(1)) for v in (low, high)]
    right = [permute(v, shift_second(3)) for v in (high, low)]
    far = [permute(left[0], shift_second(1)), permute(right[0], shift_second(3))]
    tables = (slab_sequence, slab_order)
    state = [None, None]
    for spots, pieces in ((LOCAL, [low, high]), (NEAR, left + right)):
        for t in range(2):
            state[t] = attend(spots, t, *tables, parts[t], pieces, state[t], False)
    (sent,) = attend(FAR, 0, *tables, parts[0], far, state[0], True)
    received = permute(sent, OTHER_CORE)
    (kept,) = attend(FAR, 1, *tables, parts[1], far, state[1], True)
    return join(core.reshape(1), kept, received)[None]


def solution(mesh):
    in_specs = (P("dp", "cp", None), P(), P("dp", "cp"), P(), P())
    out_specs = P("dp", "cp", None)
    return jax.shard_map(local, mesh=mesh, in_specs=in_specs, out_specs=out_specs, check_vma=False)
```

```python
import functools

import jax
import jax.numpy as jnp
from jax import lax
from jax.experimental import pallas as pl
from jax.experimental.pallas import tpu as pltpu
from jax.sharding import PartitionSpec as P


QH = 16
KVH = 4
HD = 128
SLAB = 128
GROUP = QH // KVH
NEG_FILL = -1e30
AXES = ("dp", "cp")
SIDE = 4
Q_COLS = QH * HD


def pairs(move):
    out = []
    for x in range(SIDE):
        for z in range(SIDE):
            for y in range(SIDE):
                for c in range(2):
                    nx, nz, ny, nc = move(x, z, y, c)
                    here = x * 32 + (z * SIDE + y) * 2 + c
                    there = (nx % SIDE) * 32 + ((nz % SIDE) * SIDE + ny % SIDE) * 2 + nc % 2
                    out.append((here, there))
    return out


def shift_x(k):
    return pairs(lambda x, z, y, c: (x + k, z, y, c))


def shift_first(k):
    return pairs(lambda x, z, y, c: (x, z + k, y, c) if c == 0 else (x, z, y + k, c))


def shift_second(k):
    return pairs(lambda x, z, y, c: (x, z, y + k, c) if c == 0 else (x, z + k, y, c))


OTHER_CORE = pairs(lambda x, z, y, c: (x, z, y, c + 1))


def permute(value, table):
    return lax.ppermute(value, AXES, table)


def rope_tables(order, slot, cos_ref, sin_ref):
    lane = lax.broadcasted_iota(jnp.int32, (SLAB, HD), 1)
    half = jnp.where(lane < HD // 2, lane, lane - HD // 2).astype(jnp.float32)
    frequency = jnp.exp(half * (-2.0 / HD * 13.122363377404328))
    row = lax.broadcasted_iota(jnp.int32, (SLAB, HD), 0)
    angle = (order * SLAB + row).astype(jnp.float32) * frequency
    cos_ref[slot] = jnp.cos(angle)
    sine = jnp.sin(angle)
    sin_ref[slot] = jnp.where(lane < HD // 2, -sine, sine)


def rope(block, slot, cos_ref, sin_ref):
    return block * cos_ref[slot] + pltpu.roll(block, HD // 2, 1) * sin_ref[slot]


def begin(core_ref, other_ref, owner_ref, order_ref, cos_ref, sin_ref):
    column = lax.axis_index("cp")
    owners = (other_ref[0, 0], owner_ref[0, 0])
    columns = (column + 1 - 2 * core_ref[0], column)

    @pl.when(pl.program_id(0) == 0)
    def _():
        for slot in range(2):
            rope_tables(order_ref[owners[slot], columns[slot]], slot, cos_ref, sin_ref)

    return owners


def store_masked(outs, owner, rows, first, value):
    my_row = lax.axis_index("dp")
    columns = pl.ds(pl.multiple_of(first, HD), HD)
    for k, out in enumerate(outs):
        mine = owner == lax.rem(my_row + k, SIDE)
        out[rows, columns] = jnp.where(mine, value, jnp.zeros_like(value))


def kv_kernel(core_ref, other_ref, owner_ref, order_ref, y_ref, x_ref, w_ref, *refs):
    outs, (cos_ref, sin_ref) = refs[:4], refs[4:]
    owners = begin(core_ref, other_ref, owner_ref, order_ref, cos_ref, sin_ref)
    both = jnp.concatenate([y_ref[...], x_ref[...]], axis=0)
    projected = jnp.dot(both, w_ref[...], preferred_element_type=jnp.float32)
    heads = w_ref.shape[1] // HD
    step = pl.program_id(0)

    @pl.when(step < 2 // heads)
    def _():
        for slot in range(2):
            rows = slice(slot * SLAB, (slot + 1) * SLAB)
            for h in range(heads):
                columns = slice(h * HD, (h + 1) * HD)
                value = rope(projected[rows, columns], slot, cos_ref, sin_ref).astype(jnp.bfloat16)
                store_masked(outs, owners[slot], rows, (step * heads + h) * HD, value)

    @pl.when(step >= 2 // heads)
    def _():
        for slot in range(2):
            rows = slice(slot * SLAB, (slot + 1) * SLAB)
            for h in range(heads):
                columns = slice(h * HD, (h + 1) * HD)
                value = projected[rows, columns].T.astype(jnp.bfloat16)
                store_masked(outs, owners[slot], rows, (step * heads + h) * HD, value)


def q_kernel(core_ref, other_ref, owner_ref, order_ref, y_ref, x_ref, w_ref, *refs):
    outs, (cos_ref, sin_ref) = refs[:8], refs[8:]
    owners = begin(core_ref, other_ref, owner_ref, order_ref, cos_ref, sin_ref)
    both = jnp.concatenate([y_ref[...], x_ref[...]], axis=0)
    projected = jnp.dot(both, w_ref[...], preferred_element_type=jnp.float32)
    heads = w_ref.shape[1] // HD
    for slot in range(2):
        for h in range(heads):
            columns = slice(h * HD, (h + 1) * HD)
            first = (pl.program_id(0) * heads + h) * HD
            block = projected[slot * SLAB : (slot + 1) * SLAB, columns]
            value = rope(block, slot, cos_ref, sin_ref).T.astype(jnp.bfloat16)
            store_masked(outs[4 * slot : 4 * slot + 4], owners[slot], slice(None), first, value)


def in_vmem(value):
    return pltpu.with_memory_space_constraint(value, pltpu.VMEM)


def in_hbm(value):
    return pltpu.with_memory_space_constraint(value, pltpu.HBM)


def project(kernel, core, owners, slab_order, others, rows, weight, block, blocks, width, out):
    depth = rows.shape[1]
    smem = pl.BlockSpec(memory_space=pltpu.SMEM)
    return pl.pallas_call(
        kernel,
        grid_spec=pltpu.PrefetchScalarGridSpec(
            num_scalar_prefetch=1,
            grid=(blocks,),
            in_specs=[
                smem,
                smem,
                smem,
                pl.BlockSpec(memory_space=pltpu.VMEM),
                pl.BlockSpec((SLAB, depth), lambda j, c: (0, 0)),
                pl.BlockSpec((depth, width), lambda j, c: (0, block(j, c[0]))),
            ],
            out_specs=[pl.BlockSpec(memory_space=pltpu.VMEM)] * len(out),
            scratch_shapes=[pltpu.VMEM((2, SLAB, HD), jnp.float32)] * 2,
        ),
        out_shape=out,
        compiler_params=pltpu.CompilerParams(
            dimension_semantics=("arbitrary",), vmem_limit_bytes=24 << 20
        ),
        cost_estimate=pl.CostEstimate(
            flops=4 * SLAB * depth * blocks * width,
            bytes_accessed=2 * depth * (2 * SLAB + blocks * width),
            transcendentals=0,
        ),
    )(core, *owners, in_hbm(slab_order), in_vmem(others), in_hbm(rows), in_hbm(weight))


FACTOR = HD**-0.5 * 1.4426950408889634
WIDE = GROUP * SLAB
HALF = Q_COLS // 2
STATE = ((2, HD, WIDE), (2, 8, WIDE), (2, 8, WIDE))
OWN, ONE, TWO = (0,), (1,), (3, 2)


def collect(t, spots, pieces, sequence_ref, order_ref, kv):
    row = lax.axis_index("dp")
    column = lax.axis_index("cp")
    core, y, z = lax.rem(column, 2), lax.rem(column // 2, SIDE), column // (2 * SIDE)
    mine = column if t == 1 else column + 1 - 2 * core
    my_sequence, my_order = sequence_ref[row, mine], order_ref[row, mine]
    count = jnp.int32(0)
    for piece, (chips, second) in zip(pieces, spots):
        for b, k in enumerate(chips):
            sz = lax.rem(z + 2 * SIDE - jnp.where(core == 0, k, second), SIDE)
            sy = lax.rem(y + 2 * SIDE - jnp.where(core == 0, second, k), SIDE)
            for c in range(2):
                source = (sz * SIDE + sy) * 2 + (core if c == 1 else 1 - core)
                wanted = (sequence_ref[row, source] == my_sequence) & (
                    order_ref[row, source] < my_order
                )

                @pl.when(wanted)
                def _():
                    kv[count] = piece[(b * 2 + c) * SLAB : (b * 2 + c + 1) * SLAB, :]

                count = count + wanted.astype(jnp.int32)

    @pl.when(lax.rem(count, 2) == 1)
    def _():
        kv[count] = jnp.zeros((SLAB, 4 * HD), jnp.bfloat16)

    return count


def attend_slab(t, spots, pieces, parts, old, new, out, sequence_ref, order_ref, q_ref, kv, scores_ref):
    acc, peak, total = new
    first = old is None
    count = collect(t, spots, pieces, sequence_ref, order_ref, kv)
    pairs_here = (count + 1) // 2
    q_ref[...] = parts[0][...] + parts[1][...] + parts[2][...] + parts[3][...]
    starts = []
    for g in range(2):
        if first:
            key_row = lax.broadcasted_iota(jnp.int32, (SLAB, WIDE), 0)
            token = lax.rem(lax.broadcasted_iota(jnp.int32, (SLAB, WIDE), 1), SLAB)
            scores = jnp.dot(
                pieces[0][t * SLAB : (t + 1) * SLAB, g * HD : (g + 1) * HD],
                q_ref[:, g * WIDE : (g + 1) * WIDE],
                preferred_element_type=jnp.float32,
            )
            scores = jnp.where(key_row <= token, scores, NEG_FILL)
            scores_ref[8, g, :SLAB] = scores
            peak[g] = jnp.max(scores.reshape(SLAB // 8, 8, WIDE), axis=0)
        else:
            starts.append(jnp.max(old[1][g], axis=0, keepdims=True))
            peak[g] = old[1][g]

    def score(p, carry):
        full = 2 * p + 1 < count
        for g in range(2):
            keys = slice(g * HD, (g + 1) * HD)
            both = jnp.concatenate([kv[2 * p, :, keys], kv[2 * p + 1, :, keys]], axis=0)
            scores = jnp.dot(
                both, q_ref[:, g * WIDE : (g + 1) * WIDE], preferred_element_type=jnp.float32
            )
            low = scores[:SLAB]
            high = jnp.where(full, scores[SLAB:], NEG_FILL)
            scores_ref[p, g, :SLAB] = low
            scores_ref[p, g, SLAB:] = high
            top = jnp.maximum(low, high).reshape(SLAB // 8, 8, WIDE)
            peak[g] = jnp.maximum(peak[g], jnp.max(top, axis=0))
        return carry

    lax.fori_loop(0, pairs_here, score, 0)
    tops = []
    for g in range(2):
        top = jnp.max(peak[g], axis=0, keepdims=True)
        tops.append(top * FACTOR)
        if first:
            weights = jnp.exp2(scores_ref[8, g, :SLAB] * FACTOR - tops[g])
            total[g] = jnp.sum(weights.reshape(SLAB // 8, 8, WIDE), axis=0)
            acc[g] = jnp.dot(
                pieces[0][t * SLAB : (t + 1) * SLAB, (2 + g) * HD : (3 + g) * HD],
                weights.astype(jnp.bfloat16),
                preferred_element_type=jnp.float32,
            )
        else:
            rescale = jnp.exp2((starts[g] - top) * FACTOR)
            total[g] = old[2][g] * rescale
            acc[g] = old[0][g] * rescale

    def weigh(p, carry):
        for g in range(2):
            values = slice((2 + g) * HD, (3 + g) * HD)
            weights = jnp.exp2(scores_ref[p, g] * FACTOR - tops[g])
            total[g] = total[g] + jnp.sum(weights.reshape(SLAB // 4, 8, WIDE), axis=0)
            both = jnp.concatenate([kv[2 * p, :, values], kv[2 * p + 1, :, values]], axis=1)
            acc[g] = acc[g] + jnp.dot(
                both, weights.astype(jnp.bfloat16), preferred_element_type=jnp.float32
            )
        return carry

    lax.fori_loop(0, pairs_here, weigh, 0)
    if out is not None:
        for g in range(2):
            context = acc[g] / jnp.sum(total[g], axis=0, keepdims=True)
            for h in range(GROUP):
                head = g * GROUP + h
                out[:, head * HD : (head + 1) * HD] = context[:, h * SLAB : (h + 1) * SLAB].T.astype(
                    jnp.bfloat16
                )


def attend_kernel(jobs, spots, last, sequence_ref, order_ref, *refs):
    pieces, refs = refs[: len(spots)], refs[len(spots) :]
    given = []
    for t, start, first in jobs:
        parts, refs = refs[:4], refs[4:]
        old = None
        if not first:
            old, refs = refs[:3], refs[3:]
        given.append((parts, old))
    per = 1 if last else 3
    outs, refs = refs[: per * len(jobs)], refs[per * len(jobs) :]
    state, refs = (refs[:3], refs[3:]) if last else (None, refs)
    q_ref, kv, scores_ref = refs
    for n, (t, start, first) in enumerate(jobs):
        parts, old = given[n]
        new = state if last else outs[3 * n : 3 * n + 3]
        out = outs[n] if last else None
        attend_slab(
            t, spots[start:], pieces[start:], parts, old, new, out,
            sequence_ref, order_ref, q_ref, kv, scores_ref,
        )


def attend(jobs, slab_sequence, slab_order, items, parts, states, last):
    vmem = pl.BlockSpec(memory_space=pltpu.VMEM)
    smem = pl.BlockSpec(memory_space=pltpu.SMEM)
    scratch = [
        pltpu.VMEM((SLAB, HALF), jnp.bfloat16),
        pltpu.VMEM((16, SLAB, 4 * HD), jnp.bfloat16),
        pltpu.VMEM((9, 2, 2 * SLAB, WIDE), jnp.float32),
    ]
    operands = [v for v, _, _ in items]
    spots = [(chips, second) for _, chips, second in items]
    for t, start, first in jobs:
        operands += parts[t]
        if not first:
            operands += states[t]
    if last:
        out_shape = [pltpu.VMEM((SLAB, HALF), jnp.bfloat16)] * len(jobs)
        scratch = [pltpu.VMEM(s, jnp.float32) for s in STATE] + scratch
    else:
        out_shape = [pltpu.VMEM(s, jnp.float32) for s in STATE] * len(jobs)
    return pl.pallas_call(
        functools.partial(attend_kernel, jobs, spots, last),
        in_specs=[smem, smem] + [vmem] * len(operands),
        out_specs=[vmem] * len(out_shape),
        out_shape=out_shape,
        scratch_shapes=scratch,
        compiler_params=pltpu.CompilerParams(vmem_limit_bytes=28 << 20),
        cost_estimate=pl.CostEstimate(
            flops=2 * SLAB * len(spots) * 4 * SLAB * HALF,
            bytes_accessed=2 << 20,
            transcendentals=0,
        ),
    )(in_hbm(slab_sequence), in_hbm(slab_order), *[in_vmem(v) for v in operands])


def join_kernel(core_ref, kept_ref, received_ref, out_ref):
    core = core_ref[0]
    out_ref[:, pl.ds(pl.multiple_of(core * HALF, HALF), HALF)] = kept_ref[...]
    out_ref[:, pl.ds(pl.multiple_of((1 - core) * HALF, HALF), HALF)] = received_ref[...]


def join(core, kept, received):
    vmem = pl.BlockSpec(memory_space=pltpu.VMEM)
    return pl.pallas_call(
        join_kernel,
        in_specs=[pl.BlockSpec(memory_space=pltpu.SMEM), vmem, vmem],
        out_specs=vmem,
        out_shape=jax.ShapeDtypeStruct((SLAB, Q_COLS), jnp.bfloat16),
        compiler_params=pltpu.CompilerParams(vmem_limit_bytes=8 << 20),
        cost_estimate=pl.CostEstimate(flops=SLAB * Q_COLS, bytes_accessed=1 << 20, transcendentals=0),
        name="join",
    )(core, in_vmem(kept), in_vmem(received))


def local(tokens, qkv_weight, owner_slot, slab_sequence, slab_order):
    rows = tokens[0]
    core = lax.rem(lax.axis_index("cp"), 2)
    others = permute(rows, OTHER_CORE)
    owners = (permute(owner_slot, OTHER_CORE), owner_slot)
    common = (core.reshape(1), owners, slab_order, others, rows, qkv_weight)
    kv = project(
        kv_kernel, *common, lambda j, c: QH // 2 + 2 * j + c, 2, 2 * HD,
        [pltpu.VMEM((2 * SLAB, 4 * HD), jnp.bfloat16)] * 4,
    )
    queries = project(
        q_kernel, *common, lambda j, c: 2 * c + j, 2, 4 * HD,
        [pltpu.VMEM((SLAB, HALF), jnp.bfloat16)] * 8,
    )
    moved = [permute(kv[k], shift_x(k)) for k in (1, 3, 2)]
    parts = [[queries[0]] + [permute(queries[k], shift_x(k)) for k in (1, 3, 2)]]
    own = kv[0] + moved[0] + moved[1] + moved[2]
    first = [permute(own, shift_first(k)) for k in (1, 3, 2)]
    left = [permute(own, shift_second(1))]
    right = [permute(own, shift_second(3))]
    parts.append([queries[4]] + [permute(queries[4 + k], shift_x(k)) for k in (1, 3, 2)])
    two = jnp.concatenate([first[1], first[2]], axis=0)
    left += [permute(v, shift_second(1)) for v in (first[0], two)]
    right += [permute(v, shift_second(3)) for v in (two, first[0])]
    far = [permute(left[0], shift_second(1))]
    far += [permute(left[1], shift_second(1)), permute(right[1], shift_second(3))]
    local_items = [
        (own, OWN, 0), (first[0], ONE, 0), (two, TWO, 0), (left[0], OWN, 1), (right[0], OWN, 3)
    ]
    near_items = [
        (left[1], ONE, 1), (right[2], ONE, 3), (far[0], OWN, 2), (left[2], TWO, 1), (right[1], TWO, 3)
    ]
    far_items = [(far[1], ONE, 2), (far[2], TWO, 2)]
    tables = (slab_sequence, slab_order)
    state = [None, None]
    state[0] = attend([(0, 0, True)], *tables, local_items, parts, state, False)
    both = attend(
        [(0, len(local_items), False), (1, 0, True)],
        *tables, local_items + near_items, parts, state, False,
    )
    state = [both[:3], both[3:]]
    sent, kept = attend([(0, 0, False), (1, 0, False)], *tables, far_items, parts, state, True)
    received = permute(sent, OTHER_CORE)
    return join(core.reshape(1), kept, received)[None]


def solution(mesh):
    in_specs = (P("dp", "cp", None), P(), P("dp", "cp"), P(), P())
    out_specs = P("dp", "cp", None)
    return jax.shard_map(local, mesh=mesh, in_specs=in_specs, out_specs=out_specs, check_vma=False)
```

```python
import functools

import jax
import jax.numpy as jnp
from jax import lax
from jax.experimental import pallas as pl
from jax.experimental.pallas import tpu as pltpu
from jax.sharding import PartitionSpec as P


QH = 16
KVH = 4
HD = 128
SLAB = 128
GROUP = QH // KVH
NEG_FILL = -1e30
AXES = ("dp", "cp")
SIDE = 4
Q_COLS = QH * HD


def pairs(move):
    out = []
    for x in range(SIDE):
        for z in range(SIDE):
            for y in range(SIDE):
                for c in range(2):
                    nx, nz, ny, nc = move(x, z, y, c)
                    here = x * 32 + (z * SIDE + y) * 2 + c
                    there = (nx % SIDE) * 32 + ((nz % SIDE) * SIDE + ny % SIDE) * 2 + nc % 2
                    out.append((here, there))
    return out


def shift_x(k):
    return pairs(lambda x, z, y, c: (x + k, z, y, c))


def shift_first(k):
    return pairs(lambda x, z, y, c: (x, z + k, y, c) if c == 0 else (x, z, y + k, c))


def shift_second(k):
    return pairs(lambda x, z, y, c: (x, z, y + k, c) if c == 0 else (x, z + k, y, c))


OTHER_CORE = pairs(lambda x, z, y, c: (x, z, y, c + 1))


def permute(value, table):
    return lax.ppermute(value, AXES, table)


def rope_tables(order, slot, cos_ref, sin_ref):
    lane = lax.broadcasted_iota(jnp.int32, (SLAB, HD), 1)
    half = jnp.where(lane < HD // 2, lane, lane - HD // 2).astype(jnp.float32)
    frequency = jnp.exp(half * (-2.0 / HD * 13.122363377404328))
    row = lax.broadcasted_iota(jnp.int32, (SLAB, HD), 0)
    angle = (order * SLAB + row).astype(jnp.float32) * frequency
    cos_ref[slot] = jnp.cos(angle)
    sine = jnp.sin(angle)
    sin_ref[slot] = jnp.where(lane < HD // 2, -sine, sine)


def rope(block, slot, cos_ref, sin_ref):
    return block * cos_ref[slot] + pltpu.roll(block, HD // 2, 1) * sin_ref[slot]


def begin(core_ref, other_ref, owner_ref, order_ref, cos_ref, sin_ref):
    column = lax.axis_index("cp")
    owners = (other_ref[0, 0], owner_ref[0, 0])
    columns = (column + 1 - 2 * core_ref[0], column)

    @pl.when(pl.program_id(0) == 0)
    def _():
        for slot in range(2):
            rope_tables(order_ref[owners[slot], columns[slot]], slot, cos_ref, sin_ref)

    return owners


def store_masked(outs, owner, rows, first, value):
    my_row = lax.axis_index("dp")
    columns = pl.ds(pl.multiple_of(first, HD), HD)
    for k, out in enumerate(outs):
        mine = owner == lax.rem(my_row + k, SIDE)
        out[rows, columns] = jnp.where(mine, value, jnp.zeros_like(value))


def kv_kernel(core_ref, other_ref, owner_ref, order_ref, y_ref, x_ref, w_ref, *refs):
    outs, (cos_ref, sin_ref) = refs[:4], refs[4:]
    owners = begin(core_ref, other_ref, owner_ref, order_ref, cos_ref, sin_ref)
    both = jnp.concatenate([y_ref[...], x_ref[...]], axis=0)
    projected = jnp.dot(both, w_ref[...], preferred_element_type=jnp.float32)
    heads = w_ref.shape[1] // HD
    step = pl.program_id(0)

    @pl.when(step < 2 // heads)
    def _():
        for slot in range(2):
            rows = slice(slot * SLAB, (slot + 1) * SLAB)
            for h in range(heads):
                columns = slice(h * HD, (h + 1) * HD)
                value = rope(projected[rows, columns], slot, cos_ref, sin_ref).astype(jnp.bfloat16)
                store_masked(outs, owners[slot], rows, (step * heads + h) * HD, value)

    @pl.when(step >= 2 // heads)
    def _():
        for slot in range(2):
            rows = slice(slot * SLAB, (slot + 1) * SLAB)
            for h in range(heads):
                columns = slice(h * HD, (h + 1) * HD)
                value = projected[rows, columns].T.astype(jnp.bfloat16)
                store_masked(outs, owners[slot], rows, (step * heads + h) * HD, value)


def q_kernel(core_ref, other_ref, owner_ref, order_ref, y_ref, x_ref, w_ref, *refs):
    outs, (cos_ref, sin_ref) = refs[:8], refs[8:]
    owners = begin(core_ref, other_ref, owner_ref, order_ref, cos_ref, sin_ref)
    both = jnp.concatenate([y_ref[...], x_ref[...]], axis=0)
    projected = jnp.dot(both, w_ref[...], preferred_element_type=jnp.float32)
    heads = w_ref.shape[1] // HD
    for slot in range(2):
        for h in range(heads):
            columns = slice(h * HD, (h + 1) * HD)
            first = (pl.program_id(0) * heads + h) * HD
            block = projected[slot * SLAB : (slot + 1) * SLAB, columns]
            value = rope(block, slot, cos_ref, sin_ref).T.astype(jnp.bfloat16)
            store_masked(outs[4 * slot : 4 * slot + 4], owners[slot], slice(None), first, value)


def in_vmem(value):
    return pltpu.with_memory_space_constraint(value, pltpu.VMEM)


def in_hbm(value):
    return pltpu.with_memory_space_constraint(value, pltpu.HBM)


def project(kernel, core, owners, slab_order, others, rows, weight, block, blocks, width, out):
    depth = rows.shape[1]
    smem = pl.BlockSpec(memory_space=pltpu.SMEM)
    return pl.pallas_call(
        kernel,
        grid_spec=pltpu.PrefetchScalarGridSpec(
            num_scalar_prefetch=1,
            grid=(blocks,),
            in_specs=[
                smem,
                smem,
                smem,
                pl.BlockSpec(memory_space=pltpu.VMEM),
                pl.BlockSpec((SLAB, depth), lambda j, c: (0, 0)),
                pl.BlockSpec((depth, width), lambda j, c: (0, block(j, c[0]))),
            ],
            out_specs=[pl.BlockSpec(memory_space=pltpu.VMEM)] * len(out),
            scratch_shapes=[pltpu.VMEM((2, SLAB, HD), jnp.float32)] * 2,
        ),
        out_shape=out,
        compiler_params=pltpu.CompilerParams(
            dimension_semantics=("arbitrary",), vmem_limit_bytes=24 << 20
        ),
        cost_estimate=pl.CostEstimate(
            flops=4 * SLAB * depth * blocks * width,
            bytes_accessed=2 * depth * (2 * SLAB + blocks * width),
            transcendentals=0,
        ),
    )(core, *owners, in_hbm(slab_order), in_vmem(others), in_hbm(rows), in_hbm(weight))


FACTOR = HD**-0.5 * 1.4426950408889634
WIDE = GROUP * SLAB
HALF = Q_COLS // 2
STATE = ((2, HD, WIDE), (2, 8, WIDE), (2, 8, WIDE))
LOW, HIGH = (0, 1), (3, 2)


def collect(t, spots, pieces, sequence_ref, order_ref, kv):
    row = lax.axis_index("dp")
    column = lax.axis_index("cp")
    core, y, z = lax.rem(column, 2), lax.rem(column // 2, SIDE), column // (2 * SIDE)
    mine = column if t == 1 else column + 1 - 2 * core
    my_sequence, my_order = sequence_ref[row, mine], order_ref[row, mine]
    count = jnp.int32(0)
    for piece, (chips, second) in zip(pieces, spots):
        for b, k in enumerate(chips):
            sz = lax.rem(z + 2 * SIDE - jnp.where(core == 0, k, second), SIDE)
            sy = lax.rem(y + 2 * SIDE - jnp.where(core == 0, second, k), SIDE)
            for c in range(2):
                source = (sz * SIDE + sy) * 2 + (core if c == 1 else 1 - core)
                wanted = (sequence_ref[row, source] == my_sequence) & (
                    order_ref[row, source] < my_order
                )

                @pl.when(wanted)
                def _():
                    kv[count] = piece[(b * 2 + c) * SLAB : (b * 2 + c + 1) * SLAB, :]

                count = count + wanted.astype(jnp.int32)

    @pl.when(lax.rem(count, 2) == 1)
    def _():
        kv[count] = jnp.zeros((SLAB, 4 * HD), jnp.bfloat16)

    return count


def attend_slab(t, spots, pieces, parts, old, new, out, sequence_ref, order_ref, q_ref, kv, scores_ref):
    acc, peak, total = new
    first = old is None
    count = collect(t, spots, pieces, sequence_ref, order_ref, kv)
    pairs_here = (count + 1) // 2
    q_ref[...] = parts[0][...] + parts[1][...] + parts[2][...] + parts[3][...]
    starts = []
    for g in range(2):
        if first:
            key_row = lax.broadcasted_iota(jnp.int32, (SLAB, WIDE), 0)
            token = lax.rem(lax.broadcasted_iota(jnp.int32, (SLAB, WIDE), 1), SLAB)
            scores = jnp.dot(
                pieces[0][t * SLAB : (t + 1) * SLAB, g * HD : (g + 1) * HD],
                q_ref[:, g * WIDE : (g + 1) * WIDE],
                preferred_element_type=jnp.float32,
            )
            scores = jnp.where(key_row <= token, scores, NEG_FILL)
            scores_ref[8, g, :SLAB] = scores
            peak[g] = jnp.max(scores.reshape(SLAB // 8, 8, WIDE), axis=0)
        else:
            starts.append(jnp.max(old[1][g], axis=0, keepdims=True))
            peak[g] = old[1][g]

    def score(p, carry):
        full = 2 * p + 1 < count
        for g in range(2):
            keys = slice(g * HD, (g + 1) * HD)
            both = jnp.concatenate([kv[2 * p, :, keys], kv[2 * p + 1, :, keys]], axis=0)
            scores = jnp.dot(
                both, q_ref[:, g * WIDE : (g + 1) * WIDE], preferred_element_type=jnp.float32
            )
            low = scores[:SLAB]
            high = jnp.where(full, scores[SLAB:], NEG_FILL)
            scores_ref[p, g, :SLAB] = low
            scores_ref[p, g, SLAB:] = high
            top = jnp.maximum(low, high).reshape(SLAB // 8, 8, WIDE)
            peak[g] = jnp.maximum(peak[g], jnp.max(top, axis=0))
        return carry

    lax.fori_loop(0, pairs_here, score, 0)
    tops = []
    for g in range(2):
        top = jnp.max(peak[g], axis=0, keepdims=True)
        tops.append(top * FACTOR)
        if first:
            weights = jnp.exp2(scores_ref[8, g, :SLAB] * FACTOR - tops[g])
            total[g] = jnp.sum(weights.reshape(SLAB // 8, 8, WIDE), axis=0)
            acc[g] = jnp.dot(
                pieces[0][t * SLAB : (t + 1) * SLAB, (2 + g) * HD : (3 + g) * HD],
                weights.astype(jnp.bfloat16),
                preferred_element_type=jnp.float32,
            )
        else:
            rescale = jnp.exp2((starts[g] - top) * FACTOR)
            total[g] = old[2][g] * rescale
            acc[g] = old[0][g] * rescale

    def weigh(p, carry):
        for g in range(2):
            values = slice((2 + g) * HD, (3 + g) * HD)
            weights = jnp.exp2(scores_ref[p, g] * FACTOR - tops[g])
            total[g] = total[g] + jnp.sum(weights.reshape(SLAB // 4, 8, WIDE), axis=0)
            both = jnp.concatenate([kv[2 * p, :, values], kv[2 * p + 1, :, values]], axis=1)
            acc[g] = acc[g] + jnp.dot(
                both, weights.astype(jnp.bfloat16), preferred_element_type=jnp.float32
            )
        return carry

    lax.fori_loop(0, pairs_here, weigh, 0)
    if out is not None:
        for g in range(2):
            context = acc[g] / jnp.sum(total[g], axis=0, keepdims=True)
            for h in range(GROUP):
                head = g * GROUP + h
                out[:, head * HD : (head + 1) * HD] = context[:, h * SLAB : (h + 1) * SLAB].T.astype(
                    jnp.bfloat16
                )


def attend_kernel(jobs, spots, last, sequence_ref, order_ref, *refs):
    pieces, refs = refs[: len(spots)], refs[len(spots) :]
    given = []
    for t, start, first in jobs:
        parts, refs = refs[:4], refs[4:]
        old = None
        if not first:
            old, refs = refs[:3], refs[3:]
        given.append((parts, old))
    per = 1 if last else 3
    outs, refs = refs[: per * len(jobs)], refs[per * len(jobs) :]
    state, refs = (refs[:3], refs[3:]) if last else (None, refs)
    q_ref, kv, scores_ref = refs
    for n, (t, start, first) in enumerate(jobs):
        parts, old = given[n]
        new = state if last else outs[3 * n : 3 * n + 3]
        out = outs[n] if last else None
        attend_slab(
            t, spots[start:], pieces[start:], parts, old, new, out,
            sequence_ref, order_ref, q_ref, kv, scores_ref,
        )


def attend(jobs, slab_sequence, slab_order, items, parts, states, last):
    vmem = pl.BlockSpec(memory_space=pltpu.VMEM)
    smem = pl.BlockSpec(memory_space=pltpu.SMEM)
    scratch = [
        pltpu.VMEM((SLAB, HALF), jnp.bfloat16),
        pltpu.VMEM((16, SLAB, 4 * HD), jnp.bfloat16),
        pltpu.VMEM((9, 2, 2 * SLAB, WIDE), jnp.float32),
    ]
    operands = [v for v, _, _ in items]
    spots = [(chips, second) for _, chips, second in items]
    for t, start, first in jobs:
        operands += parts[t]
        if not first:
            operands += states[t]
    if last:
        out_shape = [pltpu.VMEM((SLAB, HALF), jnp.bfloat16)] * len(jobs)
        scratch = [pltpu.VMEM(s, jnp.float32) for s in STATE] + scratch
    else:
        out_shape = [pltpu.VMEM(s, jnp.float32) for s in STATE] * len(jobs)
    return pl.pallas_call(
        functools.partial(attend_kernel, jobs, spots, last),
        in_specs=[smem, smem] + [vmem] * len(operands),
        out_specs=[vmem] * len(out_shape),
        out_shape=out_shape,
        scratch_shapes=scratch,
        compiler_params=pltpu.CompilerParams(vmem_limit_bytes=28 << 20),
        cost_estimate=pl.CostEstimate(
            flops=2 * SLAB * len(spots) * 4 * SLAB * HALF,
            bytes_accessed=2 << 20,
            transcendentals=0,
        ),
    )(in_hbm(slab_sequence), in_hbm(slab_order), *[in_vmem(v) for v in operands])


def join_kernel(core_ref, kept_ref, received_ref, out_ref):
    core = core_ref[0]
    out_ref[:, pl.ds(pl.multiple_of(core * HALF, HALF), HALF)] = kept_ref[...]
    out_ref[:, pl.ds(pl.multiple_of((1 - core) * HALF, HALF), HALF)] = received_ref[...]


def join(core, kept, received):
    vmem = pl.BlockSpec(memory_space=pltpu.VMEM)
    return pl.pallas_call(
        join_kernel,
        in_specs=[pl.BlockSpec(memory_space=pltpu.SMEM), vmem, vmem],
        out_specs=vmem,
        out_shape=jax.ShapeDtypeStruct((SLAB, Q_COLS), jnp.bfloat16),
        compiler_params=pltpu.CompilerParams(vmem_limit_bytes=8 << 20),
        cost_estimate=pl.CostEstimate(flops=SLAB * Q_COLS, bytes_accessed=1 << 20, transcendentals=0),
        name="join",
    )(core, in_vmem(kept), in_vmem(received))


def local(tokens, qkv_weight, owner_slot, slab_sequence, slab_order):
    rows = tokens[0]
    core = lax.rem(lax.axis_index("cp"), 2)
    others = permute(rows, OTHER_CORE)
    owners = (permute(owner_slot, OTHER_CORE), owner_slot)
    common = (core.reshape(1), owners, slab_order, others, rows, qkv_weight)
    kv = project(
        kv_kernel, *common, lambda j, c: QH // 2 + 2 * j + c, 2, 2 * HD,
        [pltpu.VMEM((2 * SLAB, 4 * HD), jnp.bfloat16)] * 4,
    )
    queries = project(
        q_kernel, *common, lambda j, c: 2 * c + j, 2, 4 * HD,
        [pltpu.VMEM((SLAB, HALF), jnp.bfloat16)] * 8,
    )
    moved = [permute(kv[k], shift_x(k)) for k in (1, 3, 2)]
    parts = [[queries[0]] + [permute(queries[k], shift_x(k)) for k in (1, 3, 2)]]
    own = kv[0] + moved[0] + moved[1] + moved[2]
    first = [permute(own, shift_first(k)) for k in (1, 3, 2)]
    parts.append([queries[4]] + [permute(queries[4 + k], shift_x(k)) for k in (1, 3, 2)])
    low = jnp.concatenate([own, first[0]], axis=0)
    high = jnp.concatenate([first[1], first[2]], axis=0)
    left = [permute(v, shift_second(1)) for v in (low, high)]
    right = [permute(v, shift_second(3)) for v in (high, low)]
    far = [permute(left[0], shift_second(1)), permute(right[0], shift_second(3))]
    local_items = [(low, LOW, 0), (high, HIGH, 0)]
    near_items = [(left[0], LOW, 1), (left[1], HIGH, 1), (right[0], HIGH, 3), (right[1], LOW, 3)]
    far_items = [(far[0], LOW, 2), (far[1], HIGH, 2)]
    tables = (slab_sequence, slab_order)
    state = [None, None]
    for t in (0, 1):
        state[t] = attend([(t, 0, True)], *tables, local_items, parts, state, False)
    both = attend([(0, 0, False), (1, 0, False)], *tables, near_items, parts, state, False)
    state = [both[:3], both[3:]]
    sent, kept = attend([(0, 0, False), (1, 0, False)], *tables, far_items, parts, state, True)
    received = permute(sent, OTHER_CORE)
    return join(core.reshape(1), kept, received)[None]


def solution(mesh):
    in_specs = (P("dp", "cp", None), P(), P("dp", "cp"), P(), P())
    out_specs = P("dp", "cp", None)
    return jax.shard_map(local, mesh=mesh, in_specs=in_specs, out_specs=out_specs, check_vma=False)
```

```python
import functools

import jax
import jax.numpy as jnp
from jax import lax
from jax.experimental import pallas as pl
from jax.experimental.pallas import tpu as pltpu
from jax.sharding import PartitionSpec as P


QH = 16
KVH = 4
HD = 128
SLAB = 128
GROUP = QH // KVH
NEG_FILL = -1e30
AXES = ("dp", "cp")
SIDE = 4
Q_COLS = QH * HD


def pairs(move):
    out = []
    for x in range(SIDE):
        for z in range(SIDE):
            for y in range(SIDE):
                for c in range(2):
                    nx, nz, ny, nc = move(x, z, y, c)
                    here = x * 32 + (z * SIDE + y) * 2 + c
                    there = (nx % SIDE) * 32 + ((nz % SIDE) * SIDE + ny % SIDE) * 2 + nc % 2
                    out.append((here, there))
    return out


def shift_x(k):
    return pairs(lambda x, z, y, c: (x + k, z, y, c))


def shift_first(k):
    return pairs(lambda x, z, y, c: (x, z + k, y, c) if c == 0 else (x, z, y + k, c))


def shift_second(k):
    return pairs(lambda x, z, y, c: (x, z, y + k, c) if c == 0 else (x, z + k, y, c))


OTHER_CORE = pairs(lambda x, z, y, c: (x, z, y, c + 1))


def permute(value, table):
    return lax.ppermute(value, AXES, table)


def rope_tables(order, cos_ref, sin_ref):
    lane = lax.broadcasted_iota(jnp.int32, (SLAB, HD), 1)
    half = jnp.where(lane < HD // 2, lane, lane - HD // 2).astype(jnp.float32)
    frequency = jnp.exp(half * (-2.0 / HD * 13.122363377404328))
    row = lax.broadcasted_iota(jnp.int32, (SLAB, HD), 0)
    angle = (order * SLAB + row).astype(jnp.float32) * frequency
    cos_ref[...] = jnp.cos(angle)
    sine = jnp.sin(angle)
    sin_ref[...] = jnp.where(lane < HD // 2, -sine, sine)


def rope(block, table):
    return block * table[0][...] + pltpu.roll(block, HD // 2, 1) * table[1][...]


CHUNKS = 4


def prepare_kernel(core_ref, owner_ref, order_ref, x_ref, w_ref, *refs):
    x_out, w_out, cos_ref, sin_ref, sems = refs
    core = core_ref[0]
    width = 2 * HD
    rows = w_out.shape[0] // CHUNKS
    copies = [pltpu.make_async_copy(x_ref, x_out, sems.at[2 * CHUNKS])]
    for part in range(2):
        base = pl.multiple_of((QH + part * KVH) * HD + core * width, width)
        for n in range(CHUNKS):
            piece = pl.ds(n * rows, rows)
            copies.append(
                pltpu.make_async_copy(
                    w_ref.at[piece, pl.ds(base, width)],
                    w_out.at[piece, part * width : (part + 1) * width],
                    sems.at[part * CHUNKS + n],
                )
            )
    for copy in copies:
        copy.start()
    rope_tables(order_ref[owner_ref[0, 0], lax.axis_index("cp")], cos_ref, sin_ref)
    for copy in copies:
        copy.wait()


def prepare(core, owner, slab_order, rows, weight):
    smem = pl.BlockSpec(memory_space=pltpu.SMEM)
    anywhere = pl.BlockSpec(memory_space=pl.ANY)
    vmem = pl.BlockSpec(memory_space=pltpu.VMEM)
    depth = rows.shape[1]
    return pl.pallas_call(
        prepare_kernel,
        in_specs=[smem] * 3 + [anywhere] * 2,
        out_specs=[vmem] * 4,
        out_shape=[
            pltpu.VMEM(rows.shape, rows.dtype),
            pltpu.VMEM((depth, 4 * HD), weight.dtype),
            pltpu.VMEM((SLAB, HD), jnp.float32),
            pltpu.VMEM((SLAB, HD), jnp.float32),
        ],
        scratch_shapes=[pltpu.SemaphoreType.DMA((2 * CHUNKS + 1,))],
        compiler_params=pltpu.CompilerParams(vmem_limit_bytes=8 << 20),
        cost_estimate=pl.CostEstimate(flops=1 << 26, bytes_accessed=5 << 20, transcendentals=1 << 16),
        name="prepare",
    )(core, owner, in_hbm(slab_order), in_hbm(rows), in_hbm(weight))


def store_masked(outs, owner, rows, first, value):
    my_row = lax.axis_index("dp")
    columns = pl.ds(first if isinstance(first, int) else pl.multiple_of(first, HD), HD)
    for k, out in enumerate(outs):
        mine = owner == lax.rem(my_row + k, SIDE)
        out[rows, columns] = jnp.where(mine, value, jnp.zeros_like(value))


def kv_kernel(core_ref, other_ref, owner_ref, order_ref, y_ref, x_ref, w_ref, *refs):
    ropes, outs = (refs[2:4], refs[:2]), refs[4:]
    column = lax.axis_index("cp") + 1 - 2 * core_ref[0]
    rope_tables(order_ref[other_ref[0, 0], column], *ropes[0])
    owners = (other_ref[0, 0], owner_ref[0, 0])
    both = jnp.concatenate([y_ref[...], x_ref[...]], axis=0)
    wide = 512
    for first in range(0, 4 * HD, wide):
        projected = jnp.dot(
            both, w_ref[:, first : first + wide], preferred_element_type=jnp.float32
        )
        for slot in range(2):
            rows = slice(slot * SLAB, (slot + 1) * SLAB)
            for h in range(wide // HD):
                block = projected[rows, h * HD : (h + 1) * HD]
                if first + h * HD < 2 * HD:
                    value = rope(block, ropes[slot]).astype(jnp.bfloat16)
                else:
                    value = block.T.astype(jnp.bfloat16)
                store_masked(outs, owners[slot], rows, first + h * HD, value)


def q_kernel(core_ref, other_ref, owner_ref, w_ref, y_ref, x_ref, *refs):
    ropes, outs = (refs[:2], refs[2:4]), refs[4:12]
    w_scr, sems = refs[12:]
    owners = (other_ref[0, 0], owner_ref[0, 0])
    depth, width = w_scr.shape[1:]
    rows = depth // CHUNKS
    copies = []
    for part in range(QPARTS):
        base = pl.multiple_of(core_ref[0] * HALF + part * width, width)
        for n in range(CHUNKS):
            piece = pl.ds(n * rows, rows)
            copies.append(
                pltpu.make_async_copy(
                    w_ref.at[piece, pl.ds(base, width)],
                    w_scr.at[part, piece, :],
                    sems.at[part * CHUNKS + n],
                )
            )
    for copy in copies:
        copy.start()
    for part in range(QPARTS):
        for copy in copies[part * CHUNKS : (part + 1) * CHUNKS]:
            copy.wait()
        both = jnp.concatenate([y_ref[...], x_ref[...]], axis=0)
        projected = jnp.dot(both, w_scr[part], preferred_element_type=jnp.float32)
        for slot in range(2):
            for h in range(width // HD):
                block = projected[slot * SLAB : (slot + 1) * SLAB, h * HD : (h + 1) * HD]
                value = rope(block, ropes[slot]).T.astype(jnp.bfloat16)
                store_masked(
                    outs[4 * slot : 4 * slot + 4], owners[slot], slice(None), part * width + h * HD, value
                )


def in_vmem(value):
    return pltpu.with_memory_space_constraint(value, pltpu.VMEM)


def in_hbm(value):
    return pltpu.with_memory_space_constraint(value, pltpu.HBM)


def project_kv(core, owners, slab_order, others, rows, weight, tables):
    smem = pl.BlockSpec(memory_space=pltpu.SMEM)
    vmem = pl.BlockSpec(memory_space=pltpu.VMEM)
    operands = [in_vmem(v) for v in (others, rows, weight, *tables)]
    return pl.pallas_call(
        kv_kernel,
        in_specs=[smem] * 4 + [vmem] * len(operands),
        out_specs=[vmem] * 6,
        out_shape=[pltpu.VMEM((SLAB, HD), jnp.float32)] * 2
        + [pltpu.VMEM((2 * SLAB, 4 * HD), jnp.bfloat16)] * 4,
        compiler_params=pltpu.CompilerParams(vmem_limit_bytes=24 << 20),
        cost_estimate=pl.CostEstimate(
            flops=4 * SLAB * rows.shape[1] * 4 * HD, bytes_accessed=4 << 20, transcendentals=0
        ),
        name="kv_proj",
    )(core, *owners, in_hbm(slab_order), *operands)


QPARTS = 2


def project_q(core, owners, others, rows, weight, tables):
    depth, width = rows.shape[1], HALF // QPARTS
    smem = pl.BlockSpec(memory_space=pltpu.SMEM)
    vmem = pl.BlockSpec(memory_space=pltpu.VMEM)
    operands = [in_vmem(v) for v in (others, rows, *tables)]
    return pl.pallas_call(
        q_kernel,
        in_specs=[smem] * 3 + [pl.BlockSpec(memory_space=pl.ANY)] + [vmem] * len(operands),
        out_specs=[vmem] * 8,
        out_shape=[pltpu.VMEM((SLAB, HALF), jnp.bfloat16)] * 8,
        scratch_shapes=[
            pltpu.VMEM((QPARTS, depth, width), weight.dtype),
            pltpu.SemaphoreType.DMA((QPARTS * CHUNKS,)),
        ],
        compiler_params=pltpu.CompilerParams(vmem_limit_bytes=28 << 20),
        cost_estimate=pl.CostEstimate(
            flops=4 * SLAB * depth * HALF, bytes_accessed=2 * depth * HALF, transcendentals=0
        ),
        name="q_proj",
    )(core, *owners, in_hbm(weight), *operands)


FACTOR = HD**-0.5 * 1.4426950408889634
WIDE = GROUP * SLAB
HALF = Q_COLS // 2
STATE = ((2, HD, WIDE), (2, 8, WIDE), (2, 8, WIDE))
LOW, HIGH = (0, 1), (3, 2)


def collect(t, spots, pieces, sequence_ref, order_ref, kv):
    row = lax.axis_index("dp")
    column = lax.axis_index("cp")
    core, y, z = lax.rem(column, 2), lax.rem(column // 2, SIDE), column // (2 * SIDE)
    mine = column if t == 1 else column + 1 - 2 * core
    my_sequence, my_order = sequence_ref[row, mine], order_ref[row, mine]
    count = jnp.int32(0)
    for piece, (chips, second) in zip(pieces, spots):
        for b, k in enumerate(chips):
            sz = lax.rem(z + 2 * SIDE - jnp.where(core == 0, k, second), SIDE)
            sy = lax.rem(y + 2 * SIDE - jnp.where(core == 0, second, k), SIDE)
            for c in range(2):
                source = (sz * SIDE + sy) * 2 + (core if c == 1 else 1 - core)
                wanted = (sequence_ref[row, source] == my_sequence) & (
                    order_ref[row, source] < my_order
                )

                @pl.when(wanted)
                def _():
                    kv[count] = piece[(b * 2 + c) * SLAB : (b * 2 + c + 1) * SLAB, :]

                count = count + wanted.astype(jnp.int32)

    @pl.when(lax.rem(count, 2) == 1)
    def _():
        kv[count] = jnp.zeros((SLAB, 4 * HD), jnp.bfloat16)

    return count


def attend_slab(t, spots, pieces, parts, old, new, out, sequence_ref, order_ref, q_ref, kv, scores_ref):
    acc, peak, total = new
    first = old is None
    count = collect(t, spots, pieces, sequence_ref, order_ref, kv)
    pairs_here = (count + 1) // 2
    q_ref[...] = parts[0][...] + parts[1][...] + parts[2][...] + parts[3][...]
    starts = []
    for g in range(2):
        if first:
            key_row = lax.broadcasted_iota(jnp.int32, (SLAB, WIDE), 0)
            token = lax.rem(lax.broadcasted_iota(jnp.int32, (SLAB, WIDE), 1), SLAB)
            scores = jnp.dot(
                pieces[0][t * SLAB : (t + 1) * SLAB, g * HD : (g + 1) * HD],
                q_ref[:, g * WIDE : (g + 1) * WIDE],
                preferred_element_type=jnp.float32,
            )
            scores = jnp.where(key_row <= token, scores, NEG_FILL)
            scores_ref[8, g, :SLAB] = scores
            peak[g] = jnp.max(scores.reshape(SLAB // 8, 8, WIDE), axis=0)
        else:
            starts.append(jnp.max(old[1][g], axis=0, keepdims=True))
            peak[g] = old[1][g]

    def score(p, carry):
        full = 2 * p + 1 < count
        for g in range(2):
            keys = slice(g * HD, (g + 1) * HD)
            both = jnp.concatenate([kv[2 * p, :, keys], kv[2 * p + 1, :, keys]], axis=0)
            scores = jnp.dot(
                both, q_ref[:, g * WIDE : (g + 1) * WIDE], preferred_element_type=jnp.float32
            )
            low = scores[:SLAB]
            high = jnp.where(full, scores[SLAB:], NEG_FILL)
            scores_ref[p, g, :SLAB] = low
            scores_ref[p, g, SLAB:] = high
            top = jnp.maximum(low, high).reshape(SLAB // 8, 8, WIDE)
            peak[g] = jnp.maximum(peak[g], jnp.max(top, axis=0))
        return carry

    lax.fori_loop(0, pairs_here, score, 0)
    tops = []
    for g in range(2):
        top = jnp.max(peak[g], axis=0, keepdims=True)
        tops.append(top * FACTOR)
        if first:
            weights = jnp.exp2(scores_ref[8, g, :SLAB] * FACTOR - tops[g])
            total[g] = jnp.sum(weights.reshape(SLAB // 8, 8, WIDE), axis=0)
            acc[g] = jnp.dot(
                pieces[0][t * SLAB : (t + 1) * SLAB, (2 + g) * HD : (3 + g) * HD],
                weights.astype(jnp.bfloat16),
                preferred_element_type=jnp.float32,
            )
        else:
            rescale = jnp.exp2((starts[g] - top) * FACTOR)
            total[g] = old[2][g] * rescale
            acc[g] = old[0][g] * rescale

    def weigh(p, carry):
        for g in range(2):
            values = slice((2 + g) * HD, (3 + g) * HD)
            weights = jnp.exp2(scores_ref[p, g] * FACTOR - tops[g])
            total[g] = total[g] + jnp.sum(weights.reshape(SLAB // 4, 8, WIDE), axis=0)
            both = jnp.concatenate([kv[2 * p, :, values], kv[2 * p + 1, :, values]], axis=1)
            acc[g] = acc[g] + jnp.dot(
                both, weights.astype(jnp.bfloat16), preferred_element_type=jnp.float32
            )
        return carry

    lax.fori_loop(0, pairs_here, weigh, 0)
    if out is not None:
        for g in range(2):
            context = acc[g] / jnp.sum(total[g], axis=0, keepdims=True)
            for h in range(GROUP):
                head = g * GROUP + h
                out[:, head * HD : (head + 1) * HD] = context[:, h * SLAB : (h + 1) * SLAB].T.astype(
                    jnp.bfloat16
                )


def attend_kernel(jobs, spots, last, sequence_ref, order_ref, *refs):
    pieces, refs = refs[: len(spots)], refs[len(spots) :]
    given = []
    for t, start, first in jobs:
        parts, refs = refs[:4], refs[4:]
        old = None
        if not first:
            old, refs = refs[:3], refs[3:]
        given.append((parts, old))
    per = 1 if last else 3
    outs, refs = refs[: per * len(jobs)], refs[per * len(jobs) :]
    state, refs = (refs[:3], refs[3:]) if last else (None, refs)
    q_ref, kv, scores_ref = refs
    for n, (t, start, first) in enumerate(jobs):
        parts, old = given[n]
        new = state if last else outs[3 * n : 3 * n + 3]
        out = outs[n] if last else None
        attend_slab(
            t, spots[start:], pieces[start:], parts, old, new, out,
            sequence_ref, order_ref, q_ref, kv, scores_ref,
        )


def attend(jobs, slab_sequence, slab_order, items, parts, states, last):
    vmem = pl.BlockSpec(memory_space=pltpu.VMEM)
    smem = pl.BlockSpec(memory_space=pltpu.SMEM)
    scratch = [
        pltpu.VMEM((SLAB, HALF), jnp.bfloat16),
        pltpu.VMEM((16, SLAB, 4 * HD), jnp.bfloat16),
        pltpu.VMEM((9, 2, 2 * SLAB, WIDE), jnp.float32),
    ]
    operands = [v for v, _, _ in items]
    spots = [(chips, second) for _, chips, second in items]
    for t, start, first in jobs:
        operands += parts[t]
        if not first:
            operands += states[t]
    if last:
        out_shape = [pltpu.VMEM((SLAB, HALF), jnp.bfloat16)] * len(jobs)
        scratch = [pltpu.VMEM(s, jnp.float32) for s in STATE] + scratch
    else:
        out_shape = [pltpu.VMEM(s, jnp.float32) for s in STATE] * len(jobs)
    return pl.pallas_call(
        functools.partial(attend_kernel, jobs, spots, last),
        in_specs=[smem, smem] + [vmem] * len(operands),
        out_specs=[vmem] * len(out_shape),
        out_shape=out_shape,
        scratch_shapes=scratch,
        compiler_params=pltpu.CompilerParams(vmem_limit_bytes=28 << 20),
        cost_estimate=pl.CostEstimate(
            flops=2 * SLAB * len(spots) * 4 * SLAB * HALF,
            bytes_accessed=2 << 20,
            transcendentals=0,
        ),
    )(in_hbm(slab_sequence), in_hbm(slab_order), *[in_vmem(v) for v in operands])


def join_kernel(core_ref, kept_ref, received_ref, out_ref):
    core = core_ref[0]
    out_ref[:, pl.ds(pl.multiple_of(core * HALF, HALF), HALF)] = kept_ref[...]
    out_ref[:, pl.ds(pl.multiple_of((1 - core) * HALF, HALF), HALF)] = received_ref[...]


def join(core, kept, received):
    vmem = pl.BlockSpec(memory_space=pltpu.VMEM)
    return pl.pallas_call(
        join_kernel,
        in_specs=[pl.BlockSpec(memory_space=pltpu.SMEM), vmem, vmem],
        out_specs=vmem,
        out_shape=jax.ShapeDtypeStruct((SLAB, Q_COLS), jnp.bfloat16),
        compiler_params=pltpu.CompilerParams(vmem_limit_bytes=8 << 20),
        cost_estimate=pl.CostEstimate(flops=SLAB * Q_COLS, bytes_accessed=1 << 20, transcendentals=0),
        name="join",
    )(core, in_vmem(kept), in_vmem(received))


def local(tokens, qkv_weight, owner_slot, slab_sequence, slab_order):
    rows = tokens[0]
    core = lax.rem(lax.axis_index("cp"), 2)
    others = permute(rows, OTHER_CORE)
    owners = (permute(owner_slot, OTHER_CORE), owner_slot)
    core = core.reshape(1)
    rows, kv_weight, *tables = prepare(core, owner_slot, slab_order, rows, qkv_weight)
    other_cos, other_sin, *kv = project_kv(
        core, owners, slab_order, others, rows, kv_weight, tables
    )
    tables = (other_cos, other_sin, *tables)
    queries = project_q(core, owners, others, rows, qkv_weight, tables)
    moved = [permute(kv[k], shift_x(k)) for k in (1, 3, 2)]
    parts = [[queries[0]] + [permute(queries[k], shift_x(k)) for k in (1, 3, 2)]]
    own = kv[0] + moved[0] + moved[1] + moved[2]
    first = [permute(own, shift_first(k)) for k in (1, 3, 2)]
    parts.append([queries[4]] + [permute(queries[4 + k], shift_x(k)) for k in (1, 3, 2)])
    low = jnp.concatenate([own, first[0]], axis=0)
    high = jnp.concatenate([first[1], first[2]], axis=0)
    left = [permute(v, shift_second(1)) for v in (low, high)]
    right = [permute(v, shift_second(3)) for v in (high, low)]
    far = [permute(left[0], shift_second(1)), permute(right[0], shift_second(3))]
    local_items = [(low, LOW, 0), (high, HIGH, 0)]
    near_items = [(left[0], LOW, 1), (left[1], HIGH, 1), (right[0], HIGH, 3), (right[1], LOW, 3)]
    far_items = [(far[0], LOW, 2), (far[1], HIGH, 2)]
    tables = (slab_sequence, slab_order)
    state = [None, None]
    for t in (0, 1):
        state[t] = attend([(t, 0, True)], *tables, local_items, parts, state, False)
    both = attend([(0, 0, False), (1, 0, False)], *tables, near_items, parts, state, False)
    state = [both[:3], both[3:]]
    sent, kept = attend([(0, 0, False), (1, 0, False)], *tables, far_items, parts, state, True)
    received = permute(sent, OTHER_CORE)
    return join(core, kept, received)[None]


def solution(mesh):
    in_specs = (P("dp", "cp", None), P(), P("dp", "cp"), P(), P())
    out_specs = P("dp", "cp", None)
    return jax.shard_map(local, mesh=mesh, in_specs=in_specs, out_specs=out_specs, check_vma=False)
```

```python
import functools

import jax
import jax.numpy as jnp
from jax import lax
from jax.experimental import pallas as pl
from jax.experimental.pallas import tpu as pltpu
from jax.sharding import PartitionSpec as P


QH = 16
KVH = 4
HD = 128
SLAB = 128
GROUP = QH // KVH
NEG_FILL = -1e30
AXES = ("dp", "cp")
SIDE = 4
Q_COLS = QH * HD


def pairs(move):
    out = []
    for x in range(SIDE):
        for z in range(SIDE):
            for y in range(SIDE):
                for c in range(2):
                    nx, nz, ny, nc = move(x, z, y, c)
                    here = x * 32 + (z * SIDE + y) * 2 + c
                    there = (nx % SIDE) * 32 + ((nz % SIDE) * SIDE + ny % SIDE) * 2 + nc % 2
                    out.append((here, there))
    return out


def shift_x(k):
    return pairs(lambda x, z, y, c: (x + k, z, y, c))


def shift_first(k):
    return pairs(lambda x, z, y, c: (x, z + k, y, c) if c == 0 else (x, z, y + k, c))


def shift_second(k):
    return pairs(lambda x, z, y, c: (x, z, y + k, c) if c == 0 else (x, z + k, y, c))


OTHER_CORE = pairs(lambda x, z, y, c: (x, z, y, c + 1))


def permute(value, table):
    return lax.ppermute(value, AXES, table)


def rope_tables(order, cos_ref, sin_ref):
    half_rows = SLAB // 2
    lane = lax.broadcasted_iota(jnp.int32, (half_rows, HD), 1)
    row = lax.broadcasted_iota(jnp.int32, (half_rows, HD), 0)
    left = lane < HD // 2
    index = jnp.where(left, lane, lane - HD // 2).astype(jnp.float32)
    frequency = jnp.exp(index * (-2.0 / HD * 13.122363377404328))
    token = jnp.where(left, row, row + half_rows)
    angle = (order * SLAB + token).astype(jnp.float32) * frequency
    for value, ref, sign in ((jnp.cos(angle), cos_ref, 1.0), (jnp.sin(angle), sin_ref, -1.0)):
        turned = pltpu.roll(value, HD // 2, 1)
        ref[:half_rows] = jnp.where(left, sign * value, turned)
        ref[half_rows:] = jnp.where(left, sign * turned, value)


def rope(block, table):
    return block * table[0][...] + pltpu.roll(block, HD // 2, 1) * table[1][...]


CHUNKS = 4


def prepare_kernel(core_ref, other_ref, owner_ref, order_ref, x_ref, w_ref, *refs):
    x_out, w_out = refs[:2]
    sems = refs[6]
    core = core_ref[0]
    width = 2 * HD
    rows = w_out.shape[0] // CHUNKS
    copies = [pltpu.make_async_copy(x_ref, x_out, sems.at[2 * CHUNKS])]
    for part in range(2):
        base = pl.multiple_of((QH + part * KVH) * HD + core * width, width)
        for n in range(CHUNKS):
            piece = pl.ds(n * rows, rows)
            copies.append(
                pltpu.make_async_copy(
                    w_ref.at[piece, pl.ds(base, width)],
                    w_out.at[piece, part * width : (part + 1) * width],
                    sems.at[part * CHUNKS + n],
                )
            )
    for copy in copies:
        copy.start()
    column = lax.axis_index("cp")
    rope_tables(order_ref[other_ref[0, 0], column + 1 - 2 * core], *refs[2:4])
    rope_tables(order_ref[owner_ref[0, 0], column], *refs[4:6])
    for copy in copies:
        copy.wait()


def prepare(core, owners, slab_order, rows, weight):
    smem = pl.BlockSpec(memory_space=pltpu.SMEM)
    anywhere = pl.BlockSpec(memory_space=pl.ANY)
    vmem = pl.BlockSpec(memory_space=pltpu.VMEM)
    depth = rows.shape[1]
    return pl.pallas_call(
        prepare_kernel,
        in_specs=[smem] * 4 + [anywhere] * 2,
        out_specs=[vmem] * 6,
        out_shape=[
            pltpu.VMEM(rows.shape, rows.dtype),
            pltpu.VMEM((depth, 4 * HD), weight.dtype),
        ]
        + [pltpu.VMEM((SLAB, HD), jnp.float32)] * 4,
        scratch_shapes=[pltpu.SemaphoreType.DMA((2 * CHUNKS + 1,))],
        compiler_params=pltpu.CompilerParams(vmem_limit_bytes=8 << 20),
        cost_estimate=pl.CostEstimate(flops=1 << 26, bytes_accessed=5 << 20, transcendentals=1 << 16),
        name="prepare",
    )(core, *owners, in_hbm(slab_order), in_hbm(rows), in_hbm(weight))


def store_masked(outs, owner, rows, first, value):
    my_row = lax.axis_index("dp")
    columns = pl.ds(first if isinstance(first, int) else pl.multiple_of(first, HD), HD)
    for k, out in enumerate(outs):
        mine = owner == lax.rem(my_row + k, SIDE)
        out[rows, columns] = jnp.where(mine, value, jnp.zeros_like(value))


def kv_kernel(other_ref, owner_ref, y_ref, x_ref, w_ref, *refs):
    ropes, outs = (refs[:2], refs[2:4]), refs[4:]
    owners = (other_ref[0, 0], owner_ref[0, 0])
    both = jnp.concatenate([y_ref[...], x_ref[...]], axis=0)
    wide = 512
    for first in range(0, 4 * HD, wide):
        projected = jnp.dot(
            both, w_ref[:, first : first + wide], preferred_element_type=jnp.float32
        )
        for slot in range(2):
            rows = slice(slot * SLAB, (slot + 1) * SLAB)
            for h in range(wide // HD):
                block = projected[rows, h * HD : (h + 1) * HD]
                if first + h * HD < 2 * HD:
                    value = rope(block, ropes[slot]).astype(jnp.bfloat16)
                else:
                    value = block.T.astype(jnp.bfloat16)
                store_masked(outs, owners[slot], rows, first + h * HD, value)


def q_kernel(core_ref, other_ref, owner_ref, w_ref, y_ref, x_ref, *refs):
    ropes, outs = (refs[:2], refs[2:4]), refs[4:12]
    w_scr, sems = refs[12:]
    owners = (other_ref[0, 0], owner_ref[0, 0])
    depth, width = w_scr.shape[1:]
    rows = depth // CHUNKS
    copies = []
    for part in range(QPARTS):
        base = pl.multiple_of(core_ref[0] * HALF + part * width, width)
        for n in range(CHUNKS):
            piece = pl.ds(n * rows, rows)
            copies.append(
                pltpu.make_async_copy(
                    w_ref.at[piece, pl.ds(base, width)],
                    w_scr.at[part, piece, :],
                    sems.at[part * CHUNKS + n],
                )
            )
    for copy in copies:
        copy.start()
    for part in range(QPARTS):
        for copy in copies[part * CHUNKS : (part + 1) * CHUNKS]:
            copy.wait()
        both = jnp.concatenate([y_ref[...], x_ref[...]], axis=0)
        projected = jnp.dot(both, w_scr[part], preferred_element_type=jnp.float32)
        for slot in range(2):
            for h in range(width // HD):
                block = projected[slot * SLAB : (slot + 1) * SLAB, h * HD : (h + 1) * HD]
                value = rope(block, ropes[slot]).T.astype(jnp.bfloat16)
                store_masked(
                    outs[4 * slot : 4 * slot + 4], owners[slot], slice(None), part * width + h * HD, value
                )


def in_vmem(value):
    return pltpu.with_memory_space_constraint(value, pltpu.VMEM)


def in_hbm(value):
    return pltpu.with_memory_space_constraint(value, pltpu.HBM)


def project_kv(owners, others, rows, weight, tables):
    smem = pl.BlockSpec(memory_space=pltpu.SMEM)
    vmem = pl.BlockSpec(memory_space=pltpu.VMEM)
    operands = [in_vmem(v) for v in (others, rows, weight, *tables)]
    return pl.pallas_call(
        kv_kernel,
        in_specs=[smem] * 2 + [vmem] * len(operands),
        out_specs=[vmem] * 4,
        out_shape=[pltpu.VMEM((2 * SLAB, 4 * HD), jnp.bfloat16)] * 4,
        compiler_params=pltpu.CompilerParams(vmem_limit_bytes=24 << 20),
        cost_estimate=pl.CostEstimate(
            flops=4 * SLAB * rows.shape[1] * 4 * HD, bytes_accessed=4 << 20, transcendentals=0
        ),
        name="kv_proj",
    )(*owners, *operands)


QPARTS = 2


def project_q(core, owners, others, rows, weight, tables):
    depth, width = rows.shape[1], HALF // QPARTS
    smem = pl.BlockSpec(memory_space=pltpu.SMEM)
    vmem = pl.BlockSpec(memory_space=pltpu.VMEM)
    operands = [in_vmem(v) for v in (others, rows, *tables)]
    return pl.pallas_call(
        q_kernel,
        in_specs=[smem] * 3 + [pl.BlockSpec(memory_space=pl.ANY)] + [vmem] * len(operands),
        out_specs=[vmem] * 8,
        out_shape=[pltpu.VMEM((SLAB, HALF), jnp.bfloat16)] * 8,
        scratch_shapes=[
            pltpu.VMEM((QPARTS, depth, width), weight.dtype),
            pltpu.SemaphoreType.DMA((QPARTS * CHUNKS,)),
        ],
        compiler_params=pltpu.CompilerParams(vmem_limit_bytes=28 << 20),
        cost_estimate=pl.CostEstimate(
            flops=4 * SLAB * depth * HALF, bytes_accessed=2 * depth * HALF, transcendentals=0
        ),
        name="q_proj",
    )(core, *owners, in_hbm(weight), *operands)


FACTOR = HD**-0.5 * 1.4426950408889634
WIDE = GROUP * SLAB
HALF = Q_COLS // 2
STATE = ((2, HD, WIDE), (2, 8, WIDE), (2, 8, WIDE))
LOW, HIGH = (0, 1), (3, 2)


def collect(t, spots, pieces, sequence_ref, order_ref, kv):
    row = lax.axis_index("dp")
    column = lax.axis_index("cp")
    core, y, z = lax.rem(column, 2), lax.rem(column // 2, SIDE), column // (2 * SIDE)
    mine = column if t == 1 else column + 1 - 2 * core
    my_sequence, my_order = sequence_ref[row, mine], order_ref[row, mine]
    count = jnp.int32(0)
    for piece, (chips, second) in zip(pieces, spots):
        for b, k in enumerate(chips):
            sz = lax.rem(z + 2 * SIDE - jnp.where(core == 0, k, second), SIDE)
            sy = lax.rem(y + 2 * SIDE - jnp.where(core == 0, second, k), SIDE)
            for c in range(2):
                source = (sz * SIDE + sy) * 2 + (core if c == 1 else 1 - core)
                wanted = (sequence_ref[row, source] == my_sequence) & (
                    order_ref[row, source] < my_order
                )

                @pl.when(wanted)
                def _():
                    kv[count] = piece[(b * 2 + c) * SLAB : (b * 2 + c + 1) * SLAB, :]

                count = count + wanted.astype(jnp.int32)

    @pl.when(lax.rem(count, 2) == 1)
    def _():
        kv[count] = jnp.zeros((SLAB, 4 * HD), jnp.bfloat16)

    return count


def attend_slab(t, spots, pieces, parts, old, new, out, sequence_ref, order_ref, kv, scores_ref):
    acc, peak, total = new[:3]
    first = old is None
    if first:
        q_ref = new[3]
        q_ref[...] = parts[0][...] + parts[1][...] + parts[2][...] + parts[3][...]
    else:
        (q_ref,) = parts
    count = collect(t, spots, pieces, sequence_ref, order_ref, kv)
    pairs_here = (count + 1) // 2
    starts = []
    for g in range(2):
        if first:
            key_row = lax.broadcasted_iota(jnp.int32, (SLAB, WIDE), 0)
            token = lax.rem(lax.broadcasted_iota(jnp.int32, (SLAB, WIDE), 1), SLAB)
            scores = jnp.dot(
                pieces[0][t * SLAB : (t + 1) * SLAB, g * HD : (g + 1) * HD],
                q_ref[:, g * WIDE : (g + 1) * WIDE],
                preferred_element_type=jnp.float32,
            )
            scores = jnp.where(key_row <= token, scores, NEG_FILL)
            scores_ref[8, g, :SLAB] = scores
            peak[g] = jnp.max(scores.reshape(SLAB // 8, 8, WIDE), axis=0)
        else:
            starts.append(jnp.max(old[1][g], axis=0, keepdims=True))
            peak[g] = old[1][g]

    def score(p, carry):
        full = 2 * p + 1 < count
        for g in range(2):
            keys = slice(g * HD, (g + 1) * HD)
            both = jnp.concatenate([kv[2 * p, :, keys], kv[2 * p + 1, :, keys]], axis=0)
            scores = jnp.dot(
                both, q_ref[:, g * WIDE : (g + 1) * WIDE], preferred_element_type=jnp.float32
            )
            low = scores[:SLAB]
            high = jnp.where(full, scores[SLAB:], NEG_FILL)
            scores_ref[p, g, :SLAB] = low
            scores_ref[p, g, SLAB:] = high
            top = jnp.maximum(low, high).reshape(SLAB // 8, 8, WIDE)
            peak[g] = jnp.maximum(peak[g], jnp.max(top, axis=0))
        return carry

    lax.fori_loop(0, pairs_here, score, 0)
    tops = []
    for g in range(2):
        top = jnp.max(peak[g], axis=0, keepdims=True)
        tops.append(top * FACTOR)
        if first:
            weights = jnp.exp2(scores_ref[8, g, :SLAB] * FACTOR - tops[g])
            total[g] = jnp.sum(weights.reshape(SLAB // 8, 8, WIDE), axis=0)
            acc[g] = jnp.dot(
                pieces[0][t * SLAB : (t + 1) * SLAB, (2 + g) * HD : (3 + g) * HD],
                weights.astype(jnp.bfloat16),
                preferred_element_type=jnp.float32,
            )
        else:
            rescale = jnp.exp2((starts[g] - top) * FACTOR)
            total[g] = old[2][g] * rescale
            acc[g] = old[0][g] * rescale

    def weigh(p, carry):
        for g in range(2):
            values = slice((2 + g) * HD, (3 + g) * HD)
            weights = jnp.exp2(scores_ref[p, g] * FACTOR - tops[g])
            total[g] = total[g] + jnp.sum(weights.reshape(SLAB // 4, 8, WIDE), axis=0)
            both = jnp.concatenate([kv[2 * p, :, values], kv[2 * p + 1, :, values]], axis=1)
            acc[g] = acc[g] + jnp.dot(
                both, weights.astype(jnp.bfloat16), preferred_element_type=jnp.float32
            )
        return carry

    lax.fori_loop(0, pairs_here, weigh, 0)
    if out is not None:
        for g in range(2):
            context = acc[g] / jnp.sum(total[g], axis=0, keepdims=True)
            for h in range(GROUP):
                head = g * GROUP + h
                out[:, head * HD : (head + 1) * HD] = context[:, h * SLAB : (h + 1) * SLAB].T.astype(
                    jnp.bfloat16
                )


def attend_kernel(jobs, spots, last, sequence_ref, order_ref, *refs):
    pieces, refs = refs[: len(spots)], refs[len(spots) :]
    given = []
    for t, start, first in jobs:
        parts, refs = (refs[:4], refs[4:]) if first else (refs[:1], refs[1:])
        old = None
        if not first:
            old, refs = refs[:3], refs[3:]
        given.append((parts, old))
    per = 1 if last else 4 if jobs[0][2] else 3
    outs, refs = refs[: per * len(jobs)], refs[per * len(jobs) :]
    state, refs = (refs[:3], refs[3:]) if last else (None, refs)
    kv, scores_ref = refs
    for n, (t, start, first) in enumerate(jobs):
        parts, old = given[n]
        new = state if last else outs[per * n : per * n + per]
        out = outs[n] if last else None
        attend_slab(
            t, spots[start:], pieces[start:], parts, old, new, out,
            sequence_ref, order_ref, kv, scores_ref,
        )


def attend(jobs, slab_sequence, slab_order, items, parts, states, last):
    vmem = pl.BlockSpec(memory_space=pltpu.VMEM)
    smem = pl.BlockSpec(memory_space=pltpu.SMEM)
    scratch = [
        pltpu.VMEM((16, SLAB, 4 * HD), jnp.bfloat16),
        pltpu.VMEM((9, 2, 2 * SLAB, WIDE), jnp.float32),
    ]
    operands = [v for v, _, _ in items]
    spots = [(chips, second) for _, chips, second in items]
    for t, start, first in jobs:
        operands += parts[t]
        if not first:
            operands += states[t]
    if last:
        out_shape = [pltpu.VMEM((SLAB, HALF), jnp.bfloat16)] * len(jobs)
        scratch = [pltpu.VMEM(s, jnp.float32) for s in STATE] + scratch
    else:
        out_shape = [pltpu.VMEM(s, jnp.float32) for s in STATE]
        if jobs[0][2]:
            out_shape.append(pltpu.VMEM((SLAB, HALF), jnp.bfloat16))
        out_shape = out_shape * len(jobs)
    return pl.pallas_call(
        functools.partial(attend_kernel, jobs, spots, last),
        in_specs=[smem, smem] + [vmem] * len(operands),
        out_specs=[vmem] * len(out_shape),
        out_shape=out_shape,
        scratch_shapes=scratch,
        compiler_params=pltpu.CompilerParams(vmem_limit_bytes=28 << 20),
        cost_estimate=pl.CostEstimate(
            flops=2 * SLAB * len(spots) * 4 * SLAB * HALF,
            bytes_accessed=2 << 20,
            transcendentals=0,
        ),
    )(in_hbm(slab_sequence), in_hbm(slab_order), *[in_vmem(v) for v in operands])


def join_kernel(core_ref, kept_ref, received_ref, out_ref):
    core = core_ref[0]
    out_ref[:, pl.ds(pl.multiple_of(core * HALF, HALF), HALF)] = kept_ref[...]
    out_ref[:, pl.ds(pl.multiple_of((1 - core) * HALF, HALF), HALF)] = received_ref[...]


def join(core, kept, received):
    vmem = pl.BlockSpec(memory_space=pltpu.VMEM)
    return pl.pallas_call(
        join_kernel,
        in_specs=[pl.BlockSpec(memory_space=pltpu.SMEM), vmem, vmem],
        out_specs=vmem,
        out_shape=jax.ShapeDtypeStruct((SLAB, Q_COLS), jnp.bfloat16),
        compiler_params=pltpu.CompilerParams(vmem_limit_bytes=8 << 20),
        cost_estimate=pl.CostEstimate(flops=SLAB * Q_COLS, bytes_accessed=1 << 20, transcendentals=0),
        name="join",
    )(core, in_vmem(kept), in_vmem(received))


def local(tokens, qkv_weight, owner_slot, slab_sequence, slab_order):
    rows = tokens[0]
    core = lax.rem(lax.axis_index("cp"), 2)
    others = permute(rows, OTHER_CORE)
    owners = (permute(owner_slot, OTHER_CORE), owner_slot)
    core = core.reshape(1)
    rows, kv_weight, *tables = prepare(core, owners, slab_order, rows, qkv_weight)
    kv = project_kv(owners, others, rows, kv_weight, tables)
    queries = project_q(core, owners, others, rows, qkv_weight, tables)
    moved = [permute(kv[k], shift_x(k)) for k in (1, 3, 2)]
    parts = [[queries[0]] + [permute(queries[k], shift_x(k)) for k in (1, 3, 2)]]
    own = kv[0] + moved[0] + moved[1] + moved[2]
    first = []
    for k in (1, 3, 2):
        first.append(permute(own, shift_first(k)))
    parts.append([queries[4]] + [permute(queries[4 + k], shift_x(k)) for k in (1, 3, 2)])
    low = jnp.concatenate([own, first[0]], axis=0)
    high = jnp.concatenate([first[1], first[2]], axis=0)
    left = [permute(v, shift_second(1)) for v in (low, high)]
    right = [permute(v, shift_second(3)) for v in (high, low)]
    far = [permute(left[0], shift_second(1)), permute(right[0], shift_second(3))]
    local_items = [(low, LOW, 0), (high, HIGH, 0)]
    near_items = [(left[0], LOW, 1), (left[1], HIGH, 1), (right[0], HIGH, 3), (right[1], LOW, 3)]
    far_items = [(far[0], LOW, 2), (far[1], HIGH, 2)]
    tables = (slab_sequence, slab_order)
    state = [None, None]
    for t in (0, 1):
        *state[t], query = attend([(t, 0, True)], *tables, local_items, parts, state, False)
        parts[t] = [query]
    both = attend([(0, 0, False), (1, 0, False)], *tables, near_items, parts, state, False)
    state = [both[:3], both[3:]]
    sent, kept = attend([(0, 0, False), (1, 0, False)], *tables, far_items, parts, state, True)
    received = permute(sent, OTHER_CORE)
    return join(core, kept, received)[None]


def solution(mesh):
    in_specs = (P("dp", "cp", None), P(), P("dp", "cp"), P(), P())
    out_specs = P("dp", "cp", None)
    return jax.shard_map(local, mesh=mesh, in_specs=in_specs, out_specs=out_specs, check_vma=False)
```

```python
import functools

import jax
import jax.numpy as jnp
from jax import lax
from jax.experimental import pallas as pl
from jax.experimental.pallas import tpu as pltpu
from jax.sharding import PartitionSpec as P


QH = 16
KVH = 4
HD = 128
SLAB = 128
GROUP = QH // KVH
NEG_FILL = -1e30
AXES = ("dp", "cp")
SIDE = 4
Q_COLS = QH * HD


def pairs(move):
    out = []
    for x in range(SIDE):
        for z in range(SIDE):
            for y in range(SIDE):
                for c in range(2):
                    nx, nz, ny, nc = move(x, z, y, c)
                    here = x * 32 + (z * SIDE + y) * 2 + c
                    there = (nx % SIDE) * 32 + ((nz % SIDE) * SIDE + ny % SIDE) * 2 + nc % 2
                    out.append((here, there))
    return out


def shift_x(k):
    return pairs(lambda x, z, y, c: (x + k, z, y, c))


def shift_first(k):
    return pairs(lambda x, z, y, c: (x, z + k, y, c) if c == 0 else (x, z, y + k, c))


def shift_second(k):
    return pairs(lambda x, z, y, c: (x, z, y + k, c) if c == 0 else (x, z + k, y, c))


OTHER_CORE = pairs(lambda x, z, y, c: (x, z, y, c + 1))


def permute(value, table):
    return lax.ppermute(value, AXES, table)


def rope_tables(order, cos_ref, sin_ref):
    half_rows = SLAB // 2
    lane = lax.broadcasted_iota(jnp.int32, (half_rows, HD), 1)
    row = lax.broadcasted_iota(jnp.int32, (half_rows, HD), 0)
    left = lane < HD // 2
    index = jnp.where(left, lane, lane - HD // 2).astype(jnp.float32)
    frequency = jnp.exp(index * (-2.0 / HD * 13.122363377404328))
    token = jnp.where(left, row, row + half_rows)
    angle = (order * SLAB + token).astype(jnp.float32) * frequency
    for value, ref, sign in ((jnp.cos(angle), cos_ref, 1.0), (jnp.sin(angle), sin_ref, -1.0)):
        turned = pltpu.roll(value, HD // 2, 1)
        ref[:half_rows] = jnp.where(left, sign * value, turned)
        ref[half_rows:] = jnp.where(left, sign * turned, value)


def rope(block, table):
    return block * table[0][...] + pltpu.roll(block, HD // 2, 1) * table[1][...]


CHUNKS = 4


def prepare_kernel(core_ref, owner_ref, order_ref, x_ref, w_ref, *refs):
    x_out, w_out, cos_ref, sin_ref, sems = refs
    core = core_ref[0]
    width = 2 * HD
    rows = w_out.shape[0] // CHUNKS
    copies = [pltpu.make_async_copy(x_ref, x_out, sems.at[2 * CHUNKS])]
    for part in range(2):
        base = pl.multiple_of((QH + part * KVH) * HD + core * width, width)
        for n in range(CHUNKS):
            piece = pl.ds(n * rows, rows)
            copies.append(
                pltpu.make_async_copy(
                    w_ref.at[piece, pl.ds(base, width)],
                    w_out.at[piece, part * width : (part + 1) * width],
                    sems.at[part * CHUNKS + n],
                )
            )
    for copy in copies:
        copy.start()
    rope_tables(order_ref[owner_ref[0, 0], lax.axis_index("cp")], cos_ref, sin_ref)
    for copy in copies:
        copy.wait()


def prepare(core, owner, slab_order, rows, weight):
    smem = pl.BlockSpec(memory_space=pltpu.SMEM)
    anywhere = pl.BlockSpec(memory_space=pl.ANY)
    vmem = pl.BlockSpec(memory_space=pltpu.VMEM)
    depth = rows.shape[1]
    return pl.pallas_call(
        prepare_kernel,
        in_specs=[smem] * 3 + [anywhere] * 2,
        out_specs=[vmem] * 4,
        out_shape=[
            pltpu.VMEM(rows.shape, rows.dtype),
            pltpu.VMEM((depth, 4 * HD), weight.dtype),
        ]
        + [pltpu.VMEM((SLAB, HD), jnp.float32)] * 2,
        scratch_shapes=[pltpu.SemaphoreType.DMA((2 * CHUNKS + 1,))],
        compiler_params=pltpu.CompilerParams(vmem_limit_bytes=8 << 20),
        cost_estimate=pl.CostEstimate(flops=1 << 26, bytes_accessed=5 << 20, transcendentals=1 << 16),
        name="prepare",
    )(core, owner, in_hbm(slab_order), in_hbm(rows), in_hbm(weight))


def store_masked(outs, owner, rows, first, value):
    my_row = lax.axis_index("dp")
    columns = pl.ds(first if isinstance(first, int) else pl.multiple_of(first, HD), HD)
    for k, out in enumerate(outs):
        mine = owner == lax.rem(my_row + k, SIDE)
        out[rows, columns] = jnp.where(mine, value, jnp.zeros_like(value))


def kv_kernel(core_ref, other_ref, owner_ref, order_ref, y_ref, x_ref, w_ref, *refs):
    ropes, outs = (refs[2:4], refs[:2]), refs[4:]
    column = lax.axis_index("cp") + 1 - 2 * core_ref[0]
    rope_tables(order_ref[other_ref[0, 0], column], *ropes[0])
    owners = (other_ref[0, 0], owner_ref[0, 0])
    both = jnp.concatenate([y_ref[...], x_ref[...]], axis=0)
    wide = 512
    for first in range(0, 4 * HD, wide):
        projected = jnp.dot(
            both, w_ref[:, first : first + wide], preferred_element_type=jnp.float32
        )
        for slot in range(2):
            rows = slice(slot * SLAB, (slot + 1) * SLAB)
            for h in range(wide // HD):
                block = projected[rows, h * HD : (h + 1) * HD]
                if first + h * HD < 2 * HD:
                    value = rope(block, ropes[slot]).astype(jnp.bfloat16)
                else:
                    value = block.T.astype(jnp.bfloat16)
                store_masked(outs, owners[slot], rows, first + h * HD, value)


def q_kernel(core_ref, other_ref, owner_ref, w_ref, y_ref, x_ref, *refs):
    ropes, outs = (refs[:2], refs[2:4]), refs[4:12]
    w_scr, sems = refs[12:]
    owners = (other_ref[0, 0], owner_ref[0, 0])
    depth, width = w_scr.shape[1:]
    rows = depth // CHUNKS
    copies = []
    for part in range(QPARTS):
        base = pl.multiple_of(core_ref[0] * HALF + part * width, width)
        for n in range(CHUNKS):
            piece = pl.ds(n * rows, rows)
            copies.append(
                pltpu.make_async_copy(
                    w_ref.at[piece, pl.ds(base, width)],
                    w_scr.at[part, piece, :],
                    sems.at[part * CHUNKS + n],
                )
            )
    for copy in copies:
        copy.start()
    for part in range(QPARTS):
        for copy in copies[part * CHUNKS : (part + 1) * CHUNKS]:
            copy.wait()
        both = jnp.concatenate([y_ref[...], x_ref[...]], axis=0)
        projected = jnp.dot(both, w_scr[part], preferred_element_type=jnp.float32)
        for slot in range(2):
            for h in range(width // HD):
                block = projected[slot * SLAB : (slot + 1) * SLAB, h * HD : (h + 1) * HD]
                value = rope(block, ropes[slot]).T.astype(jnp.bfloat16)
                store_masked(
                    outs[4 * slot : 4 * slot + 4], owners[slot], slice(None), part * width + h * HD, value
                )


def in_vmem(value):
    return pltpu.with_memory_space_constraint(value, pltpu.VMEM)


def in_hbm(value):
    return pltpu.with_memory_space_constraint(value, pltpu.HBM)


def project_kv(core, owners, slab_order, others, rows, weight, tables):
    smem = pl.BlockSpec(memory_space=pltpu.SMEM)
    vmem = pl.BlockSpec(memory_space=pltpu.VMEM)
    operands = [in_vmem(v) for v in (others, rows, weight, *tables)]
    return pl.pallas_call(
        kv_kernel,
        in_specs=[smem] * 4 + [vmem] * len(operands),
        out_specs=[vmem] * 6,
        out_shape=[pltpu.VMEM((SLAB, HD), jnp.float32)] * 2
        + [pltpu.VMEM((2 * SLAB, 4 * HD), jnp.bfloat16)] * 4,
        compiler_params=pltpu.CompilerParams(vmem_limit_bytes=24 << 20),
        cost_estimate=pl.CostEstimate(
            flops=4 * SLAB * rows.shape[1] * 4 * HD, bytes_accessed=4 << 20, transcendentals=0
        ),
        name="kv_proj",
    )(core, *owners, in_hbm(slab_order), *operands)


QPARTS = 2


def project_q(core, owners, others, rows, weight, tables):
    depth, width = rows.shape[1], HALF // QPARTS
    smem = pl.BlockSpec(memory_space=pltpu.SMEM)
    vmem = pl.BlockSpec(memory_space=pltpu.VMEM)
    operands = [in_vmem(v) for v in (others, rows, *tables)]
    return pl.pallas_call(
        q_kernel,
        in_specs=[smem] * 3 + [pl.BlockSpec(memory_space=pl.ANY)] + [vmem] * len(operands),
        out_specs=[vmem] * 8,
        out_shape=[pltpu.VMEM((SLAB, HALF), jnp.bfloat16)] * 8,
        scratch_shapes=[
            pltpu.VMEM((QPARTS, depth, width), weight.dtype),
            pltpu.SemaphoreType.DMA((QPARTS * CHUNKS,)),
        ],
        compiler_params=pltpu.CompilerParams(vmem_limit_bytes=28 << 20),
        cost_estimate=pl.CostEstimate(
            flops=4 * SLAB * depth * HALF, bytes_accessed=2 * depth * HALF, transcendentals=0
        ),
        name="q_proj",
    )(core, *owners, in_hbm(weight), *operands)


FACTOR = HD**-0.5 * 1.4426950408889634
WIDE = GROUP * SLAB
HALF = Q_COLS // 2
STATE = ((2, HD, WIDE), (2, 8, WIDE), (2, 8, WIDE))
LOW, HIGH = (0, 1), (3, 2)


def collect(t, spots, pieces, sequence_ref, order_ref, kv):
    row = lax.axis_index("dp")
    column = lax.axis_index("cp")
    core, y, z = lax.rem(column, 2), lax.rem(column // 2, SIDE), column // (2 * SIDE)
    mine = column if t == 1 else column + 1 - 2 * core
    my_sequence, my_order = sequence_ref[row, mine], order_ref[row, mine]
    count = jnp.int32(0)
    for piece, (chips, second) in zip(pieces, spots):
        for b, k in enumerate(chips):
            sz = lax.rem(z + 2 * SIDE - jnp.where(core == 0, k, second), SIDE)
            sy = lax.rem(y + 2 * SIDE - jnp.where(core == 0, second, k), SIDE)
            for c in range(2):
                source = (sz * SIDE + sy) * 2 + (core if c == 1 else 1 - core)
                wanted = (sequence_ref[row, source] == my_sequence) & (
                    order_ref[row, source] < my_order
                )

                @pl.when(wanted)
                def _():
                    kv[count] = piece[(b * 2 + c) * SLAB : (b * 2 + c + 1) * SLAB, :]

                count = count + wanted.astype(jnp.int32)

    @pl.when(lax.rem(count, 2) == 1)
    def _():
        kv[count] = jnp.zeros((SLAB, 4 * HD), jnp.bfloat16)

    return count


def attend_slab(t, spots, pieces, parts, old, new, out, sequence_ref, order_ref, kv, scores_ref):
    acc, peak, total = new[:3]
    first = old is None
    if first:
        q_ref = new[3]
        q_ref[...] = parts[0][...] + parts[1][...] + parts[2][...] + parts[3][...]
    else:
        (q_ref,) = parts
    count = collect(t, spots, pieces, sequence_ref, order_ref, kv)
    pairs_here = (count + 1) // 2
    starts = []
    for g in range(2):
        if first:
            key_row = lax.broadcasted_iota(jnp.int32, (SLAB, WIDE), 0)
            token = lax.rem(lax.broadcasted_iota(jnp.int32, (SLAB, WIDE), 1), SLAB)
            scores = jnp.dot(
                pieces[0][t * SLAB : (t + 1) * SLAB, g * HD : (g + 1) * HD],
                q_ref[:, g * WIDE : (g + 1) * WIDE],
                preferred_element_type=jnp.float32,
            )
            scores = jnp.where(key_row <= token, scores, NEG_FILL)
            scores_ref[8, g, :SLAB] = scores
            peak[g] = jnp.max(scores.reshape(SLAB // 8, 8, WIDE), axis=0)
        else:
            starts.append(jnp.max(old[1][g], axis=0, keepdims=True))
            peak[g] = old[1][g]

    def score(p, carry):
        full = 2 * p + 1 < count
        for g in range(2):
            keys = slice(g * HD, (g + 1) * HD)
            both = jnp.concatenate([kv[2 * p, :, keys], kv[2 * p + 1, :, keys]], axis=0)
            scores = jnp.dot(
                both, q_ref[:, g * WIDE : (g + 1) * WIDE], preferred_element_type=jnp.float32
            )
            low = scores[:SLAB]
            high = jnp.where(full, scores[SLAB:], NEG_FILL)
            scores_ref[p, g, :SLAB] = low
            scores_ref[p, g, SLAB:] = high
            top = jnp.maximum(low, high).reshape(SLAB // 8, 8, WIDE)
            peak[g] = jnp.maximum(peak[g], jnp.max(top, axis=0))
        return carry

    lax.fori_loop(0, pairs_here, score, 0)
    tops = []
    for g in range(2):
        top = jnp.max(peak[g], axis=0, keepdims=True)
        tops.append(top * FACTOR)
        if first:
            weights = jnp.exp2(scores_ref[8, g, :SLAB] * FACTOR - tops[g])
            total[g] = jnp.sum(weights.reshape(SLAB // 8, 8, WIDE), axis=0)
            acc[g] = jnp.dot(
                pieces[0][t * SLAB : (t + 1) * SLAB, (2 + g) * HD : (3 + g) * HD],
                weights.astype(jnp.bfloat16),
                preferred_element_type=jnp.float32,
            )
        else:
            rescale = jnp.exp2((starts[g] - top) * FACTOR)
            total[g] = old[2][g] * rescale
            acc[g] = old[0][g] * rescale

    def weigh(p, carry):
        for g in range(2):
            values = slice((2 + g) * HD, (3 + g) * HD)
            weights = jnp.exp2(scores_ref[p, g] * FACTOR - tops[g])
            total[g] = total[g] + jnp.sum(weights.reshape(SLAB // 4, 8, WIDE), axis=0)
            both = jnp.concatenate([kv[2 * p, :, values], kv[2 * p + 1, :, values]], axis=1)
            acc[g] = acc[g] + jnp.dot(
                both, weights.astype(jnp.bfloat16), preferred_element_type=jnp.float32
            )
        return carry

    lax.fori_loop(0, pairs_here, weigh, 0)
    if out is not None:
        for g in range(2):
            context = acc[g] * (1.0 / jnp.sum(total[g], axis=0, keepdims=True))
            for h in range(GROUP):
                head = g * GROUP + h
                out[:, head * HD : (head + 1) * HD] = context[:, h * SLAB : (h + 1) * SLAB].T.astype(
                    jnp.bfloat16
                )


def attend_kernel(jobs, spots, last, sequence_ref, order_ref, *refs):
    pieces, refs = refs[: len(spots)], refs[len(spots) :]
    given = []
    for t, start, first in jobs:
        parts, refs = (refs[:4], refs[4:]) if first else (refs[:1], refs[1:])
        old = None
        if not first:
            old, refs = refs[:3], refs[3:]
        given.append((parts, old))
    per = 1 if last else 4 if jobs[0][2] else 3
    outs, refs = refs[: per * len(jobs)], refs[per * len(jobs) :]
    state, refs = (refs[:3], refs[3:]) if last else (None, refs)
    kv, scores_ref = refs
    for n, (t, start, first) in enumerate(jobs):
        parts, old = given[n]
        new = state if last else outs[per * n : per * n + per]
        out = outs[n] if last else None
        attend_slab(
            t, spots[start:], pieces[start:], parts, old, new, out,
            sequence_ref, order_ref, kv, scores_ref,
        )


def attend(jobs, slab_sequence, slab_order, items, parts, states, last):
    vmem = pl.BlockSpec(memory_space=pltpu.VMEM)
    smem = pl.BlockSpec(memory_space=pltpu.SMEM)
    scratch = [
        pltpu.VMEM((16, SLAB, 4 * HD), jnp.bfloat16),
        pltpu.VMEM((9, 2, 2 * SLAB, WIDE), jnp.float32),
    ]
    operands = [v for v, _, _ in items]
    spots = [(chips, second) for _, chips, second in items]
    for t, start, first in jobs:
        operands += parts[t]
        if not first:
            operands += states[t]
    if last:
        out_shape = [pltpu.VMEM((SLAB, HALF), jnp.bfloat16)] * len(jobs)
        scratch = [pltpu.VMEM(s, jnp.float32) for s in STATE] + scratch
    else:
        out_shape = [pltpu.VMEM(s, jnp.float32) for s in STATE]
        if jobs[0][2]:
            out_shape.append(pltpu.VMEM((SLAB, HALF), jnp.bfloat16))
        out_shape = out_shape * len(jobs)
    return pl.pallas_call(
        functools.partial(attend_kernel, jobs, spots, last),
        in_specs=[smem, smem] + [vmem] * len(operands),
        out_specs=[vmem] * len(out_shape),
        out_shape=out_shape,
        scratch_shapes=scratch,
        compiler_params=pltpu.CompilerParams(vmem_limit_bytes=28 << 20),
        cost_estimate=pl.CostEstimate(
            flops=2 * SLAB * len(spots) * 4 * SLAB * HALF,
            bytes_accessed=2 << 20,
            transcendentals=0,
        ),
    )(in_hbm(slab_sequence), in_hbm(slab_order), *[in_vmem(v) for v in operands])


def join_kernel(core_ref, kept_ref, received_ref, out_ref):
    core = core_ref[0]
    out_ref[:, pl.ds(pl.multiple_of(core * HALF, HALF), HALF)] = kept_ref[...]
    out_ref[:, pl.ds(pl.multiple_of((1 - core) * HALF, HALF), HALF)] = received_ref[...]


def join(core, kept, received):
    vmem = pl.BlockSpec(memory_space=pltpu.VMEM)
    return pl.pallas_call(
        join_kernel,
        in_specs=[pl.BlockSpec(memory_space=pltpu.SMEM), vmem, vmem],
        out_specs=vmem,
        out_shape=jax.ShapeDtypeStruct((SLAB, Q_COLS), jnp.bfloat16),
        compiler_params=pltpu.CompilerParams(vmem_limit_bytes=8 << 20),
        cost_estimate=pl.CostEstimate(flops=SLAB * Q_COLS, bytes_accessed=1 << 20, transcendentals=0),
        name="join",
    )(core, in_vmem(kept), in_vmem(received))


def local(tokens, qkv_weight, owner_slot, slab_sequence, slab_order):
    rows = tokens[0]
    core = lax.rem(lax.axis_index("cp"), 2)
    others = permute(rows, OTHER_CORE)
    owners = (permute(owner_slot, OTHER_CORE), owner_slot)
    core = core.reshape(1)
    rows, kv_weight, *tables = prepare(core, owner_slot, slab_order, rows, qkv_weight)
    other_cos, other_sin, *kv = project_kv(
        core, owners, slab_order, others, rows, kv_weight, tables
    )
    tables = (other_cos, other_sin, *tables)
    queries = project_q(core, owners, others, rows, qkv_weight, tables)
    moved = [permute(kv[k], shift_x(k)) for k in (1, 3, 2)]
    parts = [[queries[0]] + [permute(queries[k], shift_x(k)) for k in (1, 3, 2)]]
    own = kv[0] + moved[0] + moved[1] + moved[2]
    first = []
    for k in (1, 3, 2):
        first.append(permute(own, shift_first(k)))
    parts.append([queries[4]] + [permute(queries[4 + k], shift_x(k)) for k in (1, 3, 2)])
    low = jnp.concatenate([own, first[0]], axis=0)
    high = jnp.concatenate([first[1], first[2]], axis=0)
    left = [permute(v, shift_second(1)) for v in (low, high)]
    right = [permute(v, shift_second(3)) for v in (high, low)]
    far = [permute(left[0], shift_second(1)), permute(right[0], shift_second(3))]
    local_items = [(low, LOW, 0), (high, HIGH, 0)]
    near_items = [(left[0], LOW, 1), (left[1], HIGH, 1), (right[0], HIGH, 3), (right[1], LOW, 3)]
    far_items = [(far[0], LOW, 2), (far[1], HIGH, 2)]
    tables = (slab_sequence, slab_order)
    state = [None, None]
    for t in (0, 1):
        *state[t], query = attend([(t, 0, True)], *tables, local_items, parts, state, False)
        parts[t] = [query]
    both = attend([(0, 0, False), (1, 0, False)], *tables, near_items, parts, state, False)
    state = [both[:3], both[3:]]
    sent, kept = attend([(0, 0, False), (1, 0, False)], *tables, far_items, parts, state, True)
    received = permute(sent, OTHER_CORE)
    return join(core, kept, received)[None]


def solution(mesh):
    in_specs = (P("dp", "cp", None), P(), P("dp", "cp"), P(), P())
    out_specs = P("dp", "cp", None)
    return jax.shard_map(local, mesh=mesh, in_specs=in_specs, out_specs=out_specs, check_vma=False)
```

```python
import functools

import jax
import jax.numpy as jnp
from jax import lax
from jax.experimental import pallas as pl
from jax.experimental.pallas import tpu as pltpu
from jax.sharding import PartitionSpec as P


QH = 16
KVH = 4
HD = 128
SLAB = 128
GROUP = QH // KVH
NEG_FILL = -1e30
AXES = ("dp", "cp")
SIDE = 4
Q_COLS = QH * HD


def pairs(move):
    out = []
    for x in range(SIDE):
        for z in range(SIDE):
            for y in range(SIDE):
                for c in range(2):
                    nx, nz, ny, nc = move(x, z, y, c)
                    here = x * 32 + (z * SIDE + y) * 2 + c
                    there = (nx % SIDE) * 32 + ((nz % SIDE) * SIDE + ny % SIDE) * 2 + nc % 2
                    out.append((here, there))
    return out


def shift_x(k):
    return pairs(lambda x, z, y, c: (x + k, z, y, c))


def shift_first(k):
    return pairs(lambda x, z, y, c: (x, z + k, y, c) if c == 0 else (x, z, y + k, c))


def shift_second(k):
    return pairs(lambda x, z, y, c: (x, z, y + k, c) if c == 0 else (x, z + k, y, c))


OTHER_CORE = pairs(lambda x, z, y, c: (x, z, y, c + 1))


def permute(value, table):
    return lax.ppermute(value, AXES, table)


def rope_tables(order, cos_ref, sin_ref):
    half_rows = SLAB // 2
    lane = lax.broadcasted_iota(jnp.int32, (half_rows, HD), 1)
    row = lax.broadcasted_iota(jnp.int32, (half_rows, HD), 0)
    left = lane < HD // 2
    index = jnp.where(left, lane, lane - HD // 2).astype(jnp.float32)
    frequency = jnp.exp(index * (-2.0 / HD * 13.122363377404328))
    token = jnp.where(left, row, row + half_rows)
    angle = (order * SLAB + token).astype(jnp.float32) * frequency
    for value, ref, sign in ((jnp.cos(angle), cos_ref, 1.0), (jnp.sin(angle), sin_ref, -1.0)):
        turned = pltpu.roll(value, HD // 2, 1)
        ref[:half_rows] = jnp.where(left, sign * value, turned)
        ref[half_rows:] = jnp.where(left, sign * turned, value)


def rope(block, table):
    return block * table[0][...] + pltpu.roll(block, HD // 2, 1) * table[1][...]


CHUNKS = 4


def prepare_kernel(core_ref, owner_ref, order_ref, x_ref, w_ref, *refs):
    x_out, w_out, cos_ref, sin_ref, sems = refs
    core = core_ref[0]
    width = 2 * HD
    rows = w_out.shape[0] // CHUNKS
    copies = [pltpu.make_async_copy(x_ref, x_out, sems.at[2 * CHUNKS])]
    for part in range(2):
        base = pl.multiple_of((QH + part * KVH) * HD + core * width, width)
        for n in range(CHUNKS):
            piece = pl.ds(n * rows, rows)
            copies.append(
                pltpu.make_async_copy(
                    w_ref.at[piece, pl.ds(base, width)],
                    w_out.at[piece, part * width : (part + 1) * width],
                    sems.at[part * CHUNKS + n],
                )
            )
    for copy in copies:
        copy.start()
    rope_tables(order_ref[owner_ref[0, 0], lax.axis_index("cp")], cos_ref, sin_ref)
    for copy in copies:
        copy.wait()


def prepare(core, owner, slab_order, rows, weight):
    smem = pl.BlockSpec(memory_space=pltpu.SMEM)
    anywhere = pl.BlockSpec(memory_space=pl.ANY)
    vmem = pl.BlockSpec(memory_space=pltpu.VMEM)
    depth = rows.shape[1]
    return pl.pallas_call(
        prepare_kernel,
        in_specs=[smem] * 3 + [anywhere] * 2,
        out_specs=[vmem] * 4,
        out_shape=[
            pltpu.VMEM(rows.shape, rows.dtype),
            pltpu.VMEM((depth, 4 * HD), weight.dtype),
        ]
        + [pltpu.VMEM((SLAB, HD), jnp.float32)] * 2,
        scratch_shapes=[pltpu.SemaphoreType.DMA((2 * CHUNKS + 1,))],
        compiler_params=pltpu.CompilerParams(vmem_limit_bytes=8 << 20),
        cost_estimate=pl.CostEstimate(flops=1 << 26, bytes_accessed=5 << 20, transcendentals=1 << 16),
        name="prepare",
    )(core, owner, in_hbm(slab_order), in_hbm(rows), in_hbm(weight))


def store_masked(outs, owner, rows, first, value):
    my_row = lax.axis_index("dp")
    columns = pl.ds(first if isinstance(first, int) else pl.multiple_of(first, HD), HD)
    for k, out in enumerate(outs):
        mine = owner == lax.rem(my_row + k, SIDE)
        out[rows, columns] = jnp.where(mine, value, jnp.zeros_like(value))


def kv_kernel(core_ref, other_ref, owner_ref, order_ref, y_ref, x_ref, w_ref, *refs):
    ropes, outs = (refs[2:4], refs[:2]), refs[4:]
    column = lax.axis_index("cp") + 1 - 2 * core_ref[0]
    rope_tables(order_ref[other_ref[0, 0], column], *ropes[0])
    owners = (other_ref[0, 0], owner_ref[0, 0])
    both = jnp.concatenate([y_ref[...], x_ref[...]], axis=0)
    wide = 512
    for first in range(0, 4 * HD, wide):
        projected = jnp.dot(
            both, w_ref[:, first : first + wide], preferred_element_type=jnp.float32
        )
        for slot in range(2):
            rows = slice(slot * SLAB, (slot + 1) * SLAB)
            for h in range(wide // HD):
                block = projected[rows, h * HD : (h + 1) * HD]
                if first + h * HD < 2 * HD:
                    value = rope(block, ropes[slot]).astype(jnp.bfloat16)
                else:
                    value = block.T.astype(jnp.bfloat16)
                store_masked(outs, owners[slot], rows, first + h * HD, value)


def q_kernel(core_ref, other_ref, owner_ref, w_ref, y_ref, x_ref, *refs):
    ropes, outs = (refs[:2], refs[2:4]), refs[4:12]
    w_scr, sems = refs[12:]
    owners = (other_ref[0, 0], owner_ref[0, 0])
    depth, width = w_scr.shape[1:]
    rows = depth // CHUNKS
    copies = []
    for part in range(QPARTS):
        base = pl.multiple_of(core_ref[0] * HALF + part * width, width)
        for n in range(CHUNKS):
            piece = pl.ds(n * rows, rows)
            copies.append(
                pltpu.make_async_copy(
                    w_ref.at[piece, pl.ds(base, width)],
                    w_scr.at[part, piece, :],
                    sems.at[part * CHUNKS + n],
                )
            )
    for copy in copies:
        copy.start()
    for part in range(QPARTS):
        for copy in copies[part * CHUNKS : (part + 1) * CHUNKS]:
            copy.wait()
        both = jnp.concatenate([y_ref[...], x_ref[...]], axis=0)
        projected = jnp.dot(both, w_scr[part], preferred_element_type=jnp.float32)
        for slot in range(2):
            for h in range(width // HD):
                block = projected[slot * SLAB : (slot + 1) * SLAB, h * HD : (h + 1) * HD]
                value = rope(block, ropes[slot]).T.astype(jnp.bfloat16)
                store_masked(
                    outs[4 * slot : 4 * slot + 4], owners[slot], slice(None), part * width + h * HD, value
                )


def in_vmem(value):
    return pltpu.with_memory_space_constraint(value, pltpu.VMEM)


def in_hbm(value):
    return pltpu.with_memory_space_constraint(value, pltpu.HBM)


def project_kv(core, owners, slab_order, others, rows, weight, tables):
    smem = pl.BlockSpec(memory_space=pltpu.SMEM)
    vmem = pl.BlockSpec(memory_space=pltpu.VMEM)
    operands = [in_vmem(v) for v in (others, rows, weight, *tables)]
    return pl.pallas_call(
        kv_kernel,
        in_specs=[smem] * 4 + [vmem] * len(operands),
        out_specs=[vmem] * 6,
        out_shape=[pltpu.VMEM((SLAB, HD), jnp.float32)] * 2
        + [pltpu.VMEM((2 * SLAB, 4 * HD), jnp.bfloat16)] * 4,
        compiler_params=pltpu.CompilerParams(vmem_limit_bytes=24 << 20),
        cost_estimate=pl.CostEstimate(
            flops=4 * SLAB * rows.shape[1] * 4 * HD, bytes_accessed=4 << 20, transcendentals=0
        ),
        name="kv_proj",
    )(core, *owners, in_hbm(slab_order), *operands)


QPARTS = 2


def project_q(core, owners, others, rows, weight, tables):
    depth, width = rows.shape[1], HALF // QPARTS
    smem = pl.BlockSpec(memory_space=pltpu.SMEM)
    vmem = pl.BlockSpec(memory_space=pltpu.VMEM)
    operands = [in_vmem(v) for v in (others, rows, *tables)]
    return pl.pallas_call(
        q_kernel,
        in_specs=[smem] * 3 + [pl.BlockSpec(memory_space=pl.ANY)] + [vmem] * len(operands),
        out_specs=[vmem] * 8,
        out_shape=[pltpu.VMEM((SLAB, HALF), jnp.bfloat16)] * 8,
        scratch_shapes=[
            pltpu.VMEM((QPARTS, depth, width), weight.dtype),
            pltpu.SemaphoreType.DMA((QPARTS * CHUNKS,)),
        ],
        compiler_params=pltpu.CompilerParams(vmem_limit_bytes=28 << 20),
        cost_estimate=pl.CostEstimate(
            flops=4 * SLAB * depth * HALF, bytes_accessed=2 * depth * HALF, transcendentals=0
        ),
        name="q_proj",
    )(core, *owners, in_hbm(weight), *operands)


FACTOR = HD**-0.5 * 1.4426950408889634
WIDE = GROUP * SLAB
HALF = Q_COLS // 2
STATE = ((2, HD, WIDE), (2, 8, WIDE), (2, 8, WIDE))
LOW, HIGH = (0, 1), (3, 2)


def collect(t, spots, pieces, sequence_ref, order_ref, kv):
    row = lax.axis_index("dp")
    column = lax.axis_index("cp")
    core, y, z = lax.rem(column, 2), lax.rem(column // 2, SIDE), column // (2 * SIDE)
    mine = column if t == 1 else column + 1 - 2 * core
    my_sequence, my_order = sequence_ref[row, mine], order_ref[row, mine]
    count = jnp.int32(0)
    for piece, (chips, second) in zip(pieces, spots):
        for b, k in enumerate(chips):
            sz = lax.rem(z + 2 * SIDE - jnp.where(core == 0, k, second), SIDE)
            sy = lax.rem(y + 2 * SIDE - jnp.where(core == 0, second, k), SIDE)
            for c in range(2):
                source = (sz * SIDE + sy) * 2 + (core if c == 1 else 1 - core)
                wanted = (sequence_ref[row, source] == my_sequence) & (
                    order_ref[row, source] < my_order
                )

                @pl.when(wanted)
                def _():
                    kv[count] = piece[(b * 2 + c) * SLAB : (b * 2 + c + 1) * SLAB, :]

                count = count + wanted.astype(jnp.int32)

    @pl.when(lax.rem(count, 2) == 1)
    def _():
        kv[count] = jnp.zeros((SLAB, 4 * HD), jnp.bfloat16)

    return count


def attend_slab(t, spots, pieces, parts, old, new, out, sequence_ref, order_ref, kv, scores_ref):
    acc, peak, total = new[:3]
    first = old is None
    if first:
        q_ref = new[3]
        q_ref[...] = parts[0][...] + parts[1][...] + parts[2][...] + parts[3][...]
    else:
        (q_ref,) = parts
    count = collect(t, spots, pieces, sequence_ref, order_ref, kv)
    pairs_here = (count + 1) // 2
    starts = []
    for g in range(2):
        if first:
            key_row = lax.broadcasted_iota(jnp.int32, (SLAB, WIDE), 0)
            token = lax.rem(lax.broadcasted_iota(jnp.int32, (SLAB, WIDE), 1), SLAB)
            scores = jnp.dot(
                pieces[0][t * SLAB : (t + 1) * SLAB, g * HD : (g + 1) * HD],
                q_ref[:, g * WIDE : (g + 1) * WIDE],
                preferred_element_type=jnp.float32,
            )
            scores = jnp.where(key_row <= token, scores, NEG_FILL)
            scores_ref[8, g, :SLAB] = scores
            peak[g] = jnp.max(scores.reshape(SLAB // 8, 8, WIDE), axis=0)
        else:
            starts.append(jnp.max(old[1][g], axis=0, keepdims=True))
            peak[g] = old[1][g]

    def score(p, carry):
        full = 2 * p + 1 < count
        for g in range(2):
            keys = slice(g * HD, (g + 1) * HD)
            both = jnp.concatenate([kv[2 * p, :, keys], kv[2 * p + 1, :, keys]], axis=0)
            scores = jnp.dot(
                both, q_ref[:, g * WIDE : (g + 1) * WIDE], preferred_element_type=jnp.float32
            )
            low = scores[:SLAB]
            high = jnp.where(full, scores[SLAB:], NEG_FILL)
            scores_ref[p, g, :SLAB] = low
            scores_ref[p, g, SLAB:] = high
            top = jnp.maximum(low, high).reshape(SLAB // 8, 8, WIDE)
            peak[g] = jnp.maximum(peak[g], jnp.max(top, axis=0))
        return carry

    lax.fori_loop(0, pairs_here, score, 0)
    tops = []
    for g in range(2):
        top = jnp.max(peak[g], axis=0, keepdims=True)
        tops.append(top * FACTOR)
        if first:
            weights = jnp.exp2(scores_ref[8, g, :SLAB] * FACTOR - tops[g])
            total[g] = jnp.sum(weights.reshape(SLAB // 8, 8, WIDE), axis=0)
            acc[g] = jnp.dot(
                pieces[0][t * SLAB : (t + 1) * SLAB, (2 + g) * HD : (3 + g) * HD],
                weights.astype(jnp.bfloat16),
                preferred_element_type=jnp.float32,
            )
        else:
            rescale = jnp.exp2((starts[g] - top) * FACTOR)
            total[g] = old[2][g] * rescale
            acc[g] = old[0][g] * rescale

    def weigh(p, carry):
        for g in range(2):
            values = slice((2 + g) * HD, (3 + g) * HD)
            weights = jnp.exp2(scores_ref[p, g] * FACTOR - tops[g])
            total[g] = total[g] + jnp.sum(weights.reshape(SLAB // 4, 8, WIDE), axis=0)
            both = jnp.concatenate([kv[2 * p, :, values], kv[2 * p + 1, :, values]], axis=1)
            acc[g] = acc[g] + jnp.dot(
                both, weights.astype(jnp.bfloat16), preferred_element_type=jnp.float32
            )
        return carry

    lax.fori_loop(0, pairs_here, weigh, 0)
    if out is not None:
        for g in range(2):
            context = acc[g] * (1.0 / jnp.sum(total[g], axis=0, keepdims=True))
            for h in range(GROUP):
                head = g * GROUP + h
                out[:, head * HD : (head + 1) * HD] = context[:, h * SLAB : (h + 1) * SLAB].T.astype(
                    jnp.bfloat16
                )


def attend_kernel(jobs, spots, last, sequence_ref, order_ref, *refs):
    pieces, refs = refs[: len(spots)], refs[len(spots) :]
    given = []
    for t, start, first in jobs:
        parts, refs = (refs[:4], refs[4:]) if first else (refs[:1], refs[1:])
        old = None
        if not first:
            old, refs = refs[:3], refs[3:]
        given.append((parts, old))
    per = 1 if last else 4 if jobs[0][2] else 3
    outs, refs = refs[: per * len(jobs)], refs[per * len(jobs) :]
    state, refs = (refs[:3], refs[3:]) if last else (None, refs)
    kv, scores_ref = refs
    for n, (t, start, first) in enumerate(jobs):
        parts, old = given[n]
        new = state if last else outs[per * n : per * n + per]
        out = outs[n] if last else None
        attend_slab(
            t, spots[start:], pieces[start:], parts, old, new, out,
            sequence_ref, order_ref, kv, scores_ref,
        )


def attend(jobs, slab_sequence, slab_order, items, parts, states, last):
    vmem = pl.BlockSpec(memory_space=pltpu.VMEM)
    smem = pl.BlockSpec(memory_space=pltpu.SMEM)
    scratch = [
        pltpu.VMEM((16, SLAB, 4 * HD), jnp.bfloat16),
        pltpu.VMEM((9, 2, 2 * SLAB, WIDE), jnp.float32),
    ]
    operands = [v for v, _, _ in items]
    spots = [(chips, second) for _, chips, second in items]
    for t, start, first in jobs:
        operands += parts[t]
        if not first:
            operands += states[t]
    if last:
        out_shape = [pltpu.VMEM((SLAB, HALF), jnp.bfloat16)] * len(jobs)
        scratch = [pltpu.VMEM(s, jnp.float32) for s in STATE] + scratch
    else:
        out_shape = [pltpu.VMEM(s, jnp.float32) for s in STATE]
        if jobs[0][2]:
            out_shape.append(pltpu.VMEM((SLAB, HALF), jnp.bfloat16))
        out_shape = out_shape * len(jobs)
    return pl.pallas_call(
        functools.partial(attend_kernel, jobs, spots, last),
        in_specs=[smem, smem] + [vmem] * len(operands),
        out_specs=[vmem] * len(out_shape),
        out_shape=out_shape,
        scratch_shapes=scratch,
        compiler_params=pltpu.CompilerParams(vmem_limit_bytes=28 << 20),
        cost_estimate=pl.CostEstimate(
            flops=2 * SLAB * len(spots) * 4 * SLAB * HALF,
            bytes_accessed=2 << 20,
            transcendentals=0,
        ),
    )(in_hbm(slab_sequence), in_hbm(slab_order), *[in_vmem(v) for v in operands])


def join_kernel(core_ref, kept_ref, received_ref, out_ref):
    core = core_ref[0]
    out_ref[:, pl.ds(pl.multiple_of(core * HALF, HALF), HALF)] = kept_ref[...]
    out_ref[:, pl.ds(pl.multiple_of((1 - core) * HALF, HALF), HALF)] = received_ref[...]


def join(core, kept, received):
    vmem = pl.BlockSpec(memory_space=pltpu.VMEM)
    return pl.pallas_call(
        join_kernel,
        in_specs=[pl.BlockSpec(memory_space=pltpu.SMEM), vmem, vmem],
        out_specs=vmem,
        out_shape=jax.ShapeDtypeStruct((SLAB, Q_COLS), jnp.bfloat16),
        compiler_params=pltpu.CompilerParams(vmem_limit_bytes=8 << 20),
        cost_estimate=pl.CostEstimate(flops=SLAB * Q_COLS, bytes_accessed=1 << 20, transcendentals=0),
        name="join",
    )(core, in_vmem(kept), in_vmem(received))


def local(tokens, qkv_weight, owner_slot, slab_sequence, slab_order):
    rows = tokens[0]
    core = lax.rem(lax.axis_index("cp"), 2)
    others = permute(rows, OTHER_CORE)
    owners = (permute(owner_slot, OTHER_CORE), owner_slot)
    core = core.reshape(1)
    rows, kv_weight, *tables = prepare(core, owner_slot, slab_order, rows, qkv_weight)
    other_cos, other_sin, *kv = project_kv(
        core, owners, slab_order, others, rows, kv_weight, tables
    )
    tables = (other_cos, other_sin, *tables)
    queries = project_q(core, owners, others, rows, qkv_weight, tables)
    moved = []
    for k in (2, 1, 3):
        moved.append(permute(kv[k], shift_x(k)))
    parts = [[queries[0]], [queries[4]]]
    for k in (2, 1, 3):
        parts[0].append(permute(queries[k], shift_x(k)))
        parts[1].append(permute(queries[4 + k], shift_x(k)))
    own = kv[0] + moved[0] + moved[1] + moved[2]
    first = []
    for k in (1, 3, 2):
        first.append(permute(own, shift_first(k)))
    low = jnp.concatenate([own, first[0]], axis=0)
    high = jnp.concatenate([first[1], first[2]], axis=0)
    left = [permute(v, shift_second(1)) for v in (low, high)]
    right = [permute(v, shift_second(3)) for v in (high, low)]
    far = [permute(left[0], shift_second(1)), permute(right[0], shift_second(3))]
    local_items = [(low, LOW, 0), (high, HIGH, 0)]
    near_items = [(left[0], LOW, 1), (left[1], HIGH, 1), (right[0], HIGH, 3), (right[1], LOW, 3)]
    far_items = [(far[0], LOW, 2), (far[1], HIGH, 2)]
    tables = (slab_sequence, slab_order)
    state = [None, None]
    for t in (0, 1):
        *state[t], query = attend([(t, 0, True)], *tables, local_items, parts, state, False)
        parts[t] = [query]
    both = attend([(0, 0, False), (1, 0, False)], *tables, near_items, parts, state, False)
    state = [both[:3], both[3:]]
    (sent,) = attend([(0, 0, False)], *tables, far_items, parts, state, True)
    received = permute(sent, OTHER_CORE)
    (kept,) = attend([(1, 0, False)], *tables, far_items, parts, state, True)
    return join(core, kept, received)[None]


def solution(mesh):
    in_specs = (P("dp", "cp", None), P(), P("dp", "cp"), P(), P())
    out_specs = P("dp", "cp", None)
    return jax.shard_map(local, mesh=mesh, in_specs=in_specs, out_specs=out_specs, check_vma=False)
```
